128 devices in a mesh: tp: 4 (over x), dp: 32 (over z, y, core).
Axes of the slice: x: 4, y: 4, z: 4, core: 2. Of those that a mesh axis runs over, the one named last changes fastest.
Arguments:
- w_in: float32 [1, 768, 5376], P(None, None, 'tp')
- w_out: float32 [1, 3840, 768], P(None, 'tp')
- g_in: float32 [32, 1, 768, 5376], P('dp', None, None, 'tp')
- g_out: float32 [32, 1, 3840, 768], P('dp', None, 'tp')
- m_in: bfloat16 [1, 768, 5376], P(None, 'dp', 'tp')
- m_out: bfloat16 [1, 3840, 768], P(None, 'tp', 'dp')
- r_in: float32 [1, 768], P(None, 'dp')
- c_in: float32 [1, 5376], P(None, 'tp')
- r_out: float32 [1, 3840], P(None, 'tp')
- c_out: float32 [1, 768], P(None, 'dp')
- learn_rate: float32 [], replicated
- weight_decay: float32 [], replicated
- beta_two: float32 [], replicated
Outputs:
- output 1: float32 [1, 768, 5376], P(None, None, 'tp')
- output 2: float32 [1, 3840, 768], P(None, 'tp')
- output 3: bfloat16 [1, 768, 5376], P(None, 'dp', 'tp')
- output 4: bfloat16 [1, 3840, 768], P(None, 'tp', 'dp')
- output 5: float32 [1, 768], P(None, 'dp')
- output 6: float32 [1, 5376], P(None, 'tp')
- output 7: float32 [1, 3840], P(None, 'tp')
- output 8: float32 [1, 768], P(None, 'dp')
All inputs are finite; a program needn't handle non-finite values.
Results may differ from the reference program's by a relative error of at most 0.0012163.
Values sent between devices are 32-bit elements.
A program may use at most 1 GiB of HBM per device.

```python
import math
import jax
import jax.numpy as jnp

LAYERS = 1
D = 768
MLP = 3072
DP = 32

FIN = MLP + 3 * D
FOUT = MLP + D


def axis_scales(key, count):
    key_ramp, key_noise = jax.random.split(key)
    ramp_slope = jax.random.uniform(key_ramp, (LAYERS, 1), jnp.float32, 0.6, 1.0)
    ramp_vals = jnp.linspace(-1.0, 1.0, count, dtype=jnp.float32)[None, :]
    noise_vals = jax.random.normal(key_noise, (LAYERS, count), jnp.float32)
    return jnp.exp(ramp_slope * ramp_vals + 0.3 * noise_vals)


def draw_matrix(key, n_rows, n_cols):
    key_list = jax.random.split(key, 7)
    row_scale = axis_scales(key_list[0], n_rows)
    col_scale = axis_scales(key_list[1], n_cols)
    noise_rep = jax.random.normal(key_list[2], (DP, LAYERS, n_rows, n_cols), jnp.float32)
    grad_rep = noise_rep * (row_scale[:, :, None] * col_scale[:, None, :] / math.sqrt(DP))
    grad_sum = jnp.sum(grad_rep, axis=0)
    grad_sq = grad_sum * grad_sum
    row_noise = jax.random.normal(key_list[3], (LAYERS, n_rows), jnp.float32)
    col_noise = jax.random.normal(key_list[4], (LAYERS, n_cols), jnp.float32)
    row_old = 0.25 * jnp.mean(grad_sq, axis=2) * jnp.exp(0.5 * row_noise)
    col_old = 0.25 * jnp.mean(grad_sq, axis=1) * jnp.exp(0.5 * col_noise)
    weight = jax.random.normal(key_list[5], (LAYERS, n_rows, n_cols), jnp.float32) * n_rows ** -0.5
    moment = (0.1 * jax.random.normal(key_list[6], (LAYERS, n_rows, n_cols), jnp.float32)).astype(jnp.bfloat16)
    return weight, grad_rep, moment, row_old, col_old


def setup_inputs(seed: int = 0) -> dict:
    key_list = jax.random.split(jax.random.key(seed), 5)
    w_in, g_in, m_in, r_in, c_in = draw_matrix(key_list[0], D, FIN)
    w_out, g_out, m_out, r_out, c_out = draw_matrix(key_list[1], FOUT, D)
    learn_rate = jax.random.uniform(key_list[2], (), jnp.float32, 0.25, 0.75) * D ** -0.5
    weight_decay = jax.random.uniform(key_list[3], (), jnp.float32, 0.15, 0.45) * D ** 0.5
    beta_two = jax.random.uniform(key_list[4], (), jnp.float32, 0.8, 0.9)
    return dict(w_in=w_in, w_out=w_out, g_in=g_in, g_out=g_out, m_in=m_in, m_out=m_out, r_in=r_in, c_in=c_in, r_out=r_out, c_out=c_out, learn_rate=learn_rate, weight_decay=weight_decay, beta_two=beta_two)


def adafactor_matrix(weight, grad_rep, moment, row_old, col_old, learn_rate, weight_decay, beta_two):
    grad_sum = jnp.sum(grad_rep, axis=0)
    grad_sq = grad_sum * grad_sum + 1e-30
    row_new = beta_two * row_old + (1.0 - beta_two) * jnp.mean(grad_sq, axis=2)
    col_new = beta_two * col_old + (1.0 - beta_two) * jnp.mean(grad_sq, axis=1)
    row_avg = jnp.mean(row_new, axis=1)
    second = row_new[:, :, None] * col_new[:, None, :] / row_avg[:, None, None]
    update = grad_sum / jnp.sqrt(second)
    rms_val = jnp.sqrt(jnp.mean(update * update, axis=(1, 2)))
    update = update / jnp.maximum(1.0, rms_val)[:, None, None]
    mom_new = (0.9 * moment.astype(jnp.float32) + 0.1 * update).astype(jnp.bfloat16)
    w_new = weight - learn_rate * mom_new.astype(jnp.float32) - learn_rate * weight_decay * weight
    return w_new, mom_new, row_new, col_new


def reference(w_in, w_out, g_in, g_out, m_in, m_out, r_in, c_in, r_out, c_out, learn_rate, weight_decay, beta_two):
    in_result = adafactor_matrix(w_in, g_in, m_in, r_in, c_in, learn_rate, weight_decay, beta_two)
    out_result = adafactor_matrix(w_out, g_out, m_out, r_out, c_out, learn_rate, weight_decay, beta_two)
    return (in_result[0], out_result[0], in_result[1], out_result[1], in_result[2], in_result[3], out_result[2], out_result[3])
```

```python
import jax
import jax.numpy as jnp
from jax import lax
from jax.experimental import pallas as pl
from jax.experimental.pallas import tpu as pltpu
from jax.sharding import PartitionSpec as P

MESH = pl.DeviceIdType.MESH
F32 = jnp.float32
BF16 = jnp.bfloat16

D = 768
F_IN = 1344
F_OUT = 960
HALF = 1152
TAIL = 192
N_IN = 5376
N_OUT = 3840
CUT = 640
PIECES = ((0, 640), (640, 960), (960, 1152))


def half_ref(in_ref, out_ref, half, lo, hi):
    if half == 0:
        return in_ref.at[pl.ds(lo, hi - lo)]
    if hi <= F_OUT:
        return out_ref.at[pl.ds(lo, hi - lo)]
    return in_ref.at[pl.ds(lo - F_OUT + HALF, hi - lo)]


def join_tail(out_val, tail_val, pad_a, pad_b):
    pad_a[...] = jnp.zeros_like(pad_a)
    pad_b[...] = jnp.zeros_like(pad_b)
    pad_a[:, 0:64] = out_val[:, 896:960]
    pad_b[:, 0:192] = tail_val
    moved = pltpu.roll(pad_b[...], 64, 1)
    lane = lax.broadcasted_iota(jnp.int32, pad_a.shape, 1)
    mid = jnp.where(lane < 64, pad_a[...], moved[:, 0:128])
    return jnp.concatenate([out_val[:, 0:896], mid, moved[:, 128:256]], axis=1)


def kernel(scal, g_in, g_out, w_in, w_out, m_in, m_out, r_in, c_in, r_out, c_out,
           o_w_in, o_w_out, o_m_in, o_m_out, o_r_in, o_c_in, o_r_out, o_c_out,
           xown, xrecv, wown, ybuf, tbuf, t2buf, far, dirb, comb, pbuf, far2, dir2, comb2,
           mx, ms, mrecv, fo, fnew, frecv, fv, rv, qa, qb, ub, pad_a, pad_b, pad_c, pad_d, rowpad,
           load_sem, send, recv):
    x = lax.axis_index("tp")
    d = lax.axis_index("dp")
    core = lax.rem(d, 2)
    p = lax.div(d, 2)
    y = lax.rem(p, 4)
    z = lax.div(p, 4)

    def at(xx, pp, cc):
        return (xx, pp * 2 + cc)

    partner = at(x, p, 1 - core)
    sem_count = [0]
    copies = []

    def remote(src, dst, dev, sem=None):
        if sem is None:
            sem = sem_count[0]
            sem_count[0] += 1
        c = pltpu.make_async_remote_copy(src_ref=src, dst_ref=dst, send_sem=send.at[sem], recv_sem=recv.at[sem], device_id=dev, device_id_type=MESH)
        copies.append(c)
        return c

    for me in (0, 1):
        @pl.when(core == me)
        def _():
            for i, (lo, hi) in enumerate(PIECES):
                pltpu.make_async_copy(half_ref(g_in, g_out, me, lo, hi), xown.at[pl.ds(lo, hi - lo)], load_sem.at[i]).start()
            for i, (lo, hi) in enumerate(PIECES):
                pltpu.make_async_copy(half_ref(w_in, w_out, me, lo, hi), wown.at[pl.ds(lo, hi - lo)], load_sem.at[3 + i]).start()

    barrier = pltpu.get_barrier_semaphore()
    greet = [at(x, z * 4 + lax.rem(y + 1, 4), core), at(x, z * 4 + lax.rem(y + 3, 4), core),
             at(x, lax.rem(z + 1, 4) * 4 + y, core), at(x, lax.rem(z + 3, 4) * 4 + y, core)]
    line = []
    for k in range(1, 8):
        other = lax.rem(x * 2 + core + k, 8)
        line.append(at(lax.div(other, 2), p, lax.rem(other, 2)))
    plane = [at(x, lax.rem(p + k, 16), core) for k in range(1, 16)]
    for dev in greet + line:
        pl.semaphore_signal(barrier, inc=1, device_id=dev, device_id_type=MESH)
    pl.semaphore_wait(barrier, len(greet) + len(line))

    swap = []
    for i, (lo, hi) in enumerate(PIECES):
        sem = sem_count[0]
        sem_count[0] += 1
        swap.append(sem)
        for me in (0, 1):
            @pl.when(core == me)
            def _():
                pltpu.make_async_remote_copy(
                    src_ref=half_ref(g_in, g_out, 1 - me, lo, hi), dst_ref=xrecv.at[pl.ds(lo, hi - lo)],
                    send_sem=send.at[sem], recv_sem=recv.at[sem], device_id=partner, device_id_type=MESH).start()

    first = m_in[:, 0:HALF].astype(F32)
    second = join_tail(m_out[...].astype(F32), m_in[:, HALF:F_IN].astype(F32), pad_a, pad_b)
    on_first = core == 0
    mx[core] = jnp.where(on_first, first, second)
    ms[...] = jnp.where(on_first, second, first)
    m_copy = remote(ms, mx.at[core], partner)
    m_copy.start()
    fo[...] = jnp.where(on_first, c_in[:, 0:HALF], join_tail(r_out[...], c_in[:, HALF:F_IN], pad_c, pad_d))

    def transpose_in(j, _):
        rows = pl.ds(pl.multiple_of(j * 128, 128), 128)
        for h in range(2):
            cols = pl.ds(h * 384, 384)
            t = (xown[rows, cols] + xrecv[rows, cols]).T
            for i in range(16):
                tbuf[2 * h + i // 8, (i // 2) % 4, i % 2, :, rows] = t[24 * i:24 * i + 24]
        return 0

    def swap_wait(i):
        lo, hi = PIECES[i]
        pltpu.make_async_copy(xown.at[pl.ds(lo, hi - lo)], xown.at[pl.ds(lo, hi - lo)], load_sem.at[i]).wait()
        pltpu.make_async_remote_copy(
            src_ref=xown.at[pl.ds(lo, hi - lo)], dst_ref=xrecv.at[pl.ds(lo, hi - lo)],
            send_sem=send.at[swap[i]], recv_sem=recv.at[swap[i]], device_id=partner, device_id_type=MESH).wait_recv()

    part_a, part_b = pl.ds(0, CUT), pl.ds(CUT, HALF - CUT)
    ring = ((y, at(x, z * 4 + lax.rem(y + 1, 4), core), at(x, z * 4 + lax.rem(y + 3, 4), core)),
            (z, at(x, lax.rem(z + 1, 4) * 4 + y, core), at(x, lax.rem(z + 3, 4) * 4 + y, core)))

    def chunk(buf, a, k, lanes):
        return buf.at[:, k, 0, :, lanes] if a == 0 else buf.at[k, :, 1, :, lanes]

    swap_wait(0)
    lax.fori_loop(0, 5, transpose_in, 0)
    ph = []
    for a in range(2):
        i, right, left = ring[a]
        r, l, f = lax.rem(i + 1, 4), lax.rem(i + 3, 4), lax.rem(i + 2, 4)
        far_a = remote(chunk(tbuf, a, f, part_a), far.at[a, :, :, part_a], right)
        dir_a = remote(chunk(tbuf, a, l, part_a), dirb.at[a, :, :, part_a], left)
        far_b = remote(chunk(tbuf, a, f, part_b), far.at[a, :, :, part_b], left)
        dir_b = remote(chunk(tbuf, a, r, part_b), dirb.at[a, :, :, part_b], right)
        comb_a = remote(chunk(tbuf, a, r, part_a), comb.at[a, :, :, part_a], right)
        comb_b = remote(chunk(tbuf, a, l, part_b), comb.at[a, :, :, part_b], left)
        ph.append((i, r, l, far_a, dir_a, far_b, dir_b, comb_a, comb_b))
        far_a.start()
        dir_a.start()
    swap_wait(1)
    swap_wait(2)
    lax.fori_loop(5, 9, transpose_in, 0)
    for a in range(2):
        ph[a][5].start()
        ph[a][6].start()
    for which, lanes in ((0, part_a), (1, part_b)):
        for a in range(2):
            i, r, l, far_a, dir_a, far_b, dir_b, comb_a, comb_b = ph[a]
            k = (r, l)[which]
            (far_a, far_b)[which].wait_recv()
            for q in range(4):
                if a == 0:
                    tbuf[q, k, 0, :, lanes] += far[a, q, :, lanes]
                else:
                    tbuf[k, q, 1, :, lanes] += far[a, q, :, lanes]
            (comb_a, comb_b)[which].start()
    for a in range(2):
        i, r, l, far_a, dir_a, far_b, dir_b, comb_a, comb_b = ph[a]
        for c in (dir_a, dir_b, comb_a, comb_b):
            c.wait_recv()
        for q in range(4):
            mine = tbuf[q, i, 0] if a == 0 else tbuf[i, q, 1]
            pbuf[a, q] = mine + dirb[a, q] + comb[a, q]

    ph = []
    for a in range(2):
        i, right, left = ring[1 - a]
        r, l, f = lax.rem(i + 1, 4), lax.rem(i + 3, 4), lax.rem(i + 2, 4)
        far_a = remote(pbuf.at[a, f, :, part_a], far2.at[a, :, part_a], right)
        far_b = remote(pbuf.at[a, f, :, part_b], far2.at[a, :, part_b], left)
        dir_a = remote(pbuf.at[a, l, :, part_a], dir2.at[a, :, part_a], left)
        dir_b = remote(pbuf.at[a, r, :, part_b], dir2.at[a, :, part_b], right)
        comb_a = remote(pbuf.at[a, r, :, part_a], comb2.at[a, :, part_a], right)
        comb_b = remote(pbuf.at[a, l, :, part_b], comb2.at[a, :, part_b], left)
        for c in (far_a, far_b, dir_a, dir_b):
            c.start()
        ph.append((i, r, l, far_a, dir_a, far_b, dir_b, comb_a, comb_b))
    for which, lanes in ((0, part_a), (1, part_b)):
        for a in range(2):
            i, r, l, far_a, dir_a, far_b, dir_b, comb_a, comb_b = ph[a]
            (far_a, far_b)[which].wait_recv()
            pbuf[a, (r, l)[which], :, lanes] += far2[a, :, lanes]
            (comb_a, comb_b)[which].start()
    parts = []
    for a in range(2):
        i, r, l, far_a, dir_a, far_b, dir_b, comb_a, comb_b = ph[a]
        for c in (dir_a, dir_b, comb_a, comb_b):
            c.wait_recv()
        parts.append(pbuf[a, i] + dir2[a] + comb2[a])

    lane = lax.broadcasted_iota(jnp.int32, (1, HALF), 1)
    is_in = lane >= jnp.where(on_first, 0, F_OUT)
    eye = lax.broadcasted_iota(jnp.int32, (48, 128), 0) == lax.broadcasted_iota(jnp.int32, (48, 128), 1)

    def to_row(col):
        return jnp.sum(jnp.where(eye, col, 0.0), axis=0, keepdims=True)

    def to_col(row):
        return jnp.sum(jnp.where(eye, row, 0.0), axis=1, keepdims=True)

    g = jnp.concatenate(parts, axis=0)
    sq = g * g + 1e-30
    fv[p] = jnp.sum(sq, axis=0, keepdims=True)
    fv_copies = [remote(fv.at[p], fv.at[p], dev) for dev in plane]
    for c in fv_copies:
        c.start()
    rv[x, core] = jnp.zeros((8, 128), F32)
    rv[x, core, 0:1, :] = to_row(jnp.sum(jnp.where(is_in, sq, 0.0), axis=1, keepdims=True))
    rv[x, core, 1:2, :] = to_row(jnp.sum(jnp.where(is_in, 0.0, sq), axis=1, keepdims=True))
    for row, ref in ((2, r_in), (3, c_out)):
        rowpad[...] = jnp.zeros_like(rowpad)
        rowpad[0:1, 0:24] = ref[...]
        rv[x, core, row:row + 1, :] = jnp.where(on_first, rowpad[...], pltpu.roll(rowpad[...], 24, 1))[0:1]
    rv_copies = [remote(rv.at[x, core], rv.at[x, core], dev) for dev in line]
    for c in rv_copies:
        c.start()

    lr, wd, beta = scal[0], scal[1], scal[2]
    for c in rv_copies:
        c.wait_recv()
    row_sum = jnp.sum(rv[...].reshape(8, 8, 128), axis=0)
    row_old = rv[0, 0] + rv[0, 1]
    r_new = beta * row_old[2:3] + (1.0 - beta) * (row_sum[0:1] / N_IN)
    c_new = beta * row_old[3:4] + (1.0 - beta) * (row_sum[1:2] / N_OUT)
    row_scale_in = 1.0 / jnp.sqrt(to_col(r_new))
    row_scale_out = 1.0 / jnp.sqrt(to_col(c_new))
    for c in fv_copies:
        c.wait_recv()
    f_new = beta * fo[...] + (1.0 - beta) * (jnp.sum(fv[...], axis=0) / D)
    fnew[...] = f_new
    f_copy = remote(fnew, frecv, partner)
    f_copy.start()
    u = g * jnp.where(is_in, row_scale_in, row_scale_out) * (1.0 / jnp.sqrt(f_new))
    ub[...] = u
    uu = u * u

    def total(v):
        return jnp.sum(jnp.sum(v, axis=0, keepdims=True), axis=1, keepdims=True)

    sum_rows = jnp.sum(r_new, axis=1, keepdims=True)
    qa[x, core] = jnp.zeros((8, 128), F32)
    qa[x, core, 0:1, :] = jnp.broadcast_to(total(jnp.where(is_in, uu, 0.0)), (1, 128))
    qa[x, core, 1:2, :] = jnp.broadcast_to(total(jnp.where(is_in, 0.0, uu)), (1, 128))
    qa[x, core, 2:3, :] = jnp.broadcast_to(total(jnp.where(is_in, 0.0, f_new)), (1, 128))
    qa_copies = [remote(qa.at[x, core], qa.at[x, core], dev) for dev in line]
    for c in qa_copies:
        c.start()
    for c in qa_copies:
        c.wait_recv()
    line_sum = jnp.sum(qa[...].reshape(8, 8, 128), axis=0)
    qb[p] = line_sum
    qb[p, 3:4, :] = jnp.broadcast_to(sum_rows, (1, 128))
    qb_copies = [remote(qb.at[p], qb.at[p], dev) for dev in plane]
    for c in qb_copies:
        c.start()
    for c in qb_copies:
        c.wait_recv()
    plane_sum = jnp.sum(qb[...], axis=0)
    mean_in = plane_sum[3:4, 0:1] / D
    mean_out = line_sum[2:3, 0:1] / N_OUT
    rms_in = jnp.sqrt(plane_sum[0:1, 0:1] * mean_in / (D * N_IN))
    rms_out = jnp.sqrt(plane_sum[1:2, 0:1] * mean_out / (D * N_OUT))
    scale = jnp.where(is_in, jnp.sqrt(mean_in) / jnp.maximum(1.0, rms_in), jnp.sqrt(mean_out) / jnp.maximum(1.0, rms_out))

    m_copy.wait_recv()
    for a in range(2):
        upd = ub[24 * a:24 * a + 24, :] * scale
        t2buf[z, y, a] = (0.9 * mx[a] + 0.1 * upd).astype(BF16).astype(F32)

    def chunk_one(a, k, lanes):
        return t2buf.at[k, y, 0, :, lanes] if a == 0 else t2buf.at[z, k, 1, :, lanes]

    def gather(ref, ring_of):
        fwd = []
        for a in range(2):
            i, right, left = ring_of[a]
            r, l = lax.rem(i + 1, 4), lax.rem(i + 3, 4)
            ra = remote(ref(a, i, part_a), ref(a, i, part_a), right)
            lb = remote(ref(a, i, part_b), ref(a, i, part_b), left)
            rb = remote(ref(a, i, part_b), ref(a, i, part_b), right)
            la = remote(ref(a, i, part_a), ref(a, i, part_a), left)
            for c in (ra, lb, rb, la):
                c.start()
            fa = remote(ref(a, l, part_a), ref(a, l, part_a), right)
            fb = remote(ref(a, r, part_b), ref(a, r, part_b), left)
            fwd.append((ra, lb, rb, la, fa, fb))
        for n in range(2):
            for a in range(2):
                fwd[a][n].wait_recv()
                fwd[a][4 + n].start()
        return [c for a in range(2) for c in fwd[a][2:]]

    pending = gather(chunk_one, (ring[1], ring[0]))
    mo_copy = remote(t2buf.at[z, y, 1 - core], mrecv, partner)
    mo_copy.start()
    for c in pending:
        c.wait_recv()
    pending = gather(lambda a, k, lanes: chunk(t2buf, a, k, lanes), ring)

    mo_copy.wait_recv()
    f_copy.wait_recv()
    for mine, theirs, out_in, out_out in ((t2buf[z, y, core], mrecv[...], o_m_in, o_m_out), (f_new, frecv[...], o_c_in, o_r_out)):
        lo = jnp.where(on_first, mine, theirs)
        hi = jnp.where(on_first, theirs, mine)
        out_in[:, 0:HALF] = lo.astype(out_in.dtype)
        out_out[...] = hi[:, 0:F_OUT].astype(out_out.dtype)
        out_in[:, HALF:F_IN] = pltpu.roll(hi[:, 896:1152], 192, 1)[:, 0:TAIL].astype(out_in.dtype)
    for new, out in ((r_new, o_r_in), (c_new, o_c_out)):
        rowpad[...] = jnp.broadcast_to(new, (8, 128))
        out[...] = jnp.where(on_first, rowpad[...], pltpu.roll(rowpad[...], 104, 1))[0:1, 0:24]

    for c in pending:
        c.wait_recv()

    for i, (lo, hi) in enumerate(PIECES):
        pltpu.make_async_copy(wown.at[pl.ds(lo, hi - lo)], wown.at[pl.ds(lo, hi - lo)], load_sem.at[3 + i]).wait()
    lr_wd = lr * wd

    def transpose_out(j, _):
        rows = pl.ds(pl.multiple_of(j * 128, 128), 128)
        for h in range(2):
            cols = pl.ds(h * 384, 384)
            t = jnp.concatenate([t2buf[2 * h + i // 8, (i // 2) % 4, i % 2, :, rows] for i in range(16)], axis=0)
            w = wown[rows, cols]
            ybuf[rows, cols] = w - lr * t.T - lr_wd * w
        return 0

    out_sems = []
    for i, (lo, hi) in enumerate(PIECES):
        sem = sem_count[0]
        sem_count[0] += 1
        out_sems.append(sem)
        lax.fori_loop((0, 5, 8)[i], (5, 8, 9)[i], transpose_out, 0)
        for me in (0, 1):
            @pl.when(core == me)
            def _():
                src = ybuf.at[pl.ds(lo, hi - lo)]
                dst = half_ref(o_w_in, o_w_out, me, lo, hi)
                pltpu.make_async_remote_copy(src_ref=src, dst_ref=dst, send_sem=send.at[sem], recv_sem=recv.at[sem], device_id=partner, device_id_type=MESH).start()
                pltpu.make_async_copy(src, dst, load_sem.at[6 + i]).start()

    for c in copies:
        c.wait_send()
    for i, (lo, hi) in enumerate(PIECES):
        for me in (0, 1):
            @pl.when(core == me)
            def _():
                src = ybuf.at[pl.ds(lo, hi - lo)]
                mine = half_ref(o_w_in, o_w_out, me, lo, hi)
                theirs = half_ref(o_w_in, o_w_out, 1 - me, lo, hi)
                pltpu.make_async_copy(src, mine, load_sem.at[6 + i]).wait()
                out = pltpu.make_async_remote_copy(src_ref=src, dst_ref=theirs, send_sem=send.at[out_sems[i]], recv_sem=recv.at[out_sems[i]], device_id=partner, device_id_type=MESH)
                out.wait_send()
                out.wait_recv()
                pltpu.make_async_remote_copy(
                    src_ref=half_ref(g_in, g_out, 1 - me, lo, hi), dst_ref=xrecv.at[pl.ds(lo, hi - lo)],
                    send_sem=send.at[swap[i]], recv_sem=recv.at[swap[i]], device_id=partner, device_id_type=MESH).wait_send()
    assert sem_count[0] == N_SEMS, sem_count[0]


N_SEMS = 3 + 1 + 12 + 12 + 15 + 7 + 1 + 7 + 15 + 12 + 1 + 12 + 3


def call(*args):
    vmem = pl.BlockSpec(memory_space=pltpu.VMEM)
    hbm = pl.BlockSpec(memory_space=pl.ANY)
    smem = pl.BlockSpec(memory_space=pltpu.SMEM)
    sds = jax.ShapeDtypeStruct
    return pl.pallas_call(
        kernel,
        name="adafactor_step",
        out_shape=(sds((F_IN, D), F32), sds((F_OUT, D), F32), sds((24, F_IN), BF16), sds((24, F_OUT), BF16),
                   sds((1, 24), F32), sds((1, F_IN), F32), sds((1, F_OUT), F32), sds((1, 24), F32)),
        in_specs=[smem] + [hbm] * 4 + [vmem] * 6,
        out_specs=(hbm, hbm) + (vmem,) * 6,
        scratch_shapes=[
            pltpu.VMEM((HALF, D), F32), pltpu.VMEM((HALF, D), F32), pltpu.VMEM((HALF, D), F32), pltpu.VMEM((HALF, D), F32),
            pltpu.VMEM((4, 4, 2, 24, HALF), F32), pltpu.VMEM((4, 4, 2, 24, HALF), F32),
            pltpu.VMEM((2, 4, 24, HALF), F32), pltpu.VMEM((2, 4, 24, HALF), F32), pltpu.VMEM((2, 4, 24, HALF), F32), pltpu.VMEM((2, 4, 24, HALF), F32),
            pltpu.VMEM((2, 24, HALF), F32), pltpu.VMEM((2, 24, HALF), F32), pltpu.VMEM((2, 24, HALF), F32),
            pltpu.VMEM((2, 24, HALF), F32), pltpu.VMEM((24, HALF), F32), pltpu.VMEM((24, HALF), F32),
            pltpu.VMEM((1, HALF), F32), pltpu.VMEM((1, HALF), F32), pltpu.VMEM((1, HALF), F32),
            pltpu.VMEM((16, 1, HALF), F32), pltpu.VMEM((4, 2, 8, 128), F32), pltpu.VMEM((4, 2, 8, 128), F32), pltpu.VMEM((16, 8, 128), F32),
            pltpu.VMEM((48, HALF), F32), pltpu.VMEM((24, 128), F32), pltpu.VMEM((24, 256), F32), pltpu.VMEM((1, 128), F32), pltpu.VMEM((1, 256), F32), pltpu.VMEM((8, 128), F32),
            pltpu.SemaphoreType.DMA((9,)), pltpu.SemaphoreType.DMA((N_SEMS,)), pltpu.SemaphoreType.DMA((N_SEMS,)),
        ],
        compiler_params=pltpu.CompilerParams(collective_id=0, has_side_effects=True, vmem_limit_bytes=48 * 1024 * 1024),
    )(*args)


def solution(mesh):
    def body(w_in, w_out, g_in, g_out, m_in, m_out, r_in, c_in, r_out, c_out, learn_rate, weight_decay, beta_two):
        scal = jnp.stack([learn_rate, weight_decay, beta_two])
        outs = call(scal, g_in[0, 0].T, g_out[0, 0], w_in[0].T, w_out[0], m_in[0], m_out[0].T, r_in, c_in, r_out, c_out)
        return (outs[0].T[None], outs[1][None], outs[2][None], outs[3].T[None], outs[4], outs[5], outs[6], outs[7])

    in_specs = (P(None, None, 'tp'), P(None, 'tp', None), P('dp', None, None, 'tp'), P('dp', None, 'tp', None), P(None, 'dp', 'tp'), P(None, 'tp', 'dp'), P(None, 'dp'), P(None, 'tp'), P(None, 'tp'), P(None, 'dp'), P(), P(), P())
    out_specs = (P(None, None, 'tp'), P(None, 'tp', None), P(None, 'dp', 'tp'), P(None, 'tp', 'dp'), P(None, 'dp'), P(None, 'tp'), P(None, 'tp'), P(None, 'dp'))
    return jax.shard_map(body, mesh=mesh, in_specs=in_specs, out_specs=out_specs, check_vma=False)
```

```python
import jax
import jax.numpy as jnp
from jax import lax
from jax.experimental import pallas as pl
from jax.experimental.pallas import tpu as pltpu
from jax.sharding import PartitionSpec as P

MESH = pl.DeviceIdType.MESH
F32 = jnp.float32
BF16 = jnp.bfloat16

D = 768
F_IN = 1344
F_OUT = 960
HALF = 1152
TAIL = 192
N_IN = 5376
N_OUT = 3840
CUT = 640
PIECES = ((0, 640), (640, 960), (960, 1152))


def half_ref(in_ref, out_ref, half, lo, hi):
    if half == 0:
        return in_ref.at[pl.ds(lo, hi - lo)]
    if hi <= F_OUT:
        return out_ref.at[pl.ds(lo, hi - lo)]
    return in_ref.at[pl.ds(lo - F_OUT + HALF, hi - lo)]


def join_tail(out_val, tail_val, pad_a, pad_b):
    pad_a[...] = jnp.zeros_like(pad_a)
    pad_b[...] = jnp.zeros_like(pad_b)
    pad_a[:, 0:64] = out_val[:, 896:960]
    pad_b[:, 0:192] = tail_val
    moved = pltpu.roll(pad_b[...], 64, 1)
    lane = lax.broadcasted_iota(jnp.int32, pad_a.shape, 1)
    mid = jnp.where(lane < 64, pad_a[...], moved[:, 0:128])
    return jnp.concatenate([out_val[:, 0:896], mid, moved[:, 128:256]], axis=1)


def kernel(lr_ref, wd_ref, beta_ref, g_in, g_out, w_in, w_out, h_m_in, h_m_out, h_r_in, h_c_in, h_r_out, h_c_out,
           o_w, o_m_in, o_m_out, o_r_in, o_c_in, o_r_out, o_c_out,
           m_in, m_out, r_in, c_in, r_out, c_out,
           xown, xrecv, wown, tbuf, t2buf, far, dirb, comb, pbuf, far2, dir2, comb2,
           mx, ms, mrecv, fo, fnew, frecv, fv, rv, qa, qb, ub, pad_a, pad_b, pad_c, pad_d, rowpad,
           load_sem, send, recv):
    x = lax.axis_index("tp")
    d = lax.axis_index("dp")
    core = lax.rem(d, 2)
    p = lax.div(d, 2)
    y = lax.rem(p, 4)
    z = lax.div(p, 4)

    def at(xx, pp, cc):
        return (xx, pp * 2 + cc)

    partner = at(x, p, 1 - core)
    sem_count = [0]
    copies = []

    def remote(src, dst, dev, sem=None):
        if sem is None:
            sem = sem_count[0]
            sem_count[0] += 1
        c = pltpu.make_async_remote_copy(src_ref=src, dst_ref=dst, send_sem=send.at[sem], recv_sem=recv.at[sem], device_id=dev, device_id_type=MESH)
        copies.append(c)
        return c

    for me in (0, 1):
        @pl.when(core == me)
        def _():
            for i, (lo, hi) in enumerate(PIECES):
                pltpu.make_async_copy(half_ref(g_in, g_out, me, lo, hi), xown.at[pl.ds(lo, hi - lo)], load_sem.at[i]).start()
            for i, (lo, hi) in enumerate(PIECES):
                pltpu.make_async_copy(half_ref(w_in, w_out, me, lo, hi), wown.at[pl.ds(lo, hi - lo)], load_sem.at[3 + i]).start()

    small = [pltpu.make_async_copy(src, dst, load_sem.at[6 + n]) for n, (src, dst) in enumerate((
        (h_m_in, m_in), (h_m_out, m_out), (h_r_in, r_in), (h_c_in, c_in), (h_r_out, r_out), (h_c_out, c_out)))]
    for c in small:
        c.start()

    barrier = pltpu.get_barrier_semaphore()
    greet = [at(x, z * 4 + lax.rem(y + 1, 4), core), at(x, z * 4 + lax.rem(y + 3, 4), core),
             at(x, lax.rem(z + 1, 4) * 4 + y, core), at(x, lax.rem(z + 3, 4) * 4 + y, core)]
    line = []
    for k in range(1, 8):
        other = lax.rem(x * 2 + core + k, 8)
        line.append(at(lax.div(other, 2), p, lax.rem(other, 2)))
    plane = [at(x, lax.rem(p + k, 16), core) for k in range(1, 16)]
    for dev in greet + line:
        pl.semaphore_signal(barrier, inc=1, device_id=dev, device_id_type=MESH)
    pl.semaphore_wait(barrier, len(greet) + len(line))

    swap = []
    for i, (lo, hi) in enumerate(PIECES):
        sem = sem_count[0]
        sem_count[0] += 1
        swap.append(sem)
        for me in (0, 1):
            @pl.when(core == me)
            def _():
                pltpu.make_async_remote_copy(
                    src_ref=half_ref(g_in, g_out, 1 - me, lo, hi), dst_ref=xrecv.at[pl.ds(lo, hi - lo)],
                    send_sem=send.at[sem], recv_sem=recv.at[sem], device_id=partner, device_id_type=MESH).start()

    for c in small:
        c.wait()
    first = m_in[:, 0:HALF].astype(F32)
    second = join_tail(m_out[...].astype(F32), m_in[:, HALF:F_IN].astype(F32), pad_a, pad_b)
    on_first = core == 0
    mx[core] = jnp.where(on_first, first, second)
    ms[...] = jnp.where(on_first, second, first)
    m_copy = remote(ms, mx.at[core], partner)
    m_copy.start()
    fo[...] = jnp.where(on_first, c_in[:, 0:HALF], join_tail(r_out[...], c_in[:, HALF:F_IN], pad_c, pad_d))

    def transpose_in(j, _):
        rows = pl.ds(pl.multiple_of(j * 128, 128), 128)
        for h in range(2):
            cols = pl.ds(h * 384, 384)
            t = (xown[rows, cols] + xrecv[rows, cols]).T
            for i in range(16):
                tbuf[2 * h + i // 8, (i // 2) % 4, i % 2, :, rows] = t[24 * i:24 * i + 24]
        return 0

    def swap_wait(i):
        lo, hi = PIECES[i]
        pltpu.make_async_copy(xown.at[pl.ds(lo, hi - lo)], xown.at[pl.ds(lo, hi - lo)], load_sem.at[i]).wait()
        pltpu.make_async_remote_copy(
            src_ref=xown.at[pl.ds(lo, hi - lo)], dst_ref=xrecv.at[pl.ds(lo, hi - lo)],
            send_sem=send.at[swap[i]], recv_sem=recv.at[swap[i]], device_id=partner, device_id_type=MESH).wait_recv()

    part_a, part_b = pl.ds(0, CUT), pl.ds(CUT, HALF - CUT)
    ring = ((y, at(x, z * 4 + lax.rem(y + 1, 4), core), at(x, z * 4 + lax.rem(y + 3, 4), core)),
            (z, at(x, lax.rem(z + 1, 4) * 4 + y, core), at(x, lax.rem(z + 3, 4) * 4 + y, core)))

    def chunk(buf, a, k, lanes):
        return buf.at[:, k, 0, :, lanes] if a == 0 else buf.at[k, :, 1, :, lanes]

    swap_wait(0)
    lax.fori_loop(0, 5, transpose_in, 0)
    ph = []
    for a in range(2):
        i, right, left = ring[a]
        r, l, f = lax.rem(i + 1, 4), lax.rem(i + 3, 4), lax.rem(i + 2, 4)
        far_a = remote(chunk(tbuf, a, f, part_a), far.at[a, :, :, part_a], right)
        dir_a = remote(chunk(tbuf, a, l, part_a), dirb.at[a, :, :, part_a], left)
        far_b = remote(chunk(tbuf, a, f, part_b), far.at[a, :, :, part_b], left)
        dir_b = remote(chunk(tbuf, a, r, part_b), dirb.at[a, :, :, part_b], right)
        comb_a = remote(chunk(tbuf, a, r, part_a), comb.at[a, :, :, part_a], right)
        comb_b = remote(chunk(tbuf, a, l, part_b), comb.at[a, :, :, part_b], left)
        ph.append((i, r, l, far_a, dir_a, far_b, dir_b, comb_a, comb_b))
        far_a.start()
        dir_a.start()
    swap_wait(1)
    swap_wait(2)
    lax.fori_loop(5, 9, transpose_in, 0)
    for a in range(2):
        ph[a][5].start()
        ph[a][6].start()
    for which, lanes in ((0, part_a), (1, part_b)):
        for a in range(2):
            i, r, l, far_a, dir_a, far_b, dir_b, comb_a, comb_b = ph[a]
            k = (r, l)[which]
            (far_a, far_b)[which].wait_recv()
            for q in range(4):
                if a == 0:
                    tbuf[q, k, 0, :, lanes] += far[a, q, :, lanes]
                else:
                    tbuf[k, q, 1, :, lanes] += far[a, q, :, lanes]
            (comb_a, comb_b)[which].start()
    for a in range(2):
        i, r, l, far_a, dir_a, far_b, dir_b, comb_a, comb_b = ph[a]
        for c in (dir_a, dir_b, comb_a, comb_b):
            c.wait_recv()
        for q in range(4):
            mine = tbuf[q, i, 0] if a == 0 else tbuf[i, q, 1]
            pbuf[a, q] = mine + dirb[a, q] + comb[a, q]

    ph = []
    for a in range(2):
        i, right, left = ring[1 - a]
        r, l, f = lax.rem(i + 1, 4), lax.rem(i + 3, 4), lax.rem(i + 2, 4)
        far_a = remote(pbuf.at[a, f, :, part_a], far2.at[a, :, part_a], right)
        far_b = remote(pbuf.at[a, f, :, part_b], far2.at[a, :, part_b], left)
        dir_a = remote(pbuf.at[a, l, :, part_a], dir2.at[a, :, part_a], left)
        dir_b = remote(pbuf.at[a, r, :, part_b], dir2.at[a, :, part_b], right)
        comb_a = remote(pbuf.at[a, r, :, part_a], comb2.at[a, :, part_a], right)
        comb_b = remote(pbuf.at[a, l, :, part_b], comb2.at[a, :, part_b], left)
        for c in (far_a, far_b, dir_a, dir_b):
            c.start()
        ph.append((i, r, l, far_a, dir_a, far_b, dir_b, comb_a, comb_b))
    for which, lanes in ((0, part_a), (1, part_b)):
        for a in range(2):
            i, r, l, far_a, dir_a, far_b, dir_b, comb_a, comb_b = ph[a]
            (far_a, far_b)[which].wait_recv()
            pbuf[a, (r, l)[which], :, lanes] += far2[a, :, lanes]
            (comb_a, comb_b)[which].start()
    parts = []
    for a in range(2):
        i, r, l, far_a, dir_a, far_b, dir_b, comb_a, comb_b = ph[a]
        for c in (dir_a, dir_b, comb_a, comb_b):
            c.wait_recv()
        parts.append(pbuf[a, i] + dir2[a] + comb2[a])

    lane = lax.broadcasted_iota(jnp.int32, (1, HALF), 1)
    is_in = lane >= jnp.where(on_first, 0, F_OUT)
    eye = lax.broadcasted_iota(jnp.int32, (48, 128), 0) == lax.broadcasted_iota(jnp.int32, (48, 128), 1)

    def to_row(col):
        return jnp.sum(jnp.where(eye, col, 0.0), axis=0, keepdims=True)

    def to_col(row):
        return jnp.sum(jnp.where(eye, row, 0.0), axis=1, keepdims=True)

    g = jnp.concatenate(parts, axis=0)
    sq = g * g + 1e-30
    fv[p] = jnp.sum(sq, axis=0, keepdims=True)
    fv_copies = [remote(fv.at[p], fv.at[p], dev) for dev in plane]
    for c in fv_copies:
        c.start()
    rv[x, core] = jnp.zeros((8, 128), F32)
    rv[x, core, 0:1, :] = to_row(jnp.sum(jnp.where(is_in, sq, 0.0), axis=1, keepdims=True))
    rv[x, core, 1:2, :] = to_row(jnp.sum(jnp.where(is_in, 0.0, sq), axis=1, keepdims=True))
    for row, ref in ((2, r_in), (3, c_out)):
        rowpad[...] = jnp.zeros_like(rowpad)
        rowpad[0:1, 0:24] = ref[...]
        rv[x, core, row:row + 1, :] = jnp.where(on_first, rowpad[...], pltpu.roll(rowpad[...], 24, 1))[0:1]
    rv_copies = [remote(rv.at[x, core], rv.at[x, core], dev) for dev in line]
    for c in rv_copies:
        c.start()

    lr, wd, beta = lr_ref[0], wd_ref[0], beta_ref[0]
    for c in rv_copies:
        c.wait_recv()
    row_sum = jnp.sum(rv[...].reshape(8, 8, 128), axis=0)
    row_old = rv[0, 0] + rv[0, 1]
    r_new = beta * row_old[2:3] + (1.0 - beta) * (row_sum[0:1] / N_IN)
    c_new = beta * row_old[3:4] + (1.0 - beta) * (row_sum[1:2] / N_OUT)
    row_scale_in = 1.0 / jnp.sqrt(to_col(r_new))
    row_scale_out = 1.0 / jnp.sqrt(to_col(c_new))
    for c in fv_copies:
        c.wait_recv()
    f_new = beta * fo[...] + (1.0 - beta) * (jnp.sum(fv[...], axis=0) / D)
    fnew[...] = f_new
    f_copy = remote(fnew, frecv, partner)
    f_copy.start()
    u = g * jnp.where(is_in, row_scale_in, row_scale_out) * (1.0 / jnp.sqrt(f_new))
    ub[...] = u
    uu = u * u

    def total(v):
        return jnp.sum(jnp.sum(v, axis=0, keepdims=True), axis=1, keepdims=True)

    sum_rows = jnp.sum(r_new, axis=1, keepdims=True)
    qa[x, core] = jnp.zeros((8, 128), F32)
    qa[x, core, 0:1, :] = jnp.broadcast_to(total(jnp.where(is_in, uu, 0.0)), (1, 128))
    qa[x, core, 1:2, :] = jnp.broadcast_to(total(jnp.where(is_in, 0.0, uu)), (1, 128))
    qa[x, core, 2:3, :] = jnp.broadcast_to(total(jnp.where(is_in, 0.0, f_new)), (1, 128))
    qa_copies = [remote(qa.at[x, core], qa.at[x, core], dev) for dev in line]
    for c in qa_copies:
        c.start()
    for c in qa_copies:
        c.wait_recv()
    line_sum = jnp.sum(qa[...].reshape(8, 8, 128), axis=0)
    qb[p] = line_sum
    qb[p, 3:4, :] = jnp.broadcast_to(sum_rows, (1, 128))
    qb_copies = [remote(qb.at[p], qb.at[p], dev) for dev in plane]
    for c in qb_copies:
        c.start()
    for c in qb_copies:
        c.wait_recv()
    plane_sum = jnp.sum(qb[...], axis=0)
    mean_in = plane_sum[3:4, 0:1] / D
    mean_out = line_sum[2:3, 0:1] / N_OUT
    rms_in = jnp.sqrt(plane_sum[0:1, 0:1] * mean_in / (D * N_IN))
    rms_out = jnp.sqrt(plane_sum[1:2, 0:1] * mean_out / (D * N_OUT))
    scale = jnp.where(is_in, jnp.sqrt(mean_in) / jnp.maximum(1.0, rms_in), jnp.sqrt(mean_out) / jnp.maximum(1.0, rms_out))

    m_copy.wait_recv()
    for a in range(2):
        upd = ub[24 * a:24 * a + 24, :] * scale
        t2buf[z, y, a] = (0.9 * mx[a] + 0.1 * upd).astype(BF16).astype(F32)

    def chunk_one(a, k, lanes):
        return t2buf.at[k, y, 0, :, lanes] if a == 0 else t2buf.at[z, k, 1, :, lanes]

    def gather(ref, ring_of):
        fwd = []
        for a in range(2):
            i, right, left = ring_of[a]
            r, l = lax.rem(i + 1, 4), lax.rem(i + 3, 4)
            ra = remote(ref(a, i, part_a), ref(a, i, part_a), right)
            lb = remote(ref(a, i, part_b), ref(a, i, part_b), left)
            rb = remote(ref(a, i, part_b), ref(a, i, part_b), right)
            la = remote(ref(a, i, part_a), ref(a, i, part_a), left)
            for c in (ra, lb, rb, la):
                c.start()
            fa = remote(ref(a, l, part_a), ref(a, l, part_a), right)
            fb = remote(ref(a, r, part_b), ref(a, r, part_b), left)
            fwd.append((ra, lb, rb, la, fa, fb))
        for n in range(2):
            for a in range(2):
                fwd[a][n].wait_recv()
                fwd[a][4 + n].start()
        return [c for a in range(2) for c in fwd[a][2:]]

    pending = gather(chunk_one, (ring[1], ring[0]))
    mo_copy = remote(t2buf.at[z, y, 1 - core], mrecv, partner)
    mo_copy.start()
    for c in pending:
        c.wait_recv()
    pending = gather(lambda a, k, lanes: chunk(t2buf, a, k, lanes), ring)

    mo_copy.wait_recv()
    f_copy.wait_recv()
    for mine, theirs, out_in, out_out in ((t2buf[z, y, core], mrecv[...], o_m_in, o_m_out), (f_new, frecv[...], o_c_in, o_r_out)):
        lo = jnp.where(on_first, mine, theirs)
        hi = jnp.where(on_first, theirs, mine)
        out_in[:, 0:HALF] = lo.astype(out_in.dtype)
        out_out[...] = hi[:, 0:F_OUT].astype(out_out.dtype)
        out_in[:, HALF:F_IN] = pltpu.roll(hi[:, 896:1152], 192, 1)[:, 0:TAIL].astype(out_in.dtype)
    for new, out in ((r_new, o_r_in), (c_new, o_c_out)):
        rowpad[...] = jnp.broadcast_to(new, (8, 128))
        out[...] = jnp.where(on_first, rowpad[...], pltpu.roll(rowpad[...], 104, 1))[0:1, 0:24]

    for c in pending:
        c.wait_recv()

    for i, (lo, hi) in enumerate(PIECES):
        pltpu.make_async_copy(wown.at[pl.ds(lo, hi - lo)], wown.at[pl.ds(lo, hi - lo)], load_sem.at[3 + i]).wait()
    lr_wd = lr * wd

    base = core * HALF

    def transpose_out(j, _):
        rows = pl.ds(pl.multiple_of(j * 128, 128), 128)
        dest = pl.ds(pl.multiple_of(base + j * 128, 128), 128)
        for h in range(2):
            cols = pl.ds(h * 384, 384)
            t = jnp.concatenate([t2buf[2 * h + i // 8, (i // 2) % 4, i % 2, :, rows] for i in range(16)], axis=0)
            w = wown[rows, cols]
            o_w[dest, cols] = w - lr * t.T - lr_wd * w
        return 0

    out_copies = []
    for j0, j1 in ((0, 3), (3, 6), (6, 9)):
        lax.fori_loop(j0, j1, transpose_out, 0)
        span = pl.ds(pl.multiple_of(base + j0 * 128, 128), (j1 - j0) * 128)
        c = remote(o_w.at[span], o_w.at[span], partner)
        c.start()
        out_copies.append(c)
    for c in out_copies:
        c.wait_recv()
    for c in copies:
        c.wait_send()
    for i, (lo, hi) in enumerate(PIECES):
        pltpu.make_async_remote_copy(
            src_ref=xown.at[pl.ds(lo, hi - lo)], dst_ref=xrecv.at[pl.ds(lo, hi - lo)],
            send_sem=send.at[swap[i]], recv_sem=recv.at[swap[i]], device_id=partner, device_id_type=MESH).wait_send()
    assert sem_count[0] == N_SEMS, sem_count[0]


N_SEMS = 3 + 1 + 12 + 12 + 15 + 7 + 1 + 7 + 15 + 12 + 1 + 12 + 3


def store_kernel(w, m_in, m_out, r_in, c_in, r_out, c_out, o_w_in, o_w_out, o_m_in, o_m_out, o_r_in, o_c_in, o_r_out, o_c_out, sem):
    pairs = [(w.at[pl.ds(0, HALF)], o_w_in.at[pl.ds(0, HALF)]), (w.at[pl.ds(HALF, F_OUT)], o_w_out), (w.at[pl.ds(HALF + F_OUT, TAIL)], o_w_in.at[pl.ds(HALF, TAIL)]),
             (m_in, o_m_in), (m_out, o_m_out), (r_in, o_r_in), (c_in, o_c_in), (r_out, o_r_out), (c_out, o_c_out)]
    work = [pltpu.make_async_copy(src, dst, sem.at[n]) for n, (src, dst) in enumerate(pairs)]
    for c in work:
        c.start()
    for c in work:
        c.wait()


def call(*args):
    vmem = pl.BlockSpec(memory_space=pltpu.VMEM)
    hbm = pl.BlockSpec(memory_space=pltpu.HBM)
    smem = pl.BlockSpec(memory_space=pltpu.SMEM)
    sds = jax.ShapeDtypeStruct
    small = (((24, F_IN), BF16), ((24, F_OUT), BF16), ((1, 24), F32), ((1, F_IN), F32), ((1, F_OUT), F32), ((1, 24), F32))
    args = args[:3] + tuple(pltpu.with_memory_space_constraint(a, pltpu.HBM) for a in args[3:])
    held = pl.pallas_call(
        kernel,
        name="adafactor_step",
        out_shape=(pltpu.VMEM((2 * HALF, D), F32),) + tuple(pltpu.VMEM(*a) for a in small),
        in_specs=[smem] * 3 + [hbm] * 10,
        out_specs=(vmem,) * 7,
        scratch_shapes=[
            pltpu.VMEM((24, F_IN), BF16), pltpu.VMEM((24, F_OUT), BF16), pltpu.VMEM((1, 24), F32), pltpu.VMEM((1, F_IN), F32), pltpu.VMEM((1, F_OUT), F32), pltpu.VMEM((1, 24), F32),
            pltpu.VMEM((HALF, D), F32), pltpu.VMEM((HALF, D), F32), pltpu.VMEM((HALF, D), F32),
            pltpu.VMEM((4, 4, 2, 24, HALF), F32), pltpu.VMEM((4, 4, 2, 24, HALF), F32),
            pltpu.VMEM((2, 4, 24, HALF), F32), pltpu.VMEM((2, 4, 24, HALF), F32), pltpu.VMEM((2, 4, 24, HALF), F32), pltpu.VMEM((2, 4, 24, HALF), F32),
            pltpu.VMEM((2, 24, HALF), F32), pltpu.VMEM((2, 24, HALF), F32), pltpu.VMEM((2, 24, HALF), F32),
            pltpu.VMEM((2, 24, HALF), F32), pltpu.VMEM((24, HALF), F32), pltpu.VMEM((24, HALF), F32),
            pltpu.VMEM((1, HALF), F32), pltpu.VMEM((1, HALF), F32), pltpu.VMEM((1, HALF), F32),
            pltpu.VMEM((16, 1, HALF), F32), pltpu.VMEM((4, 2, 8, 128), F32), pltpu.VMEM((4, 2, 8, 128), F32), pltpu.VMEM((16, 8, 128), F32),
            pltpu.VMEM((48, HALF), F32), pltpu.VMEM((24, 128), F32), pltpu.VMEM((24, 256), F32), pltpu.VMEM((1, 128), F32), pltpu.VMEM((1, 256), F32), pltpu.VMEM((8, 128), F32),
            pltpu.SemaphoreType.DMA((12,)), pltpu.SemaphoreType.DMA((N_SEMS,)), pltpu.SemaphoreType.DMA((N_SEMS,)),
        ],
        compiler_params=pltpu.CompilerParams(collective_id=0, has_side_effects=True, vmem_limit_bytes=40 * 1024 * 1024),
    )(*args)
    return pl.pallas_call(
        store_kernel,
        name="store_outputs",
        out_shape=(sds((F_IN, D), F32), sds((F_OUT, D), F32)) + tuple(sds(*a) for a in small),
        in_specs=[vmem] * 7,
        out_specs=(hbm,) * 8,
        scratch_shapes=[pltpu.SemaphoreType.DMA((9,))],
        compiler_params=pltpu.CompilerParams(vmem_limit_bytes=16 * 1024 * 1024),
    )(*held)


def solution(mesh):
    def body(w_in, w_out, g_in, g_out, m_in, m_out, r_in, c_in, r_out, c_out, learn_rate, weight_decay, beta_two):
        outs = call(learn_rate[None], weight_decay[None], beta_two[None], g_in[0, 0].T, g_out[0, 0], w_in[0].T, w_out[0], m_in[0], m_out[0].T, r_in, c_in, r_out, c_out)
        return (outs[0].T[None], outs[1][None], outs[2][None], outs[3].T[None], outs[4], outs[5], outs[6], outs[7])

    in_specs = (P(None, None, 'tp'), P(None, 'tp', None), P('dp', None, None, 'tp'), P('dp', None, 'tp', None), P(None, 'dp', 'tp'), P(None, 'tp', 'dp'), P(None, 'dp'), P(None, 'tp'), P(None, 'tp'), P(None, 'dp'), P(), P(), P())
    out_specs = (P(None, None, 'tp'), P(None, 'tp', None), P(None, 'dp', 'tp'), P(None, 'tp', 'dp'), P(None, 'dp'), P(None, 'tp'), P(None, 'tp'), P(None, 'dp'))
    return jax.shard_map(body, mesh=mesh, in_specs=in_specs, out_specs=out_specs, check_vma=False)
```

```python
import jax
import jax.numpy as jnp
from jax import lax
from jax.experimental import pallas as pl
from jax.experimental.pallas import tpu as pltpu
from jax.sharding import PartitionSpec as P

MESH = pl.DeviceIdType.MESH
F32 = jnp.float32
BF16 = jnp.bfloat16
ALL = slice(None)

D = 768
F_IN = 1344
F_OUT = 960
HALF = 1152
TAIL = 192
N_IN = 5376
N_OUT = 3840
T = 128
W = 24
RING = 4
REDUCE_SEGS = ((0, 2, 1), (2, 3, 2), (5, 2, 1), (7, 2, 1))
GATHER_SEGS = ((0, 3, 2), (3, 2, 1), (5, 2, 1), (7, 2, 1))
ROWS_ONE = pl.ds(0, 1)
N_SEND = 13
N_RECV = 44
N_LOAD = 11


def spans(half, lo, hi):
    if half == 0:
        return [(0, lo, lo, hi - lo)]
    out = []
    if lo < F_OUT:
        out.append((1, lo, lo, min(hi, F_OUT) - lo))
    if hi > F_OUT:
        start = max(lo, F_OUT)
        out.append((0, start + TAIL, start, hi - start))
    return out


def join_tail(out_val, tail_val, pad_a, pad_b):
    pad_a[...] = jnp.zeros_like(pad_a)
    pad_b[...] = jnp.zeros_like(pad_b)
    cut = F_OUT - F_OUT % T
    pad_a[:, :F_OUT - cut] = out_val[:, cut:]
    pad_b[:, :TAIL] = tail_val
    moved = pltpu.roll(pad_b[...], F_OUT - cut, 1)
    lane = lax.broadcasted_iota(jnp.int32, pad_a.shape, 1)
    mid = jnp.where(lane < F_OUT - cut, pad_a[...], moved[:, :T])
    return jnp.concatenate([out_val[:, :cut], mid, moved[:, T:]], axis=1)


def kernel(lr_ref, wd_ref, beta_ref, g_in, g_out, w_in, w_out, h_m_in, h_m_out, h_r_in, h_c_in, h_r_out, h_c_out,
           o_w, o_m_in, o_m_out, o_r_in, o_c_in, o_r_out, o_c_out,
           m_in, m_out, r_in, c_in, r_out, c_out,
           xown, xrecv, wown, tbuf, t2buf, far, dc, pbuf, far2, dc2,
           mx, ms, mrecv, fo, fnew, frecv, fv, rv, qa, qb, gb, pad_a, pad_b, pad_c, pad_d, rowpad,
           load_sem, send, recv):
    x = lax.axis_index("tp")
    d = lax.axis_index("dp")
    core = lax.rem(d, 2)
    p = lax.div(d, 2)
    y = lax.rem(p, RING)
    z = lax.div(p, RING)
    on_first = core == 0
    line_me = x * 2 + core

    def at(xx, pp, cc):
        return (xx, pp * 2 + cc)

    def step(i, k):
        return lax.rem(i + k, RING)

    partner = at(x, p, 1 - core)
    sends = iter(range(N_SEND))
    recvs = iter(range(N_RECV))
    loads = iter(range(N_LOAD))

    def remote(src, dst, dev, s, r):
        c = pltpu.make_async_remote_copy(src_ref=src, dst_ref=dst, send_sem=send.at[s], recv_sem=recv.at[r], device_id=dev, device_id_type=MESH)
        c.start()

    def wait(ref, sem):
        pltpu.make_async_copy(ref, ref, sem).wait()

    x_load = [next(loads) for _ in REDUCE_SEGS]
    w_load = next(loads)
    for me in range(2):
        @pl.when(core == me)
        def _():
            for (t0, n, _), sem in zip(REDUCE_SEGS, x_load):
                for which, lo, to, rows in spans(me, t0 * T, (t0 + n) * T):
                    pltpu.make_async_copy((g_in, g_out)[which].at[pl.ds(lo, rows)], xown.at[pl.ds(to, rows)], load_sem.at[sem]).start()
            for which, lo, to, rows in spans(me, 0, HALF):
                pltpu.make_async_copy((w_in, w_out)[which].at[pl.ds(lo, rows)], wown.at[pl.ds(to, rows)], load_sem.at[w_load]).start()
    small = [pltpu.make_async_copy(src, dst, load_sem.at[next(loads)]) for src, dst in (
        (h_m_in, m_in), (h_m_out, m_out), (h_r_in, r_in), (h_c_in, c_in), (h_r_out, r_out), (h_c_out, c_out))]
    for c in small:
        c.start()

    barrier = pltpu.get_barrier_semaphore()
    ring = ((y, at(x, z * RING + step(y, 1), core), at(x, z * RING + step(y, 3), core)),
            (z, at(x, step(z, 1) * RING + y, core), at(x, step(z, 3) * RING + y, core)))
    line = []
    for k in range(1, 8):
        other = lax.rem(line_me + k, 8)
        line.append(at(lax.div(other, 2), p, lax.rem(other, 2)))
    plane = [at(x, lax.rem(p + k, 16), core) for k in range(1, 16)]
    greet = [dev for _, right, left in ring for dev in (right, left)] + line
    for dev in greet:
        pl.semaphore_signal(barrier, inc=1, device_id=dev, device_id_type=MESH)
    pl.semaphore_wait(barrier, len(greet))

    swap_send = next(sends)
    swap_recv = [next(recvs) for _ in REDUCE_SEGS]
    for me in range(2):
        @pl.when(core == me)
        def _():
            for (t0, n, _), sem in zip(REDUCE_SEGS, swap_recv):
                for which, lo, to, rows in spans(1 - me, t0 * T, (t0 + n) * T):
                    remote((g_in, g_out)[which].at[pl.ds(lo, rows)], xrecv.at[pl.ds(to, rows)], partner, swap_send, sem)

    def lanes_of(seg):
        t0, n, n_a = seg
        return pl.ds(t0 * T, n_a * T), pl.ds((t0 + n_a) * T, (n - n_a) * T), pl.ds(t0 * T, n * T)

    blocks = [(i // 8, i // 2 % RING, i % 2) for i in range(16)]

    def transpose_in(j, _):
        rows = pl.ds(pl.multiple_of(j * T, T), T)
        for h in range(2):
            cols = pl.ds(h * D // 2, D // 2)
            t = (xown[rows, cols] + xrecv[rows, cols]).T
            for i, (zz, yy, a) in enumerate(blocks):
                tbuf[2 * h + zz, yy, a, :, rows] = t[W * i:W * i + W]
        return 0

    def chunk(buf, a, k, lanes):
        return buf.at[:, k, 0, :, lanes] if a == 0 else buf.at[k, :, 1, :, lanes]

    send_1, send_2 = next(sends), next(sends)
    far_sem, dc_sem, far2_sem, dc2_sem = ([next(recvs) for _ in REDUCE_SEGS] for _ in range(4))

    def rs_ring(a, phase):
        i, right, left = ring[a if phase == 1 else 1 - a]
        return i, right, left, step(i, 1), step(i, 3), step(i, 2)

    def rs_refs(phase):
        if phase == 1:
            return (lambda a, k, lanes: chunk(tbuf, a, k, lanes), lambda a, lanes: far.at[a, :, :, lanes],
                    lambda kind, a, lanes: dc.at[kind, a, :, :, lanes], send_1, far_sem, dc_sem)
        return (lambda a, k, lanes: pbuf.at[a, k, :, lanes], lambda a, lanes: far2.at[a, :, lanes],
                lambda kind, a, lanes: dc2.at[kind, a, :, lanes], send_2, far2_sem, dc2_sem)

    def rs_begin(s, phase):
        la, lb, _ = lanes_of(REDUCE_SEGS[s])
        src, far_at, dc_at, ss, fs, ds = rs_refs(phase)
        for a in range(2):
            i, right, left, r, l, f = rs_ring(a, phase)
            remote(src(a, f, la), far_at(a, la), right, ss, fs[s])
            remote(src(a, f, lb), far_at(a, lb), left, ss, fs[s])
        for a in range(2):
            i, right, left, r, l, f = rs_ring(a, phase)
            remote(src(a, r, lb), dc_at(0, a, lb), right, ss, ds[s])
            remote(src(a, l, la), dc_at(0, a, la), left, ss, ds[s])

    def rs_middle(s, phase):
        la, lb, full = lanes_of(REDUCE_SEGS[s])
        src, far_at, dc_at, ss, fs, ds = rs_refs(phase)
        wait((far.at[:, :, :, full] if phase == 1 else far2.at[:, :, full]), recv.at[fs[s]])
        for a in range(2):
            i, right, left, r, l, f = rs_ring(a, phase)
            for k, lanes, dev in ((r, la, right), (l, lb, left)):
                if phase == 1:
                    for q in range(RING):
                        where = (q, k, 0) if a == 0 else (k, q, 1)
                        tbuf[(*where, ALL, lanes)] += far[a, q, :, lanes]
                else:
                    pbuf[a, k, :, lanes] += far2[a, :, lanes]
                remote(src(a, k, lanes), dc_at(1, a, lanes), dev, ss, ds[s])

    def rs_end(s, phase):
        _, _, full = lanes_of(REDUCE_SEGS[s])
        wait((dc.at[:, :, :, :, full] if phase == 1 else dc2.at[:, :, :, full]), recv.at[rs_refs(phase)[-1][s]])
        for a in range(2):
            i = rs_ring(a, phase)[0]
            if phase == 1:
                for q in range(RING):
                    where = (q, i, 0) if a == 0 else (i, q, 1)
                    pbuf[a, q, :, full] = tbuf[(*where, ALL, full)] + dc[0, a, q, :, full] + dc[1, a, q, :, full]
            else:
                gb[W * a:W * a + W, full] = pbuf[a, i, :, full] + dc2[0, a, :, full] + dc2[1, a, :, full]

    def prepare():
        for c in small:
            c.wait()
        first = m_in[:, :HALF].astype(F32)
        second = join_tail(m_out[...].astype(F32), m_in[:, HALF:].astype(F32), pad_a, pad_b)
        mx[core] = jnp.where(on_first, first, second)
        ms[...] = jnp.where(on_first, second, first)
        remote(ms, mx.at[core], partner, m_send, m_recv)
        fo[...] = jnp.where(on_first, c_in[:, :HALF], join_tail(r_out[...], c_in[:, HALF:], pad_c, pad_d))

    m_send, m_recv = next(sends), next(recvs)
    n_segs = len(REDUCE_SEGS)
    for t in range(n_segs + RING):
        if t < n_segs:
            t0, n, _ = REDUCE_SEGS[t]
            rows = pl.ds(t0 * T, n * T)
            wait(xown.at[rows], load_sem.at[x_load[t]])
            wait(xown.at[rows], recv.at[swap_recv[t]])
            lax.fori_loop(t0, t0 + n, transpose_in, 0)
            rs_begin(t, 1)
        if t == 1:
            prepare()
        for lag, work in enumerate((lambda s: rs_middle(s, 1), lambda s: (rs_end(s, 1), rs_begin(s, 2)), lambda s: rs_middle(s, 2), lambda s: rs_end(s, 2))):
            s = t - 1 - lag
            if 0 <= s < n_segs:
                work(s)

    lane = lax.broadcasted_iota(jnp.int32, (1, HALF), 1)
    is_in = lane >= jnp.where(on_first, 0, F_OUT)
    eye = lax.broadcasted_iota(jnp.int32, (2 * W, T), 0) == lax.broadcasted_iota(jnp.int32, (2 * W, T), 1)

    def sum_of(v, axis):
        return jnp.sum(v, axis=axis, keepdims=True)

    def only_in(v):
        return jnp.where(is_in, v, 0.0)

    def only_out(v):
        return jnp.where(is_in, 0.0, v)

    def to_row(col):
        return sum_of(jnp.where(eye, col, 0.0), 0)

    def to_col(row):
        return sum_of(jnp.where(eye, row, 0.0), 1)

    def spread(slots, me, devs):
        ss, rs = next(sends), next(recvs)
        for dev in devs:
            remote(slots.at[me], slots.at[me], dev, ss, rs)
        return slots.at[pl.ds(0, len(devs))], ss, rs

    g = gb[...]
    sq = g * g + 1e-30
    fv[p] = sum_of(sq, 0)
    fv_ref, fv_send, fv_recv = spread(fv, p, plane)
    for row, col in enumerate((only_in(sq), only_out(sq))):
        rv[line_me, row:row + 1, :] = to_row(sum_of(col, 1))
    for row, ref in ((2, r_in), (3, c_out)):
        rowpad[...] = jnp.zeros_like(rowpad)
        rowpad[ROWS_ONE, :W] = ref[...]
        rv[line_me, row:row + 1, :] = jnp.where(on_first, rowpad[...], pltpu.roll(rowpad[...], W, 1))[:1]
    rv[line_me, RING:, :] = jnp.zeros((RING, T), F32)
    rv_ref, rv_send, rv_recv = spread(rv, line_me, line)

    lr, wd, beta = lr_ref[0], wd_ref[0], beta_ref[0]
    wait(rv_ref, recv.at[rv_recv])
    row_sum = jnp.sum(rv[...], axis=0)
    row_old = rv[0] + rv[1]
    r_new = beta * row_old[2:3] + (1.0 - beta) * (row_sum[:1] / N_IN)
    c_new = beta * row_old[3:4] + (1.0 - beta) * (row_sum[1:2] / N_OUT)
    v = g * jnp.where(is_in, 1.0 / jnp.sqrt(to_col(r_new)), 1.0 / jnp.sqrt(to_col(c_new)))
    sum_rows = sum_of(r_new, 1)
    wait(fv_ref, recv.at[fv_recv])
    f_new = beta * fo[...] + (1.0 - beta) * (jnp.sum(fv[...], axis=0) / D)
    u = v * (1.0 / jnp.sqrt(f_new))
    uu = u * u
    f_out = sum_of(only_out(f_new), 1)

    def total(v):
        return jnp.broadcast_to(sum_of(sum_of(v, 0), 1), (1, T))

    qa[line_me] = jnp.concatenate([total(only_in(uu)), total(only_out(uu)), jnp.broadcast_to(f_out, (6, T))], axis=0)
    qa_ref, qa_send, qa_recv = spread(qa, line_me, line)
    gb[...] = u
    fnew[...] = f_new
    f_send, f_recv = next(sends), next(recvs)
    remote(fnew, frecv, partner, f_send, f_recv)
    wait(qa_ref, recv.at[qa_recv])
    line_sum = jnp.sum(qa[...], axis=0)
    qb[p] = jnp.concatenate([line_sum[:2], jnp.broadcast_to(sum_rows, (6, T))], axis=0)
    qb_ref, qb_send, qb_recv = spread(qb, p, plane)
    wait(mx.at[0], recv.at[m_recv])
    wait(qb_ref, recv.at[qb_recv])
    plane_sum = jnp.sum(qb[...], axis=0)[:, :1]
    mean_in = plane_sum[2:3] / D
    mean_out = line_sum[2:3, :1] / N_OUT
    rms_in = jnp.sqrt(plane_sum[:1] * mean_in / (D * N_IN))
    rms_out = jnp.sqrt(plane_sum[1:2] * mean_out / (D * N_OUT))
    scale = jnp.where(is_in, jnp.sqrt(mean_in) / jnp.maximum(1.0, rms_in), jnp.sqrt(mean_out) / jnp.maximum(1.0, rms_out))

    for a in range(2):
        t2buf[z, y, a] = (0.9 * mx[a] + 0.1 * (gb[W * a:W * a + W] * scale)).astype(BF16).astype(F32)

    send_3, send_4 = next(sends), next(sends)
    first_sem, rest_sem, first2_sem, rest2_sem = ([next(recvs) for _ in GATHER_SEGS] for _ in range(4))

    def ag_refs(phase):
        if phase == 1:
            return (lambda a, k, lanes: t2buf.at[k, y, 0, :, lanes] if a == 0 else t2buf.at[z, k, 1, :, lanes]), send_3, first_sem, rest_sem
        return (lambda a, k, lanes: chunk(t2buf, a, k, lanes)), send_4, first2_sem, rest2_sem

    def ag_begin(s, phase):
        la, lb, _ = lanes_of(GATHER_SEGS[s])
        ref, ss, fs, rs = ag_refs(phase)
        for lanes_r, lanes_l, sem in ((la, lb, fs[s]), (lb, la, rs[s])):
            for a in range(2):
                i, right, left, r, l, f = rs_ring(a, 3 - phase)
                remote(ref(a, i, lanes_r), ref(a, i, lanes_r), right, ss, sem)
                remote(ref(a, i, lanes_l), ref(a, i, lanes_l), left, ss, sem)

    def ag_middle(s, phase):
        la, lb, full = lanes_of(GATHER_SEGS[s])
        ref, ss, fs, rs = ag_refs(phase)
        wait((far2.at[:, :, full] if phase == 1 else far.at[:, :, :, full]), recv.at[fs[s]])
        for a in range(2):
            i, right, left, r, l, f = rs_ring(a, 3 - phase)
            remote(ref(a, l, la), ref(a, l, la), right, ss, rs[s])
            remote(ref(a, r, lb), ref(a, r, lb), left, ss, rs[s])

    def ag_end(s, phase):
        full = lanes_of(GATHER_SEGS[s])[-1]
        wait((dc2.at[:, :, :, full] if phase == 1 else dc.at[:, :, :, :, full]), recv.at[ag_refs(phase)[-1][s]])

    lr_wd = lr * wd
    base = core * HALF

    def transpose_out(j, _):
        rows = pl.ds(pl.multiple_of(j * T, T), T)
        dest = pl.ds(pl.multiple_of(base + j * T, T), T)
        for h in range(2):
            cols = pl.ds(h * D // 2, D // 2)
            t = jnp.concatenate([t2buf[2 * h + zz, yy, a, :, rows] for zz, yy, a in blocks], axis=0)
            w = wown[rows, cols]
            o_w[dest, cols] = w - lr * t.T - lr_wd * w
        return 0

    mo_send, mo_recv = next(sends), next(recvs)
    out_send, out_recv = next(sends), next(recvs)

    def state_out():
        remote(t2buf.at[z, y, 1 - core], mrecv, partner, mo_send, mo_recv)
        wait(frecv, recv.at[f_recv])
        wait(mrecv, recv.at[mo_recv])
        for mine, theirs, out_in, out_out in ((t2buf[z, y, core], mrecv[...], o_m_in, o_m_out), (fnew[...], frecv[...], o_c_in, o_r_out)):
            lo = jnp.where(on_first, mine, theirs)
            hi = jnp.where(on_first, theirs, mine)
            out_in[:, :HALF] = lo.astype(out_in.dtype)
            out_out[...] = hi[:, :F_OUT].astype(out_out.dtype)
            out_in[:, HALF:] = pltpu.roll(hi[:, HALF - 2 * T:], TAIL, 1)[:, :TAIL].astype(out_in.dtype)
        for new, out in ((r_new, o_r_in), (c_new, o_c_out)):
            rowpad[...] = jnp.broadcast_to(new, rowpad.shape)
            out[...] = jnp.where(on_first, rowpad[...], pltpu.roll(rowpad[...], T - W, 1))[:1, :W]
        wait(wown, load_sem.at[w_load])

    def finish(s):
        ag_end(s, 2)
        t0, n, _ = GATHER_SEGS[s]
        lax.fori_loop(t0, t0 + n, transpose_out, 0)
        span = pl.ds(pl.multiple_of(base + t0 * T, T), n * T)
        remote(o_w.at[span], o_w.at[span], partner, out_send, out_recv)

    n_segs = len(GATHER_SEGS)
    for t in range(n_segs + RING):
        if t < n_segs:
            ag_begin(t, 1)
        if t == 3:
            state_out()
        for lag, work in enumerate((lambda s: ag_middle(s, 1), lambda s: (ag_end(s, 1), ag_begin(s, 2)), lambda s: ag_middle(s, 2), finish)):
            s = t - 1 - lag
            if 0 <= s < n_segs:
                work(s)

    wait(xown, recv.at[out_recv])
    for ref, sem in ((xown, swap_send), (ms, m_send), (tbuf.at[:3], send_1), (tbuf.at[0, :3], send_2), (fv_ref, fv_send), (rv_ref, rv_send), (qa_ref, qa_send), (qb_ref, qb_send),
                     (fnew, f_send), (t2buf.at[0, :3], send_3), (t2buf.at[:3], send_4), (ms, mo_send), (xown, out_send)):
        wait(ref, send.at[sem])


def store_kernel(w, m_in, m_out, r_in, c_in, r_out, c_out, o_w_in, o_w_out, o_m_in, o_m_out, o_r_in, o_c_in, o_r_out, o_c_out, sem):
    pairs = [(w.at[pl.ds(0, HALF)], o_w_in.at[pl.ds(0, HALF)]), (w.at[pl.ds(HALF, F_OUT)], o_w_out), (w.at[pl.ds(HALF + F_OUT, TAIL)], o_w_in.at[pl.ds(HALF, TAIL)]),
             (m_in, o_m_in), (m_out, o_m_out), (r_in, o_r_in), (c_in, o_c_in), (r_out, o_r_out), (c_out, o_c_out)]
    work = [pltpu.make_async_copy(src, dst, sem.at[n]) for n, (src, dst) in enumerate(pairs)]
    for c in work:
        c.start()
    for c in work:
        c.wait()


def call(*args):
    vmem = pl.BlockSpec(memory_space=pltpu.VMEM)
    hbm = pl.BlockSpec(memory_space=pltpu.HBM)
    smem = pl.BlockSpec(memory_space=pltpu.SMEM)
    small = (((W, F_IN), BF16), ((W, F_OUT), BF16), ((1, W), F32), ((1, F_IN), F32), ((1, F_OUT), F32), ((1, W), F32))
    in_vmem = [pltpu.VMEM(*a) for a in small]
    args = args[:3] + tuple(pltpu.with_memory_space_constraint(a, pltpu.HBM) for a in args[3:])

    def buf(*shape):
        return pltpu.VMEM(shape, F32)

    half, whole, part, line = (HALF, D), (RING, RING, 2, W, HALF), (W, HALF), (1, HALF)
    held = pl.pallas_call(
        kernel,
        name="adafactor_step",
        out_shape=(buf(2 * HALF, D), *in_vmem),
        in_specs=[smem] * 3 + [hbm] * (len(args) - 3),
        out_specs=(vmem,) * (1 + len(small)),
        scratch_shapes=[
            *in_vmem, buf(*half), buf(*half), buf(*half), buf(*whole), buf(*whole),
            buf(2, RING, *part), buf(2, 2, RING, *part), buf(2, RING, *part), buf(2, *part), buf(2, 2, *part),
            buf(2, *part), buf(*part), buf(*part), buf(*line), buf(*line), buf(*line),
            buf(16, *line), buf(8, 8, T), buf(8, 8, T), buf(16, 8, T),
            buf(2 * W, HALF), buf(W, T), buf(W, 2 * T), buf(1, T), buf(1, 2 * T), buf(8, T),
            pltpu.SemaphoreType.DMA((N_LOAD,)), pltpu.SemaphoreType.DMA((N_SEND,)), pltpu.SemaphoreType.DMA((N_RECV,)),
        ],
        compiler_params=pltpu.CompilerParams(collective_id=0, has_side_effects=True, vmem_limit_bytes=40 << 20),
    )(*args)
    return pl.pallas_call(
        store_kernel,
        name="store_outputs",
        out_shape=tuple(jax.ShapeDtypeStruct(*a) for a in (((F_IN, D), F32), ((F_OUT, D), F32), *small)),
        in_specs=[vmem] * (1 + len(small)),
        out_specs=(hbm,) * (2 + len(small)),
        scratch_shapes=[pltpu.SemaphoreType.DMA((9,))],
        compiler_params=pltpu.CompilerParams(vmem_limit_bytes=16 << 20),
    )(*held)


def solution(mesh):
    def body(w_in, w_out, g_in, g_out, m_in, m_out, r_in, c_in, r_out, c_out, learn_rate, weight_decay, beta_two):
        outs = call(learn_rate[None], weight_decay[None], beta_two[None], g_in[0, 0].T, g_out[0, 0], w_in[0].T, w_out[0], m_in[0], m_out[0].T, r_in, c_in, r_out, c_out)
        return (outs[0].T[None], outs[1][None], outs[2][None], outs[3].T[None], *outs[4:])

    rows, cols, f_last, f_mid = P(None, 'dp'), P(None, 'tp'), P(None, None, 'tp'), P(None, 'tp', None)
    m_specs = (P(None, 'dp', 'tp'), P(None, 'tp', 'dp'))
    stats = (rows, cols, cols, rows)
    in_specs = (f_last, f_mid, P('dp', None, None, 'tp'), P('dp', None, 'tp', None), *m_specs, *stats, P(), P(), P())
    return jax.shard_map(body, mesh=mesh, in_specs=in_specs, out_specs=(f_last, f_mid, *m_specs, *stats), check_vma=False)
```

```python
import jax
import jax.numpy as jnp
from jax import lax
from jax.experimental import pallas as pl
from jax.experimental.pallas import tpu as pltpu
from jax.sharding import PartitionSpec as P

MESH = pl.DeviceIdType.MESH
F32 = jnp.float32
BF16 = jnp.bfloat16
ALL = slice(None)

D = 768
F_IN = 1344
F_OUT = 960
HALF = 1152
TAIL = 192
N_IN = 5376
N_OUT = 3840
T = 128
W = 24
RING = 4
REDUCE_SEGS = ((0, 2, 1), (2, 2, 1), (4, 5, 2))
GATHER_SEGS = ((0, 3, 2), (3, 4, 2), (7, 2, 1))
REDUCE_UNITS = ((None,), (None,), (2, 1, 3, 0))
BLOCKS = (0, 1, 3, 2)
GATHER_UNITS = (((0,), (1, 3), (2,)), ((0,), (1, 3), (2,)), (None,))
RELAY_LAST = (True, False, False)
REDUCE_PLAN = ("S0,B00,S1,B10,M00,S2,B20,B21,B22,B23,H0,M10,E00", "M20,M21,M22,M23,E10,C0,E20,E21,E22,E23,F1,F0,F2")
GATHER_PLAN = ("A0,B00,A1,A2,M0,N0,B01,P00,M1,N1,M2,N2,W0,B02,B10,B11", "P01,W1,W2,B12,P02,P10,B20,P11,P12,F0,P20,F1,F2")
ROWS_ONE = pl.ds(0, 1)
N_SEND = 11
N_RECV = 45
N_LOAD = 10


def spans(half, lo, hi):
    if half == 0:
        return [(0, lo, lo, hi - lo)]
    out = []
    if lo < F_OUT:
        out.append((1, lo, lo, min(hi, F_OUT) - lo))
    if hi > F_OUT:
        start = max(lo, F_OUT)
        out.append((0, start + TAIL, start, hi - start))
    return out


def join_tail(out_val, tail_val, pad_a, pad_b):
    pad_a[...] = jnp.zeros_like(pad_a)
    pad_b[...] = jnp.zeros_like(pad_b)
    cut = F_OUT - F_OUT % T
    pad_a[:, :F_OUT - cut] = out_val[:, cut:]
    pad_b[:, :TAIL] = tail_val
    moved = pltpu.roll(pad_b[...], F_OUT - cut, 1)
    lane = lax.broadcasted_iota(jnp.int32, pad_a.shape, 1)
    mid = jnp.where(lane < F_OUT - cut, pad_a[...], moved[:, :T])
    return jnp.concatenate([out_val[:, :cut], mid, moved[:, T:]], axis=1)


def kernel(lr_ref, wd_ref, beta_ref, g_in, g_out, w_in, w_out, h_m_in, h_m_out, h_r_in, h_c_in, h_r_out, h_c_out,
           o_w, o_m_in, o_m_out, o_r_in, o_c_in, o_r_out, o_c_out,
           m_in, m_out, r_in, c_in, r_out, c_out,
           xown, xrecv, wown, tbuf, t2buf, far, dc, pbuf, far2, dc2,
           mx, ms, mrecv, fo, fnew, frecv, fv, rv, qs, gb, pad_a, pad_b, pad_c, pad_d, rowpad,
           load_sem, send, recv):
    x = lax.axis_index("tp")
    d = lax.axis_index("dp")
    core = lax.rem(d, 2)
    p = lax.div(d, 2)
    y = lax.rem(p, RING)
    z = lax.div(p, RING)
    on_first = core == 0
    line_me = x * 2 + core

    def at(xx, pp, cc):
        return (xx, pp * 2 + cc)

    def step(i, k):
        return lax.rem(i + k, RING)

    partner = at(x, p, 1 - core)
    sends = iter(range(N_SEND))
    recvs = iter(range(N_RECV))
    loads = iter(range(N_LOAD))

    def remote(src, dst, dev, s, r):
        c = pltpu.make_async_remote_copy(src_ref=src, dst_ref=dst, send_sem=send.at[s], recv_sem=recv.at[r], device_id=dev, device_id_type=MESH)
        c.start()

    def wait(ref, sem):
        pltpu.make_async_copy(ref, ref, sem).wait()

    x_load = [next(loads) for _ in REDUCE_SEGS]
    w_load = next(loads)
    for me in range(2):
        @pl.when(core == me)
        def _():
            for (t0, n, _), sem in zip(REDUCE_SEGS, x_load):
                for which, lo, to, rows in spans(me, t0 * T, (t0 + n) * T):
                    pltpu.make_async_copy((g_in, g_out)[which].at[pl.ds(lo, rows)], xown.at[pl.ds(to, rows)], load_sem.at[sem]).start()
            for which, lo, to, rows in spans(me, 0, HALF):
                pltpu.make_async_copy((w_in, w_out)[which].at[pl.ds(lo, rows)], wown.at[pl.ds(to, rows)], load_sem.at[w_load]).start()
    small = [pltpu.make_async_copy(src, dst, load_sem.at[next(loads)]) for src, dst in (
        (h_m_in, m_in), (h_m_out, m_out), (h_r_in, r_in), (h_c_in, c_in), (h_r_out, r_out), (h_c_out, c_out))]
    for c in small:
        c.start()

    barrier = pltpu.get_barrier_semaphore()
    ring = ((y, *(at(x, z * RING + step(y, k), core) for k in (1, 3, 2))),
            (z, *(at(x, step(z, k) * RING + y, core) for k in (1, 3, 2))))
    line = []
    for k in range(1, 8):
        other = lax.rem(line_me + k, 8)
        line.append(at(lax.div(other, 2), p, lax.rem(other, 2)))
    plane = [at(x, lax.rem(p + k, 16), core) for k in range(1, 16)]
    greet = [dev for _, right, left, _ in ring for dev in (right, left)] + line
    for dev in greet:
        pl.semaphore_signal(barrier, inc=1, device_id=dev, device_id_type=MESH)
    pl.semaphore_wait(barrier, len(greet))

    swap_send = next(sends)
    swap_recv = [next(recvs) for _ in REDUCE_SEGS]
    for me in range(2):
        @pl.when(core == me)
        def _():
            for (t0, n, _), sem in zip(REDUCE_SEGS, swap_recv):
                for which, lo, to, rows in spans(1 - me, t0 * T, (t0 + n) * T):
                    remote((g_in, g_out)[which].at[pl.ds(lo, rows)], xrecv.at[pl.ds(to, rows)], partner, swap_send, sem)

    def lanes_of(seg):
        t0, n, n_a = seg
        return pl.ds(t0 * T, n_a * T), pl.ds((t0 + n_a) * T, (n - n_a) * T), pl.ds(t0 * T, n * T)

    blocks = [(i // 8, i // 2 % RING, i % 2) for i in range(16)]

    def transpose_in(j, _):
        rows = pl.ds(pl.multiple_of(j * T, T), T)
        for h in range(2):
            cols = pl.ds(h * D // 2, D // 2)
            t = (xown[rows, cols] + xrecv[rows, cols]).T
            for i, (zz, yy, a) in enumerate(blocks):
                tbuf[2 * h + zz, yy, a, :, rows] = t[W * i:W * i + W]
        return 0

    cross = (z, y)

    def spot(a, k, q):
        return (q, k, 0) if a == 0 else (k, q, 1)

    def piece(buf, a, k, q, lanes):
        return buf.at[(*spot(a, k, q), ALL, lanes)]

    def ring_of(a):
        i, right, left, _ = ring[a]
        return i, right, left, step(i, 1), step(i, 3), step(i, 2)

    def block(a, off):
        return ALL if off is None else step(cross[a], off)

    send_1, send_2 = next(sends), next(sends)
    far_sem, dc_sem = ([[next(recvs) for _ in u] for u in REDUCE_UNITS] for _ in range(2))
    dc2_sem = [next(recvs) for _ in REDUCE_SEGS]
    far2_sem = [next(recvs) if relay else None for relay in RELAY_LAST]

    def rs_begin(s, u):
        la, lb, _ = lanes_of(REDUCE_SEGS[s])
        off = REDUCE_UNITS[s][u]
        for a in range(2):
            i, right, left, r, l, f = ring_of(a)
            q = block(a, off)
            remote(piece(tbuf, a, f, q, la), far.at[a, q, :, la], right, send_1, far_sem[s][u])
            remote(piece(tbuf, a, f, q, lb), far.at[a, q, :, lb], left, send_1, far_sem[s][u])
        for a in range(2):
            i, right, left, r, l, f = ring_of(a)
            q = block(a, off)
            remote(piece(tbuf, a, r, q, lb), dc.at[0, a, q, :, lb], right, send_1, dc_sem[s][u])
            remote(piece(tbuf, a, l, q, la), dc.at[0, a, q, :, la], left, send_1, dc_sem[s][u])

    def unit_blocks(off):
        return pl.ds(0, RING if off is None else 1)

    def rs_middle(s, u):
        la, lb, full = lanes_of(REDUCE_SEGS[s])
        off = REDUCE_UNITS[s][u]
        wait(far.at[:, unit_blocks(off), :, full], recv.at[far_sem[s][u]])
        for a in range(2):
            i, right, left, r, l, f = ring_of(a)
            q = block(a, off)
            for k, lanes, dev in ((r, la, right), (l, lb, left)):
                tbuf[(*spot(a, k, q), ALL, lanes)] += far[a, q, :, lanes]
                remote(piece(tbuf, a, k, q, lanes), dc.at[1, a, q, :, lanes], dev, send_1, dc_sem[s][u])

    def rs_end(s, u):
        la, lb, full = lanes_of(REDUCE_SEGS[s])
        off = REDUCE_UNITS[s][u]
        wait(dc.at[:, :, unit_blocks(off), :, full], recv.at[dc_sem[s][u]])
        for a in range(2):
            q = block(a, off)
            pbuf[a, q, :, full] = tbuf[(*spot(a, ring_of(a)[0], q), ALL, full)] + dc[0, a, q, :, full] + dc[1, a, q, :, full]
        for a in range(2):
            i, right, left, r, l, f = ring_of(1 - a)
            if RELAY_LAST[s]:
                remote(pbuf.at[a, f, :, la], far2.at[a, :, la], right, send_2, far2_sem[s])
                remote(pbuf.at[a, f, :, lb], far2.at[a, :, lb], left, send_2, far2_sem[s])
                remote(pbuf.at[a, r, :, lb], dc2.at[0, a, :, lb], right, send_2, dc2_sem[s])
                remote(pbuf.at[a, l, :, la], dc2.at[0, a, :, la], left, send_2, dc2_sem[s])
            else:
                for slot, (k, o, dev) in enumerate(((f, 2, ring[1 - a][-1]), (r, 1, right), (l, 3, left))):
                    if off is None or off == o:
                        remote(pbuf.at[a, k, :, full], dc2.at[slot, a, :, full], dev, send_2, dc2_sem[s])

    def rs_cross(s):
        la, lb, full = lanes_of(REDUCE_SEGS[s])
        wait(far2.at[:, :, full], recv.at[far2_sem[s]])
        for a in range(2):
            i, right, left, r, l, f = ring_of(1 - a)
            for k, lanes, dev in ((r, la, right), (l, lb, left)):
                pbuf[a, k, :, lanes] += far2[a, :, lanes]
                remote(pbuf.at[a, k, :, lanes], dc2.at[1, a, :, lanes], dev, send_2, dc2_sem[s])

    def rs_finish(s):
        full = lanes_of(REDUCE_SEGS[s])[-1]
        slots = 2 if RELAY_LAST[s] else 3
        wait(dc2.at[:slots, :, :, full], recv.at[dc2_sem[s]])
        for a in range(2):
            acc = pbuf[a, cross[a], :, full]
            for slot in range(slots):
                acc = acc + dc2[slot, a, :, full]
            gb[W * a:W * a + W, full] = acc

    def rs_load(s):
        t0, n, _ = REDUCE_SEGS[s]
        rows = pl.ds(t0 * T, n * T)
        wait(xown.at[rows], load_sem.at[x_load[s]])
        wait(xown.at[rows], recv.at[swap_recv[s]])
        lax.fori_loop(t0, t0 + n, transpose_in, 0)

    def prepare(_):
        for c in small:
            c.wait()
        first = m_in[:, :HALF].astype(F32)
        second = join_tail(m_out[...].astype(F32), m_in[:, HALF:].astype(F32), pad_a, pad_b)
        mx[core] = jnp.where(on_first, first, second)
        ms[...] = jnp.where(on_first, second, first)
        remote(ms, mx.at[core], partner, m_send, m_recv)
        fo[...] = jnp.where(on_first, c_in[:, :HALF], join_tail(r_out[...], c_in[:, HALF:], pad_c, pad_d))

    m_send, m_recv = next(sends), next(recvs)
    def follow(plan, table):
        for item in ",".join(plan).split(","):
            table[item[0]](*(int(c) for c in item[1:]))

    follow(REDUCE_PLAN, dict(S=rs_load, B=rs_begin, M=rs_middle, E=rs_end, C=rs_cross, F=rs_finish, H=prepare))

    lane = lax.broadcasted_iota(jnp.int32, (1, HALF), 1)
    is_in = lane >= jnp.where(on_first, 0, F_OUT)
    eye = lax.broadcasted_iota(jnp.int32, (2 * W, T), 0) == lax.broadcasted_iota(jnp.int32, (2 * W, T), 1)

    def sum_of(v, axis):
        return jnp.sum(v, axis=axis, keepdims=True)

    def only_in(v):
        return jnp.where(is_in, v, 0.0)

    def only_out(v):
        return jnp.where(is_in, 0.0, v)

    def to_row(col):
        return sum_of(jnp.where(eye, col, 0.0), 0)

    def to_col(row):
        return sum_of(jnp.where(eye, row, 0.0), 1)

    def spread(slots, me, devs):
        ss, rs = next(sends), next(recvs)
        for dev in devs:
            remote(slots.at[me], slots.at[me], dev, ss, rs)
        return slots.at[pl.ds(0, len(devs))], ss, rs

    g = gb[...]
    sq = g * g + 1e-30
    fv[p] = sum_of(sq, 0)
    fv_ref, fv_send, fv_recv = spread(fv, p, plane)
    for row, col in enumerate((only_in(sq), only_out(sq))):
        rv[line_me, row:row + 1, :] = to_row(sum_of(col, 1))
    for row, ref in ((2, r_in), (3, c_out)):
        rowpad[...] = jnp.zeros_like(rowpad)
        rowpad[ROWS_ONE, :W] = ref[...]
        rv[line_me, row:row + 1, :] = jnp.where(on_first, rowpad[...], pltpu.roll(rowpad[...], W, 1))[:1]
    rv[line_me, RING:, :] = jnp.zeros((RING, T), F32)
    rv_ref, rv_send, rv_recv = spread(rv, line_me, line)

    lr, wd, beta = lr_ref[0], wd_ref[0], beta_ref[0]
    wait(rv_ref, recv.at[rv_recv])
    row_sum = jnp.sum(rv[...], axis=0)
    row_old = rv[0] + rv[1]
    r_new = beta * row_old[2:3] + (1.0 - beta) * (row_sum[:1] / N_IN)
    c_new = beta * row_old[3:4] + (1.0 - beta) * (row_sum[1:2] / N_OUT)
    v = g * jnp.where(is_in, 1.0 / jnp.sqrt(to_col(r_new)), 1.0 / jnp.sqrt(to_col(c_new)))
    sum_rows = sum_of(r_new, 1)
    wait(fv_ref, recv.at[fv_recv])
    f_new = beta * fo[...] + (1.0 - beta) * (jnp.sum(fv[...], axis=0) / D)
    u = v * (1.0 / jnp.sqrt(f_new))
    uu = u * u
    f_out = sum_of(only_out(f_new), 1)

    def total(v):
        return jnp.broadcast_to(sum_of(sum_of(v, 0), 1), (1, T))

    pick = lax.broadcasted_iota(jnp.int32, (1, T), 1)
    me_all = x * 32 + d
    share = jnp.where(pick == 0, total(only_in(uu)), jnp.where(pick == 1, total(only_out(uu)), jnp.where(pick == 2, f_out / 16, jnp.where(pick == 3, sum_rows / 8, 0.0))))
    qs[me_all] = share
    q_send, q_recv = next(sends), next(recvs)

    def tell(k, _):
        other = lax.rem(me_all + k, 128)
        remote(qs.at[me_all], qs.at[me_all], (lax.div(other, 32), lax.rem(other, 32)), q_send, q_recv)
        return 0

    lax.fori_loop(1, 128, tell, 0)
    q_ref = qs.at[pl.ds(0, 127)]
    gb[...] = u
    fnew[...] = f_new
    f_send, f_recv = next(sends), next(recvs)
    remote(fnew, frecv, partner, f_send, f_recv)
    wait(mx.at[0], recv.at[m_recv])
    wait(q_ref, recv.at[q_recv])
    totals = jnp.sum(qs[...], axis=0)
    mean_in = totals[:, 3:4] / D
    mean_out = totals[:, 2:3] / N_OUT
    rms_in = jnp.sqrt(totals[:, :1] * mean_in / (D * N_IN))
    rms_out = jnp.sqrt(totals[:, 1:2] * mean_out / (D * N_OUT))
    scale = jnp.where(is_in, jnp.sqrt(mean_in) / jnp.maximum(1.0, rms_in), jnp.sqrt(mean_out) / jnp.maximum(1.0, rms_out))

    for a in range(2):
        t2buf[z, y, a] = (0.9 * mx[a] + 0.1 * (gb[W * a:W * a + W] * scale)).astype(BF16).astype(F32)

    send_3 = next(sends)
    a1_first, a1_rest, a1_fwd, a2_rest = ([next(recvs) for _ in GATHER_SEGS] for _ in range(4))
    a2_first = [[next(recvs) for _ in u] for u in GATHER_UNITS]

    def swap_around(ref, ring_a, s, first, rest):
        la, lb, _ = lanes_of(GATHER_SEGS[s])
        for lanes_r, lanes_l, sem in ((la, lb, first), (lb, la, rest)):
            for a in range(2):
                i, right, left, r, l, f = ring_of(ring_a(a))
                for src in ref(a, i, lanes_r):
                    remote(src, src, right, send_3, sem)
                for src in ref(a, i, lanes_l):
                    remote(src, src, left, send_3, sem)

    def pass_on(ref, ring_a, s, sem):
        la, lb, _ = lanes_of(GATHER_SEGS[s])
        for a in range(2):
            i, right, left, r, l, f = ring_of(ring_a(a))
            for src in ref(a, l, la):
                remote(src, src, right, send_3, sem)
            for src in ref(a, r, lb):
                remote(src, src, left, send_3, sem)

    def one_ref(a, q, lanes):
        return [piece(t2buf, a, ring_of(a)[0], q, lanes)]

    def two_ref(s, u):
        offs = GATHER_UNITS[s][u]
        return lambda a, k, lanes: [piece(t2buf, a, k, block(a, o), lanes) for o in (offs or (None,))]

    def same(a):
        return a

    def other(a):
        return 1 - a

    def a1_begin(s):
        swap_around(one_ref, other, s, a1_first[s], a1_rest[s])

    def a2_begin(s, u):
        swap_around(two_ref(s, u), same, s, a2_first[s][u], a2_rest[s])

    def a1_middle(s):
        wait(far2.at[:, :, lanes_of(GATHER_SEGS[s])[-1]], recv.at[a1_first[s]])
        pass_on(one_ref, other, s, a1_fwd[s])

    def a1_near(s):
        wait(far2.at[:, :, lanes_of(GATHER_SEGS[s])[-1]], recv.at[a1_rest[s]])

    def a1_far(s):
        wait(far2.at[:, :, lanes_of(GATHER_SEGS[s])[-1]], recv.at[a1_fwd[s]])

    def a2_middle(s, u):
        wait(far.at[:, :len(GATHER_UNITS[s][u] or BLOCKS), :, lanes_of(GATHER_SEGS[s])[-1]], recv.at[a2_first[s][u]])
        pass_on(two_ref(s, u), same, s, a2_rest[s])

    def a2_end(s):
        wait(dc.at[:, :, :, :, lanes_of(GATHER_SEGS[s])[-1]], recv.at[a2_rest[s]])

    lr_wd = lr * wd
    base = core * HALF

    def transpose_out(j, _):
        rows = pl.ds(pl.multiple_of(j * T, T), T)
        dest = pl.ds(pl.multiple_of(base + j * T, T), T)
        for h in range(2):
            cols = pl.ds(h * D // 2, D // 2)
            t = jnp.concatenate([t2buf[2 * h + zz, yy, a, :, rows] for zz, yy, a in blocks], axis=0)
            w = wown[rows, cols]
            o_w[dest, cols] = w - lr * t.T - lr_wd * w
        return 0

    mo_send, mo_recv = next(sends), next(recvs)
    out_send, out_recv = next(sends), next(recvs)

    def state_out():
        wait(frecv, recv.at[f_recv])
        wait(mrecv, recv.at[mo_recv])
        for mine, theirs, out_in, out_out in ((t2buf[z, y, core], mrecv[...], o_m_in, o_m_out), (fnew[...], frecv[...], o_c_in, o_r_out)):
            lo = jnp.where(on_first, mine, theirs)
            hi = jnp.where(on_first, theirs, mine)
            out_in[:, :HALF] = lo.astype(out_in.dtype)
            out_out[...] = hi[:, :F_OUT].astype(out_out.dtype)
            out_in[:, HALF:] = pltpu.roll(hi[:, HALF - 2 * T:], TAIL, 1)[:, :TAIL].astype(out_in.dtype)
        for new, out in ((r_new, o_r_in), (c_new, o_c_out)):
            rowpad[...] = jnp.broadcast_to(new, rowpad.shape)
            out[...] = jnp.where(on_first, rowpad[...], pltpu.roll(rowpad[...], T - W, 1))[:1, :W]
        wait(wown, load_sem.at[w_load])

    def finish(s):
        if s == 0:
            state_out()
        a2_end(s)
        t0, n, _ = GATHER_SEGS[s]
        lax.fori_loop(t0, t0 + n, transpose_out, 0)
        span = pl.ds(pl.multiple_of(base + t0 * T, T), n * T)
        remote(o_w.at[span], o_w.at[span], partner, out_send, out_recv)

    remote(t2buf.at[z, y, 1 - core], mrecv, partner, mo_send, mo_recv)
    follow(GATHER_PLAN, dict(A=a1_begin, B=a2_begin, M=a1_middle, N=a1_near, W=a1_far, P=a2_middle, F=finish))

    wait(xown, recv.at[out_recv])
    for ref, sem in ((xown, swap_send), (ms, m_send), (tbuf.at[:3], send_1), (tbuf.at[0, :3], send_2), (fv_ref, fv_send), (rv_ref, rv_send), (q_ref, q_send),
                     (fnew, f_send), (xown.at[pl.ds(0, HALF - HALF // 16)], send_3), (ms, mo_send), (xown, out_send)):
        wait(ref, send.at[sem])


def store_kernel(w, m_in, m_out, r_in, c_in, r_out, c_out, o_w_in, o_w_out, o_m_in, o_m_out, o_r_in, o_c_in, o_r_out, o_c_out, sem):
    pairs = [(w.at[pl.ds(0, HALF)], o_w_in.at[pl.ds(0, HALF)]), (w.at[pl.ds(HALF, F_OUT)], o_w_out), (w.at[pl.ds(HALF + F_OUT, TAIL)], o_w_in.at[pl.ds(HALF, TAIL)]),
             (m_in, o_m_in), (m_out, o_m_out), (r_in, o_r_in), (c_in, o_c_in), (r_out, o_r_out), (c_out, o_c_out)]
    work = [pltpu.make_async_copy(src, dst, sem.at[n]) for n, (src, dst) in enumerate(pairs)]
    for c in work:
        c.start()
    for c in work:
        c.wait()


def call(*args):
    vmem = pl.BlockSpec(memory_space=pltpu.VMEM)
    hbm = pl.BlockSpec(memory_space=pltpu.HBM)
    smem = pl.BlockSpec(memory_space=pltpu.SMEM)
    small = (((W, F_IN), BF16), ((W, F_OUT), BF16), ((1, W), F32), ((1, F_IN), F32), ((1, F_OUT), F32), ((1, W), F32))
    in_vmem = [pltpu.VMEM(*a) for a in small]
    args = args[:3] + tuple(pltpu.with_memory_space_constraint(a, pltpu.HBM) for a in args[3:])

    def buf(*shape):
        return pltpu.VMEM(shape, F32)

    half, whole, part, line = (HALF, D), (RING, RING, 2, W, HALF), (W, HALF), (1, HALF)
    held = pl.pallas_call(
        kernel,
        name="adafactor_step",
        out_shape=(buf(2 * HALF, D), *in_vmem),
        in_specs=[smem] * 3 + [hbm] * (len(args) - 3),
        out_specs=(vmem,) * (1 + len(small)),
        scratch_shapes=[
            *in_vmem, buf(*half), buf(*half), buf(*half), buf(*whole), buf(*whole),
            buf(2, RING, *part), buf(2, 2, RING, *part), buf(2, RING, *part), buf(2, *part), buf(3, 2, *part),
            buf(2, *part), buf(*part), buf(*part), buf(*line), buf(*line), buf(*line),
            buf(16, *line), buf(8, 8, T), buf(128, 1, T),
            buf(2 * W, HALF), buf(W, T), buf(W, 2 * T), buf(1, T), buf(1, 2 * T), buf(8, T),
            pltpu.SemaphoreType.DMA((N_LOAD,)), pltpu.SemaphoreType.DMA((N_SEND,)), pltpu.SemaphoreType.DMA((N_RECV,)),
        ],
        compiler_params=pltpu.CompilerParams(collective_id=0, has_side_effects=True, vmem_limit_bytes=40 << 20),
    )(*args)
    return pl.pallas_call(
        store_kernel,
        name="store_outputs",
        out_shape=tuple(jax.ShapeDtypeStruct(*a) for a in (((F_IN, D), F32), ((F_OUT, D), F32), *small)),
        in_specs=[vmem] * (1 + len(small)),
        out_specs=(hbm,) * (2 + len(small)),
        scratch_shapes=[pltpu.SemaphoreType.DMA((9,))],
        compiler_params=pltpu.CompilerParams(vmem_limit_bytes=16 << 20),
    )(*held)


def solution(mesh):
    def body(w_in, w_out, g_in, g_out, m_in, m_out, r_in, c_in, r_out, c_out, learn_rate, weight_decay, beta_two):
        outs = call(learn_rate[None], weight_decay[None], beta_two[None], g_in[0, 0].T, g_out[0, 0], w_in[0].T, w_out[0], m_in[0], m_out[0].T, r_in, c_in, r_out, c_out)
        return (outs[0].T[None], outs[1][None], outs[2][None], outs[3].T[None], *outs[4:])

    rows, cols, f_last, f_mid = P(None, 'dp'), P(None, 'tp'), P(None, None, 'tp'), P(None, 'tp', None)
    m_specs = (P(None, 'dp', 'tp'), P(None, 'tp', 'dp'))
    stats = (rows, cols, cols, rows)
    in_specs = (f_last, f_mid, P('dp', None, None, 'tp'), P('dp', None, 'tp', None), *m_specs, *stats, P(), P(), P())
    return jax.shard_map(body, mesh=mesh, in_specs=in_specs, out_specs=(f_last, f_mid, *m_specs, *stats), check_vma=False)
```

```python
import jax
import jax.numpy as jnp
from jax import lax
from jax.experimental import pallas as pl
from jax.experimental.pallas import tpu as pltpu
from jax.sharding import PartitionSpec as P

MESH = pl.DeviceIdType.MESH
F32 = jnp.float32
BF16 = jnp.bfloat16
ALL = slice(None)

D = 768
F_IN = 1344
F_OUT = 960
HALF = 1152
TAIL = 192
N_IN = 5376
N_OUT = 3840
T = 128
W = 24
RING = 4
REDUCE_SEGS = ((0, 2, 1), (2, 2, 1), (4, 5, 2))
GATHER_SEGS = ((0, 3, 2), (3, 4, 2), (7, 2, 1))
REDUCE_UNITS = ((None,), (None,), (2, 1, 3, 0))
BLOCKS = (0, 1, 3, 2)
GATHER_UNITS = (((0,), (1, 3), (2,)), ((0,), (1, 3), (2,)), (None,))
RELAY_LAST = (True, False, False)
REDUCE_PLAN = ("S0,B00,S1,B10,M00,S2,B20,B21,B22,B23,H0,M10,E00", "M20,M21,M22,M23,E10,C0,E20,E21,E22,E23,F1,F0,F2")
GATHER_PLAN = ("A0,B00,A1,A2,M0,N0,B01,P00,M1,N1,M2,N2,W0,B02,B10,B11", "P01,W1,W2,B12,P02,P10,B20,P11,P12,F0,P20,F1,F2")
FAR_FIRST = (2, 1, 3, 0)
ROWS_ONE = pl.ds(0, 1)
N_SEND = 11
N_RECV = 45
N_LOAD = 10


def spans(half, lo, hi):
    if half == 0:
        return [(0, lo, lo, hi - lo)]
    out = []
    if lo < F_OUT:
        out.append((1, lo, lo, min(hi, F_OUT) - lo))
    if hi > F_OUT:
        start = max(lo, F_OUT)
        out.append((0, start + TAIL, start, hi - start))
    return out


def join_tail(out_val, tail_val, pad_a, pad_b):
    pad_a[...] = jnp.zeros_like(pad_a)
    pad_b[...] = jnp.zeros_like(pad_b)
    cut = F_OUT - F_OUT % T
    pad_a[:, :F_OUT - cut] = out_val[:, cut:]
    pad_b[:, :TAIL] = tail_val
    moved = pltpu.roll(pad_b[...], F_OUT - cut, 1)
    lane = lax.broadcasted_iota(jnp.int32, pad_a.shape, 1)
    mid = jnp.where(lane < F_OUT - cut, pad_a[...], moved[:, :T])
    return jnp.concatenate([out_val[:, :cut], mid, moved[:, T:]], axis=1)


def kernel(lr_ref, wd_ref, beta_ref, g_in, g_out, w_in, w_out, h_m_in, h_m_out, h_r_in, h_c_in, h_r_out, h_c_out,
           o_w, o_m_in, o_m_out, o_r_in, o_c_in, o_r_out, o_c_out,
           m_in, m_out, r_in, c_in, r_out, c_out,
           xown, xrecv, wown, tbuf, t2buf, far, dc, pbuf, far2, dc2,
           mx, ms, mrecv, fo, fnew, frecv, fv, rv, qs, gb, pad_a, pad_b, pad_c, pad_d, rowpad,
           load_sem, send, recv):
    x = lax.axis_index("tp")
    d = lax.axis_index("dp")
    core = lax.rem(d, 2)
    p = lax.div(d, 2)
    y = lax.rem(p, RING)
    z = lax.div(p, RING)
    on_first = core == 0
    line_me = x * 2 + core

    def at(xx, pp, cc):
        return (xx, pp * 2 + cc)

    turn = 1 + 2 * core

    def step(i, k):
        return lax.rem(i + k * turn, RING)

    partner = at(x, p, 1 - core)
    sends = iter(range(N_SEND))
    recvs = iter(range(N_RECV))
    loads = iter(range(N_LOAD))

    def remote(src, dst, dev, s, r):
        c = pltpu.make_async_remote_copy(src_ref=src, dst_ref=dst, send_sem=send.at[s], recv_sem=recv.at[r], device_id=dev, device_id_type=MESH)
        c.start()

    def wait(ref, sem):
        pltpu.make_async_copy(ref, ref, sem).wait()

    x_load = [next(loads) for _ in REDUCE_SEGS]
    w_load = next(loads)
    for me in range(2):
        @pl.when(core == me)
        def _():
            for (t0, n, _), sem in zip(REDUCE_SEGS, x_load):
                for which, lo, to, rows in spans(me, t0 * T, (t0 + n) * T):
                    pltpu.make_async_copy((g_in, g_out)[which].at[pl.ds(lo, rows)], xown.at[pl.ds(to, rows)], load_sem.at[sem]).start()
            for which, lo, to, rows in spans(me, 0, HALF):
                pltpu.make_async_copy((w_in, w_out)[which].at[pl.ds(lo, rows)], wown.at[pl.ds(to, rows)], load_sem.at[w_load]).start()
    small = [pltpu.make_async_copy(src, dst, load_sem.at[next(loads)]) for src, dst in (
        (h_m_in, m_in), (h_m_out, m_out), (h_r_in, r_in), (h_c_in, c_in), (h_r_out, r_out), (h_c_out, c_out))]
    for c in small:
        c.start()

    barrier = pltpu.get_barrier_semaphore()
    ring = ((y, *(at(x, z * RING + step(y, k), core) for k in (1, 3, 2))),
            (z, *(at(x, step(z, k) * RING + y, core) for k in (1, 3, 2))))
    line = []
    for k in range(1, 8):
        other = lax.rem(line_me + k, 8)
        line.append(at(lax.div(other, 2), p, lax.rem(other, 2)))
    plane = [at(x, step(z, i) * RING + step(y, k), core) for i in FAR_FIRST for k in FAR_FIRST if i or k]
    greet = [dev for _, right, left, _ in ring for dev in (right, left)] + line
    for dev in greet:
        pl.semaphore_signal(barrier, inc=1, device_id=dev, device_id_type=MESH)
    pl.semaphore_wait(barrier, len(greet))

    swap_send = next(sends)
    swap_recv = [next(recvs) for _ in REDUCE_SEGS]
    for me in range(2):
        @pl.when(core == me)
        def _():
            for (t0, n, _), sem in zip(REDUCE_SEGS, swap_recv):
                for which, lo, to, rows in spans(1 - me, t0 * T, (t0 + n) * T):
                    remote((g_in, g_out)[which].at[pl.ds(lo, rows)], xrecv.at[pl.ds(to, rows)], partner, swap_send, sem)

    def lanes_of(seg):
        t0, n, n_a = seg
        return pl.ds(t0 * T, n_a * T), pl.ds((t0 + n_a) * T, (n - n_a) * T), pl.ds(t0 * T, n * T)

    blocks = [(i // 8, i // 2 % RING, i % 2) for i in range(16)]

    def transpose_in(j, _):
        rows = pl.ds(pl.multiple_of(j * T, T), T)
        for h in range(2):
            cols = pl.ds(h * D // 2, D // 2)
            t = (xown[rows, cols] + xrecv[rows, cols]).T
            for i, (zz, yy, a) in enumerate(blocks):
                tbuf[2 * h + zz, yy, a, :, rows] = t[W * i:W * i + W]
        return 0

    cross = (z, y)

    def spot(a, k, q):
        return (q, k, 0) if a == 0 else (k, q, 1)

    def piece(buf, a, k, q, lanes):
        return buf.at[(*spot(a, k, q), ALL, lanes)]

    def ring_of(a):
        i, right, left, _ = ring[a]
        return i, right, left, step(i, 1), step(i, 3), step(i, 2)

    def block(a, off):
        return ALL if off is None else step(cross[a], off)

    send_1, send_2 = next(sends), next(sends)
    far_sem, dc_sem = ([[next(recvs) for _ in u] for u in REDUCE_UNITS] for _ in range(2))
    dc2_sem = [next(recvs) for _ in REDUCE_SEGS]
    far2_sem = [next(recvs) if relay else None for relay in RELAY_LAST]

    def rs_begin(s, u):
        la, lb, _ = lanes_of(REDUCE_SEGS[s])
        off = REDUCE_UNITS[s][u]
        for a in range(2):
            i, right, left, r, l, f = ring_of(a)
            q = block(a, off)
            remote(piece(tbuf, a, f, q, la), far.at[a, q, :, la], right, send_1, far_sem[s][u])
            remote(piece(tbuf, a, f, q, lb), far.at[a, q, :, lb], left, send_1, far_sem[s][u])
        for a in range(2):
            i, right, left, r, l, f = ring_of(a)
            q = block(a, off)
            remote(piece(tbuf, a, r, q, lb), dc.at[0, a, q, :, lb], right, send_1, dc_sem[s][u])
            remote(piece(tbuf, a, l, q, la), dc.at[0, a, q, :, la], left, send_1, dc_sem[s][u])

    def unit_blocks(off):
        return pl.ds(0, RING if off is None else 1)

    def rs_middle(s, u):
        la, lb, full = lanes_of(REDUCE_SEGS[s])
        off = REDUCE_UNITS[s][u]
        wait(far.at[:, unit_blocks(off), :, full], recv.at[far_sem[s][u]])
        for a in range(2):
            i, right, left, r, l, f = ring_of(a)
            q = block(a, off)
            for k, lanes, dev in ((r, la, right), (l, lb, left)):
                tbuf[(*spot(a, k, q), ALL, lanes)] += far[a, q, :, lanes]
                remote(piece(tbuf, a, k, q, lanes), dc.at[1, a, q, :, lanes], dev, send_1, dc_sem[s][u])

    def rs_end(s, u):
        la, lb, full = lanes_of(REDUCE_SEGS[s])
        off = REDUCE_UNITS[s][u]
        wait(dc.at[:, :, unit_blocks(off), :, full], recv.at[dc_sem[s][u]])
        for a in range(2):
            q = block(a, off)
            pbuf[a, q, :, full] = tbuf[(*spot(a, ring_of(a)[0], q), ALL, full)] + dc[0, a, q, :, full] + dc[1, a, q, :, full]
        for a in range(2):
            i, right, left, r, l, f = ring_of(1 - a)
            if RELAY_LAST[s]:
                remote(pbuf.at[a, f, :, la], far2.at[a, :, la], right, send_2, far2_sem[s])
                remote(pbuf.at[a, f, :, lb], far2.at[a, :, lb], left, send_2, far2_sem[s])
                remote(pbuf.at[a, r, :, lb], dc2.at[0, a, :, lb], right, send_2, dc2_sem[s])
                remote(pbuf.at[a, l, :, la], dc2.at[0, a, :, la], left, send_2, dc2_sem[s])
            else:
                for slot, (k, o, dev) in enumerate(((f, 2, ring[1 - a][-1]), (r, 1, right), (l, 3, left))):
                    if off is None or off == o:
                        remote(pbuf.at[a, k, :, full], dc2.at[slot, a, :, full], dev, send_2, dc2_sem[s])

    def rs_cross(s):
        la, lb, full = lanes_of(REDUCE_SEGS[s])
        wait(far2.at[:, :, full], recv.at[far2_sem[s]])
        for a in range(2):
            i, right, left, r, l, f = ring_of(1 - a)
            for k, lanes, dev in ((r, la, right), (l, lb, left)):
                pbuf[a, k, :, lanes] += far2[a, :, lanes]
                remote(pbuf.at[a, k, :, lanes], dc2.at[1, a, :, lanes], dev, send_2, dc2_sem[s])

    def rs_finish(s):
        full = lanes_of(REDUCE_SEGS[s])[-1]
        slots = 2 if RELAY_LAST[s] else 3
        wait(dc2.at[:slots, :, :, full], recv.at[dc2_sem[s]])
        for a in range(2):
            acc = pbuf[a, cross[a], :, full]
            for slot in range(slots):
                acc = acc + dc2[slot, a, :, full]
            gb[W * a:W * a + W, full] = acc

    def rs_load(s):
        t0, n, _ = REDUCE_SEGS[s]
        rows = pl.ds(t0 * T, n * T)
        wait(xown.at[rows], load_sem.at[x_load[s]])
        wait(xown.at[rows], recv.at[swap_recv[s]])
        lax.fori_loop(t0, t0 + n, transpose_in, 0)

    def prepare(_):
        for c in small:
            c.wait()
        first = m_in[:, :HALF].astype(F32)
        second = join_tail(m_out[...].astype(F32), m_in[:, HALF:].astype(F32), pad_a, pad_b)
        mx[core] = jnp.where(on_first, first, second)
        ms[...] = jnp.where(on_first, second, first)
        remote(ms, mx.at[core], partner, m_send, m_recv)
        fo[...] = jnp.where(on_first, c_in[:, :HALF], join_tail(r_out[...], c_in[:, HALF:], pad_c, pad_d))

    m_send, m_recv = next(sends), next(recvs)
    def follow(plan, table):
        for item in ",".join(plan).split(","):
            table[item[0]](*(int(c) for c in item[1:]))

    follow(REDUCE_PLAN, dict(S=rs_load, B=rs_begin, M=rs_middle, E=rs_end, C=rs_cross, F=rs_finish, H=prepare))

    lane = lax.broadcasted_iota(jnp.int32, (1, HALF), 1)
    is_in = lane >= jnp.where(on_first, 0, F_OUT)
    eye = lax.broadcasted_iota(jnp.int32, (2 * W, T), 0) == lax.broadcasted_iota(jnp.int32, (2 * W, T), 1)

    def sum_of(v, axis):
        return jnp.sum(v, axis=axis, keepdims=True)

    def only_in(v):
        return jnp.where(is_in, v, 0.0)

    def only_out(v):
        return jnp.where(is_in, 0.0, v)

    def to_row(col):
        return sum_of(jnp.where(eye, col, 0.0), 0)

    def to_col(row):
        return sum_of(jnp.where(eye, row, 0.0), 1)

    def spread(slots, me, devs):
        ss, rs = next(sends), next(recvs)
        for dev in devs:
            remote(slots.at[me], slots.at[me], dev, ss, rs)
        return slots.at[pl.ds(0, len(devs))], ss, rs

    g = gb[...]
    sq = g * g + 1e-30
    fv[p] = sum_of(sq, 0)
    fv_ref, fv_send, fv_recv = spread(fv, p, plane)
    for row, col in enumerate((only_in(sq), only_out(sq))):
        rv[line_me, row:row + 1, :] = to_row(sum_of(col, 1))
    for row, ref in ((2, r_in), (3, c_out)):
        rowpad[...] = jnp.zeros_like(rowpad)
        rowpad[ROWS_ONE, :W] = ref[...]
        rv[line_me, row:row + 1, :] = jnp.where(on_first, rowpad[...], pltpu.roll(rowpad[...], W, 1))[:1]
    rv[line_me, RING:, :] = jnp.zeros((RING, T), F32)
    rv_ref, rv_send, rv_recv = spread(rv, line_me, line)

    lr, wd, beta = lr_ref[0], wd_ref[0], beta_ref[0]
    wait(rv_ref, recv.at[rv_recv])
    row_sum = jnp.sum(rv[...], axis=0)
    row_old = rv[0] + rv[1]
    r_new = beta * row_old[2:3] + (1.0 - beta) * (row_sum[:1] / N_IN)
    c_new = beta * row_old[3:4] + (1.0 - beta) * (row_sum[1:2] / N_OUT)
    v = g * jnp.where(is_in, 1.0 / jnp.sqrt(to_col(r_new)), 1.0 / jnp.sqrt(to_col(c_new)))
    sum_rows = sum_of(r_new, 1)
    wait(fv_ref, recv.at[fv_recv])
    f_new = beta * fo[...] + (1.0 - beta) * (jnp.sum(fv[...], axis=0) / D)
    u = v * (1.0 / jnp.sqrt(f_new))
    uu = u * u
    f_out = sum_of(only_out(f_new), 1)

    def total(v):
        return jnp.broadcast_to(sum_of(sum_of(v, 0), 1), (1, T))

    pick = lax.broadcasted_iota(jnp.int32, (1, T), 1)
    me_all = x * 32 + d
    share = jnp.where(pick == 0, total(only_in(uu)), jnp.where(pick == 1, total(only_out(uu)), jnp.where(pick == 2, f_out / 16, jnp.where(pick == 3, sum_rows / 8, 0.0))))
    qs[me_all] = share
    q_send, q_recv = next(sends), next(recvs)

    def tell(k, _):
        chip = lax.rem(z + 6 - lax.div(k, RING), RING) * RING + lax.rem(y + 6 - lax.rem(k, RING), RING)
        for i in FAR_FIRST:
            for c in (1 - core, core):
                def go():
                    remote(qs.at[me_all], qs.at[me_all], at(lax.rem(x + i, RING), chip, c), q_send, q_recv)
                if i == 0 and c is core:
                    pl.when(k != 10)(go)
                else:
                    go()
        return 0

    lax.fori_loop(0, 16, tell, 0)
    q_ref = qs.at[pl.ds(0, 127)]
    gb[...] = u
    fnew[...] = f_new
    f_send, f_recv = next(sends), next(recvs)
    remote(fnew, frecv, partner, f_send, f_recv)
    wait(mx.at[0], recv.at[m_recv])
    wait(q_ref, recv.at[q_recv])
    totals = jnp.sum(qs[...], axis=0)
    mean_in = totals[:, 3:4] / D
    mean_out = totals[:, 2:3] / N_OUT
    rms_in = jnp.sqrt(totals[:, :1] * mean_in / (D * N_IN))
    rms_out = jnp.sqrt(totals[:, 1:2] * mean_out / (D * N_OUT))
    scale = jnp.where(is_in, jnp.sqrt(mean_in) / jnp.maximum(1.0, rms_in), jnp.sqrt(mean_out) / jnp.maximum(1.0, rms_out))

    for a in range(2):
        t2buf[z, y, a] = (0.9 * mx[a] + 0.1 * (gb[W * a:W * a + W] * scale)).astype(BF16).astype(F32)

    send_3 = next(sends)
    a1_first, a1_rest, a1_fwd, a2_rest = ([next(recvs) for _ in GATHER_SEGS] for _ in range(4))
    a2_first = [[next(recvs) for _ in u] for u in GATHER_UNITS]

    def swap_around(ref, ring_a, s, first, rest):
        la, lb, _ = lanes_of(GATHER_SEGS[s])
        for lanes_r, lanes_l, sem in ((la, lb, first), (lb, la, rest)):
            for a in range(2):
                i, right, left, r, l, f = ring_of(ring_a(a))
                for src in ref(a, i, lanes_r):
                    remote(src, src, right, send_3, sem)
                for src in ref(a, i, lanes_l):
                    remote(src, src, left, send_3, sem)

    def pass_on(ref, ring_a, s, sem):
        la, lb, _ = lanes_of(GATHER_SEGS[s])
        for a in range(2):
            i, right, left, r, l, f = ring_of(ring_a(a))
            for src in ref(a, l, la):
                remote(src, src, right, send_3, sem)
            for src in ref(a, r, lb):
                remote(src, src, left, send_3, sem)

    def one_ref(a, q, lanes):
        return [piece(t2buf, a, ring_of(a)[0], q, lanes)]

    def two_ref(s, u):
        offs = GATHER_UNITS[s][u]
        return lambda a, k, lanes: [piece(t2buf, a, k, block(a, o), lanes) for o in (offs or (None,))]

    def same(a):
        return a

    def other(a):
        return 1 - a

    def a1_begin(s):
        swap_around(one_ref, other, s, a1_first[s], a1_rest[s])

    def a2_begin(s, u):
        swap_around(two_ref(s, u), same, s, a2_first[s][u], a2_rest[s])

    def a1_middle(s):
        wait(far2.at[:, :, lanes_of(GATHER_SEGS[s])[-1]], recv.at[a1_first[s]])
        pass_on(one_ref, other, s, a1_fwd[s])

    def a1_near(s):
        wait(far2.at[:, :, lanes_of(GATHER_SEGS[s])[-1]], recv.at[a1_rest[s]])

    def a1_far(s):
        wait(far2.at[:, :, lanes_of(GATHER_SEGS[s])[-1]], recv.at[a1_fwd[s]])

    def a2_middle(s, u):
        wait(far.at[:, :len(GATHER_UNITS[s][u] or BLOCKS), :, lanes_of(GATHER_SEGS[s])[-1]], recv.at[a2_first[s][u]])
        pass_on(two_ref(s, u), same, s, a2_rest[s])

    def a2_end(s):
        wait(dc.at[:, :, :, :, lanes_of(GATHER_SEGS[s])[-1]], recv.at[a2_rest[s]])

    lr_wd = lr * wd
    base = core * HALF

    def transpose_out(j, _):
        rows = pl.ds(pl.multiple_of(j * T, T), T)
        dest = pl.ds(pl.multiple_of(base + j * T, T), T)
        for h in range(2):
            cols = pl.ds(h * D // 2, D // 2)
            t = jnp.concatenate([t2buf[2 * h + zz, yy, a, :, rows] for zz, yy, a in blocks], axis=0)
            w = wown[rows, cols]
            o_w[dest, cols] = w - lr * t.T - lr_wd * w
        return 0

    mo_send, mo_recv = next(sends), next(recvs)
    out_send, out_recv = next(sends), next(recvs)

    def state_out():
        wait(frecv, recv.at[f_recv])
        wait(mrecv, recv.at[mo_recv])
        for mine, theirs, out_in, out_out in ((t2buf[z, y, core], mrecv[...], o_m_in, o_m_out), (fnew[...], frecv[...], o_c_in, o_r_out)):
            lo = jnp.where(on_first, mine, theirs)
            hi = jnp.where(on_first, theirs, mine)
            out_in[:, :HALF] = lo.astype(out_in.dtype)
            out_out[...] = hi[:, :F_OUT].astype(out_out.dtype)
            out_in[:, HALF:] = pltpu.roll(hi[:, HALF - 2 * T:], TAIL, 1)[:, :TAIL].astype(out_in.dtype)
        for new, out in ((r_new, o_r_in), (c_new, o_c_out)):
            rowpad[...] = jnp.broadcast_to(new, rowpad.shape)
            out[...] = jnp.where(on_first, rowpad[...], pltpu.roll(rowpad[...], T - W, 1))[:1, :W]
        wait(wown, load_sem.at[w_load])

    def finish(s):
        if s == 0:
            state_out()
        a2_end(s)
        t0, n, _ = GATHER_SEGS[s]

        def tile(j, _):
            transpose_out(j, 0)
            span = pl.ds(pl.multiple_of(base + j * T, T), T)
            remote(o_w.at[span], o_w.at[span], partner, out_send, out_recv)
            return 0

        lax.fori_loop(t0, t0 + n, tile, 0)

    remote(t2buf.at[z, y, 1 - core], mrecv, partner, mo_send, mo_recv)
    follow(GATHER_PLAN, dict(A=a1_begin, B=a2_begin, M=a1_middle, N=a1_near, W=a1_far, P=a2_middle, F=finish))

    wait(xown, recv.at[out_recv])
    for ref, sem in ((xown, swap_send), (ms, m_send), (tbuf.at[:3], send_1), (tbuf.at[0, :3], send_2), (fv_ref, fv_send), (rv_ref, rv_send), (q_ref, q_send),
                     (fnew, f_send), (xown.at[pl.ds(0, HALF - HALF // 16)], send_3), (ms, mo_send), (xown, out_send)):
        wait(ref, send.at[sem])


def store_kernel(w, m_in, m_out, r_in, c_in, r_out, c_out, o_w_in, o_w_out, o_m_in, o_m_out, o_r_in, o_c_in, o_r_out, o_c_out, sem):
    pairs = [(w.at[pl.ds(src + k * rows, rows)], out.at[pl.ds(dst + k * rows, rows)]) for src, out, dst, rows, count in (
        (0, o_w_in, 0, TAIL, 6), (HALF, o_w_out, 0, TAIL, 5), (HALF + F_OUT, o_w_in, HALF, TAIL, 1)) for k in range(count)]
    pairs += [(m_in, o_m_in), (m_out, o_m_out), (r_in, o_r_in), (c_in, o_c_in), (r_out, o_r_out), (c_out, o_c_out)]
    work = [pltpu.make_async_copy(src, dst, sem.at[n]) for n, (src, dst) in enumerate(pairs)]
    for c in work:
        c.start()
    for c in work:
        c.wait()


def call(*args):
    vmem = pl.BlockSpec(memory_space=pltpu.VMEM)
    hbm = pl.BlockSpec(memory_space=pltpu.HBM)
    smem = pl.BlockSpec(memory_space=pltpu.SMEM)
    small = (((W, F_IN), BF16), ((W, F_OUT), BF16), ((1, W), F32), ((1, F_IN), F32), ((1, F_OUT), F32), ((1, W), F32))
    in_vmem = [pltpu.VMEM(*a) for a in small]
    args = args[:3] + tuple(pltpu.with_memory_space_constraint(a, pltpu.HBM) for a in args[3:])

    def buf(*shape):
        return pltpu.VMEM(shape, F32)

    half, whole, part, line = (HALF, D), (RING, RING, 2, W, HALF), (W, HALF), (1, HALF)
    held = pl.pallas_call(
        kernel,
        name="adafactor_step",
        out_shape=(buf(2 * HALF, D), *in_vmem),
        in_specs=[smem] * 3 + [hbm] * (len(args) - 3),
        out_specs=(vmem,) * (1 + len(small)),
        scratch_shapes=[
            *in_vmem, buf(*half), buf(*half), buf(*half), buf(*whole), buf(*whole),
            buf(2, RING, *part), buf(2, 2, RING, *part), buf(2, RING, *part), buf(2, *part), buf(3, 2, *part),
            buf(2, *part), buf(*part), buf(*part), buf(*line), buf(*line), buf(*line),
            buf(16, *line), buf(8, 8, T), buf(128, 1, T),
            buf(2 * W, HALF), buf(W, T), buf(W, 2 * T), buf(1, T), buf(1, 2 * T), buf(8, T),
            pltpu.SemaphoreType.DMA((N_LOAD,)), pltpu.SemaphoreType.DMA((N_SEND,)), pltpu.SemaphoreType.DMA((N_RECV,)),
        ],
        compiler_params=pltpu.CompilerParams(collective_id=0, has_side_effects=True, vmem_limit_bytes=40 << 20),
    )(*args)
    return pl.pallas_call(
        store_kernel,
        name="store_outputs",
        out_shape=tuple(jax.ShapeDtypeStruct(*a) for a in (((F_IN, D), F32), ((F_OUT, D), F32), *small)),
        in_specs=[vmem] * (1 + len(small)),
        out_specs=(hbm,) * (2 + len(small)),
        scratch_shapes=[pltpu.SemaphoreType.DMA((18,))],
        compiler_params=pltpu.CompilerParams(vmem_limit_bytes=16 << 20),
    )(*held)


def solution(mesh):
    def body(w_in, w_out, g_in, g_out, m_in, m_out, r_in, c_in, r_out, c_out, learn_rate, weight_decay, beta_two):
        outs = call(learn_rate[None], weight_decay[None], beta_two[None], g_in[0, 0].T, g_out[0, 0], w_in[0].T, w_out[0], m_in[0], m_out[0].T, r_in, c_in, r_out, c_out)
        return (outs[0].T[None], outs[1][None], outs[2][None], outs[3].T[None], *outs[4:])

    rows, cols, f_last, f_mid = P(None, 'dp'), P(None, 'tp'), P(None, None, 'tp'), P(None, 'tp', None)
    m_specs = (P(None, 'dp', 'tp'), P(None, 'tp', 'dp'))
    stats = (rows, cols, cols, rows)
    in_specs = (f_last, f_mid, P('dp', None, None, 'tp'), P('dp', None, 'tp', None), *m_specs, *stats, P(), P(), P())
    return jax.shard_map(body, mesh=mesh, in_specs=in_specs, out_specs=(f_last, f_mid, *m_specs, *stats), check_vma=False)
```

```python
import jax
import jax.numpy as jnp
from jax import lax
from jax.experimental import pallas as pl
from jax.experimental.pallas import tpu as pltpu
from jax.sharding import PartitionSpec as P

MESH = pl.DeviceIdType.MESH
F32 = jnp.float32
BF16 = jnp.bfloat16
ALL = slice(None)

D = 768
F_IN = 1344
F_OUT = 960
HALF = 1152
TAIL = 192
N_IN = 5376
N_OUT = 3840
T = 128
W = 24
RING = 4
REDUCE_SEGS = ((0, 2, 1), (2, 2, 1), (4, 5, 2))
EARLY = 2
GATHER_SEGS = ((0, 2, 1), (0, 2, 1), (2, 3, 2), (5, 2, 1), (7, 2, 1))
BLOCKS = (0, 1, 3, 2)
SPLIT = ((0,), (1, 3), (2,))
GATHER_UNITS = (SPLIT, SPLIT, SPLIT, SPLIT, (None,))
REDUCE_UNITS = ((None,), (None,), (2, 1, 3, 0))
RELAY_LAST = (True, False, False)
REDUCE_PLAN = ("S0,B00,S1,B10,M00,S2,B20,B21,B22,B23,H0,M10,E00", "M20,M21,M22,M23,E10,C0,E20,E21,K0,E22,E23,a1,b10,F1,F0,F2")
EARLY_PLAN = ("M1,N1,B11,P10,A0,B00,W1,B12,P11",)
EARLY_PLAN_END = ("M0,N0,B01,P00,P12,W0,B02,P01",)
GATHER_PLAN = ("A2,B20,A3,A4,P02,M2,N2,B21,P20,M3,N3,M4,N4,W2,B22,F0", "B30,B31,P21,W3,B32,W4,B40,P22,P30,P31,P32,P40,F2,F3,F4")
FAR_FIRST = (2, 1, 3, 0)
ROWS_ONE = pl.ds(0, 1)
N_SEND = 11
N_RECV = 59
N_LOAD = 10


def spans(half, lo, hi):
    if half == 0:
        return [(0, lo, lo, hi - lo)]
    out = []
    if lo < F_OUT:
        out.append((1, lo, lo, min(hi, F_OUT) - lo))
    if hi > F_OUT:
        start = max(lo, F_OUT)
        out.append((0, start + TAIL, start, hi - start))
    return out


def join_tail(out_val, tail_val, pad_a, pad_b):
    pad_a[...] = jnp.zeros_like(pad_a)
    pad_b[...] = jnp.zeros_like(pad_b)
    cut = F_OUT - F_OUT % T
    pad_a[:, :F_OUT - cut] = out_val[:, cut:]
    pad_b[:, :TAIL] = tail_val
    moved = pltpu.roll(pad_b[...], F_OUT - cut, 1)
    lane = lax.broadcasted_iota(jnp.int32, pad_a.shape, 1)
    mid = jnp.where(lane < F_OUT - cut, pad_a[...], moved[:, :T])
    return jnp.concatenate([out_val[:, :cut], mid, moved[:, T:]], axis=1)


def kernel(lr_ref, wd_ref, beta_ref, g_in, g_out, w_in, w_out, h_m_in, h_m_out, h_r_in, h_c_in, h_r_out, h_c_out,
           o_w, o_m_in, o_m_out, o_r_in, o_c_in, o_r_out, o_c_out,
           m_in, m_out, r_in, c_in, r_out, c_out,
           xown, xrecv, wown, tbuf, t2buf, m2buf, mnew, rf, colv, far, dc, pbuf, far2, dc2,
           mx, ms, mrecv, fo, fnew, frecv, fv, rv, qs, gb, pad_a, pad_b, pad_c, pad_d, rowpad,
           load_sem, send, recv):
    x = lax.axis_index("tp")
    d = lax.axis_index("dp")
    core = lax.rem(d, 2)
    p = lax.div(d, 2)
    y = lax.rem(p, RING)
    z = lax.div(p, RING)
    on_first = core == 0
    line_me = x * 2 + core

    def at(xx, pp, cc):
        return (xx, pp * 2 + cc)

    turn = 1 + 2 * core

    def step(i, k):
        return lax.rem(i + k * turn, RING)

    partner = at(x, p, 1 - core)
    sends = iter(range(N_SEND))
    recvs = iter(range(N_RECV))
    loads = iter(range(N_LOAD))

    def remote(src, dst, dev, s, r):
        c = pltpu.make_async_remote_copy(src_ref=src, dst_ref=dst, send_sem=send.at[s], recv_sem=recv.at[r], device_id=dev, device_id_type=MESH)
        c.start()

    def wait(ref, sem):
        pltpu.make_async_copy(ref, ref, sem).wait()

    x_load = [next(loads) for _ in REDUCE_SEGS]
    w_load = next(loads)
    for me in range(2):
        @pl.when(core == me)
        def _():
            for (t0, n, _), sem in zip(REDUCE_SEGS, x_load):
                for which, lo, to, rows in spans(me, t0 * T, (t0 + n) * T):
                    pltpu.make_async_copy((g_in, g_out)[which].at[pl.ds(lo, rows)], xown.at[pl.ds(to, rows)], load_sem.at[sem]).start()
            for which, lo, to, rows in spans(me, 0, HALF):
                pltpu.make_async_copy((w_in, w_out)[which].at[pl.ds(lo, rows)], wown.at[pl.ds(to, rows)], load_sem.at[w_load]).start()
    small = [pltpu.make_async_copy(src, dst, load_sem.at[next(loads)]) for src, dst in (
        (h_m_in, m_in), (h_m_out, m_out), (h_r_in, r_in), (h_c_in, c_in), (h_r_out, r_out), (h_c_out, c_out))]
    for c in small:
        c.start()

    barrier = pltpu.get_barrier_semaphore()
    ring = ((y, *(at(x, z * RING + step(y, k), core) for k in (1, 3, 2))),
            (z, *(at(x, step(z, k) * RING + y, core) for k in (1, 3, 2))))
    line = []
    for k in range(1, 8):
        other = lax.rem(line_me + k, 8)
        line.append(at(lax.div(other, 2), p, lax.rem(other, 2)))
    plane = [at(x, step(z, i) * RING + step(y, k), core) for i in FAR_FIRST for k in FAR_FIRST if i or k]
    greet = [dev for _, right, left, _ in ring for dev in (right, left)] + line
    for dev in greet:
        pl.semaphore_signal(barrier, inc=1, device_id=dev, device_id_type=MESH)
    pl.semaphore_wait(barrier, len(greet))

    swap_send = next(sends)
    swap_recv = [next(recvs) for _ in REDUCE_SEGS]
    for me in range(2):
        @pl.when(core == me)
        def _():
            for (t0, n, _), sem in zip(REDUCE_SEGS, swap_recv):
                for which, lo, to, rows in spans(1 - me, t0 * T, (t0 + n) * T):
                    remote((g_in, g_out)[which].at[pl.ds(lo, rows)], xrecv.at[pl.ds(to, rows)], partner, swap_send, sem)

    def lanes_of(seg):
        t0, n, n_a = seg
        return pl.ds(t0 * T, n_a * T), pl.ds((t0 + n_a) * T, (n - n_a) * T), pl.ds(t0 * T, n * T)

    blocks = [(i // 8, i // 2 % RING, i % 2) for i in range(16)]

    def transpose_in(j, _):
        rows = pl.ds(pl.multiple_of(j * T, T), T)
        for h in range(2):
            cols = pl.ds(h * D // 2, D // 2)
            t = (xown[rows, cols] + xrecv[rows, cols]).T
            for i, (zz, yy, a) in enumerate(blocks):
                tbuf[2 * h + zz, yy, a, :, rows] = t[W * i:W * i + W]
        return 0

    cross = (z, y)

    def spot(a, k, q):
        return (q, k, 0) if a == 0 else (k, q, 1)

    def piece(buf, a, k, q, lanes):
        return buf.at[(*spot(a, k, q), ALL, lanes)]

    def ring_of(a):
        i, right, left, _ = ring[a]
        return i, right, left, step(i, 1), step(i, 3), step(i, 2)

    def block(a, off):
        return ALL if off is None else step(cross[a], off)

    send_1, send_2 = next(sends), next(sends)
    far_sem, dc_sem = ([[next(recvs) for _ in u] for u in REDUCE_UNITS] for _ in range(2))
    dc2_sem = [next(recvs) for _ in REDUCE_SEGS]
    far2_sem = [next(recvs) if relay else None for relay in RELAY_LAST]

    def rs_begin(s, u):
        la, lb, _ = lanes_of(REDUCE_SEGS[s])
        off = REDUCE_UNITS[s][u]
        for a in range(2):
            i, right, left, r, l, f = ring_of(a)
            q = block(a, off)
            remote(piece(tbuf, a, f, q, la), far.at[a, q, :, la], right, send_1, far_sem[s][u])
            remote(piece(tbuf, a, f, q, lb), far.at[a, q, :, lb], left, send_1, far_sem[s][u])
        for a in range(2):
            i, right, left, r, l, f = ring_of(a)
            q = block(a, off)
            remote(piece(tbuf, a, r, q, lb), dc.at[0, a, q, :, lb], right, send_1, dc_sem[s][u])
            remote(piece(tbuf, a, l, q, la), dc.at[0, a, q, :, la], left, send_1, dc_sem[s][u])

    def unit_blocks(off):
        return pl.ds(0, RING if off is None else 1)

    def rs_middle(s, u):
        la, lb, full = lanes_of(REDUCE_SEGS[s])
        off = REDUCE_UNITS[s][u]
        wait(far.at[:, unit_blocks(off), :, full], recv.at[far_sem[s][u]])
        for a in range(2):
            i, right, left, r, l, f = ring_of(a)
            q = block(a, off)
            for k, lanes, dev in ((r, la, right), (l, lb, left)):
                tbuf[(*spot(a, k, q), ALL, lanes)] += far[a, q, :, lanes]
                remote(piece(tbuf, a, k, q, lanes), dc.at[1, a, q, :, lanes], dev, send_1, dc_sem[s][u])

    def rs_end(s, u):
        la, lb, full = lanes_of(REDUCE_SEGS[s])
        off = REDUCE_UNITS[s][u]
        wait(dc.at[:, :, unit_blocks(off), :, full], recv.at[dc_sem[s][u]])
        for a in range(2):
            q = block(a, off)
            pbuf[a, q, :, full] = tbuf[(*spot(a, ring_of(a)[0], q), ALL, full)] + dc[0, a, q, :, full] + dc[1, a, q, :, full]
        for a in range(2):
            i, right, left, r, l, f = ring_of(1 - a)
            if RELAY_LAST[s]:
                remote(pbuf.at[a, f, :, la], far2.at[a, :, la], right, send_2, far2_sem[s])
                remote(pbuf.at[a, f, :, lb], far2.at[a, :, lb], left, send_2, far2_sem[s])
                remote(pbuf.at[a, r, :, lb], dc2.at[0, a, :, lb], right, send_2, dc2_sem[s])
                remote(pbuf.at[a, l, :, la], dc2.at[0, a, :, la], left, send_2, dc2_sem[s])
            else:
                for slot, (k, o, dev) in enumerate(((f, 2, ring[1 - a][-1]), (r, 1, right), (l, 3, left))):
                    if off is None or off == o:
                        remote(pbuf.at[a, k, :, full], dc2.at[slot, a, :, full], dev, send_2, dc2_sem[s])

    def rs_cross(s):
        la, lb, full = lanes_of(REDUCE_SEGS[s])
        wait(far2.at[:, :, full], recv.at[far2_sem[s]])
        for a in range(2):
            i, right, left, r, l, f = ring_of(1 - a)
            for k, lanes, dev in ((r, la, right), (l, lb, left)):
                pbuf[a, k, :, lanes] += far2[a, :, lanes]
                remote(pbuf.at[a, k, :, lanes], dc2.at[1, a, :, lanes], dev, send_2, dc2_sem[s])

    def rs_finish(s):
        full = lanes_of(REDUCE_SEGS[s])[-1]
        slots = 2 if RELAY_LAST[s] else 3
        wait(dc2.at[:slots, :, :, full], recv.at[dc2_sem[s]])
        for a in range(2):
            acc = pbuf[a, cross[a], :, full]
            for slot in range(slots):
                acc = acc + dc2[slot, a, :, full]
            gb[W * a:W * a + W, full] = acc

    def rs_load(s):
        t0, n, _ = REDUCE_SEGS[s]
        rows = pl.ds(t0 * T, n * T)
        wait(xown.at[rows], load_sem.at[x_load[s]])
        wait(xown.at[rows], recv.at[swap_recv[s]])
        lax.fori_loop(t0, t0 + n, transpose_in, 0)

    def prepare(_):
        for c in small:
            c.wait()
        first = m_in[:, :HALF].astype(F32)
        second = join_tail(m_out[...].astype(F32), m_in[:, HALF:].astype(F32), pad_a, pad_b)
        mx[core] = jnp.where(on_first, first, second)
        ms[...] = jnp.where(on_first, second, first)
        remote(ms, mx.at[core], partner, m_send, m_recv)
        fo[...] = jnp.where(on_first, c_in[:, :HALF], join_tail(r_out[...], c_in[:, HALF:], pad_c, pad_d))

    m_send, m_recv = next(sends), next(recvs)
    send_3 = next(sends)
    a1_first, a1_rest, a1_fwd, a2_rest = ([next(recvs) for _ in GATHER_SEGS] for _ in range(4))
    a2_first = [[next(recvs) for _ in u] for u in GATHER_UNITS]

    def swap_around(ref, ring_a, s, first, rest):
        la, lb, _ = lanes_of(GATHER_SEGS[s])
        for lanes_r, lanes_l, sem in ((la, lb, first), (lb, la, rest)):
            for a in range(2):
                i, right, left, r, l, f = ring_of(ring_a(a))
                for src in ref(a, i, lanes_r):
                    remote(src, src, right, send_3, sem)
                for src in ref(a, i, lanes_l):
                    remote(src, src, left, send_3, sem)

    def pass_on(ref, ring_a, s, sem):
        la, lb, _ = lanes_of(GATHER_SEGS[s])
        for a in range(2):
            i, right, left, r, l, f = ring_of(ring_a(a))
            for src in ref(a, l, la):
                remote(src, src, right, send_3, sem)
            for src in ref(a, r, lb):
                remote(src, src, left, send_3, sem)

    def store_of(s):
        return m2buf if s == 1 else t2buf

    def one_ref(s):
        return lambda a, q, lanes: [piece(store_of(s), a, ring_of(a)[0], q, lanes)]

    def two_ref(s, u):
        offs = GATHER_UNITS[s][u]
        return lambda a, k, lanes: [piece(store_of(s), a, k, block(a, o), lanes) for o in (offs or (None,))]

    def same(a):
        return a

    def other(a):
        return 1 - a

    def a1_begin(s):
        swap_around(one_ref(s), other, s, a1_first[s], a1_rest[s])

    def a2_begin(s, u):
        swap_around(two_ref(s, u), same, s, a2_first[s][u], a2_rest[s])

    def a1_middle(s):
        wait(far2.at[:, :, lanes_of(GATHER_SEGS[s])[-1]], recv.at[a1_first[s]])
        pass_on(one_ref(s), other, s, a1_fwd[s])

    def a1_near(s):
        wait(far2.at[:, :, lanes_of(GATHER_SEGS[s])[-1]], recv.at[a1_rest[s]])

    def a1_far(s):
        wait(far2.at[:, :, lanes_of(GATHER_SEGS[s])[-1]], recv.at[a1_fwd[s]])

    def a2_middle(s, u):
        wait(far.at[:, :len(GATHER_UNITS[s][u] or BLOCKS), :, lanes_of(GATHER_SEGS[s])[-1]], recv.at[a2_first[s][u]])
        pass_on(two_ref(s, u), same, s, a2_rest[s])

    def a2_end(s):
        wait(dc.at[:, :, :, :, lanes_of(GATHER_SEGS[s])[-1]], recv.at[a2_rest[s]])

    def gather(plan, **more):
        follow(plan, dict(A=a1_begin, B=a2_begin, M=a1_middle, N=a1_near, W=a1_far, P=a2_middle, **more))

    early = pl.ds(0, EARLY * T)
    late = pl.ds(EARLY * T, HALF - EARLY * T)

    def keep(_):
        wait(mx.at[0], recv.at[m_recv])
        for a in range(2):
            m2buf[z, y, a] = mx[a, :, early]

    def follow(plan, table):
        for item in ",".join(plan).split(","):
            table[item[0]](*(int(c) for c in item[1:]))

    follow(REDUCE_PLAN, dict(S=rs_load, B=rs_begin, M=rs_middle, E=rs_end, C=rs_cross, F=rs_finish, H=prepare, K=keep, a=a1_begin, b=a2_begin))

    lane = lax.broadcasted_iota(jnp.int32, (1, HALF), 1)
    is_in = lane >= jnp.where(on_first, 0, F_OUT)
    eye = lax.broadcasted_iota(jnp.int32, (2 * W, T), 0) == lax.broadcasted_iota(jnp.int32, (2 * W, T), 1)

    def sum_of(v, axis):
        return jnp.sum(v, axis=axis, keepdims=True)

    def only_in(v):
        return jnp.where(is_in, v, 0.0)

    def only_out(v):
        return jnp.where(is_in, 0.0, v)

    def to_row(col):
        return sum_of(jnp.where(eye, col, 0.0), 0)

    def to_col(row):
        return sum_of(jnp.where(eye, row, 0.0), 1)

    def spread(slots, me, devs):
        ss, rs = next(sends), next(recvs)
        for dev in devs:
            remote(slots.at[me], slots.at[me], dev, ss, rs)
        return slots.at[pl.ds(0, len(devs))], ss, rs

    g = gb[...]
    sq = g * g + 1e-30
    fv[p] = sum_of(sq, 0)
    fv_ref, fv_send, fv_recv = spread(fv, p, plane)
    for row, col in enumerate((only_in(sq), only_out(sq))):
        rv[line_me, row:row + 1, :] = to_row(sum_of(col, 1))
    for row, ref in ((2, r_in), (3, c_out)):
        rowpad[...] = jnp.zeros_like(rowpad)
        rowpad[ROWS_ONE, :W] = ref[...]
        rv[line_me, row:row + 1, :] = jnp.where(on_first, rowpad[...], pltpu.roll(rowpad[...], W, 1))[:1]
    rv[line_me, RING:, :] = jnp.zeros((RING, T), F32)
    rv_ref, rv_send, rv_recv = spread(rv, line_me, line)

    lr, wd, beta = lr_ref[0], wd_ref[0], beta_ref[0]
    for a in range(2):
        t2buf[z, y, a, :, early] = gb[W * a:W * a + W, early]
    gather(EARLY_PLAN)
    wait(rv_ref, recv.at[rv_recv])
    row_sum = jnp.sum(rv[...], axis=0)
    row_old = rv[0] + rv[1]
    r_new = beta * row_old[2:3] + (1.0 - beta) * (row_sum[:1] / N_IN)
    c_new = beta * row_old[3:4] + (1.0 - beta) * (row_sum[1:2] / N_OUT)
    v = g * jnp.where(is_in, 1.0 / jnp.sqrt(to_col(r_new)), 1.0 / jnp.sqrt(to_col(c_new)))
    sum_rows = sum_of(r_new, 1)
    wait(fv_ref, recv.at[fv_recv])
    f_new = beta * fo[...] + (1.0 - beta) * (jnp.sum(fv[...], axis=0) / D)
    col_scale = 1.0 / jnp.sqrt(f_new)
    u = v * col_scale
    uu = u * u
    f_out = sum_of(only_out(f_new), 1)

    def total(v):
        return jnp.broadcast_to(sum_of(sum_of(v, 0), 1), (1, T))

    pick = lax.broadcasted_iota(jnp.int32, (1, T), 1)
    me_all = x * 32 + d
    share = jnp.where(pick == 0, total(only_in(uu)), jnp.where(pick == 1, total(only_out(uu)), jnp.where(pick == 2, f_out / 16, sum_rows / 8)))
    share = jnp.where(pick < 16, share, pltpu.roll(jnp.where(on_first, r_new, c_new), 16, 1))
    qs[me_all] = share
    q_send, q_recv = next(sends), next(recvs)

    def tell(k, _):
        chip = lax.rem(z + 6 - lax.div(k, RING), RING) * RING + lax.rem(y + 6 - lax.rem(k, RING), RING)
        for i in FAR_FIRST:
            for c in (1 - core, core):
                def go():
                    remote(qs.at[me_all], qs.at[me_all], at(lax.rem(x + i, RING), chip, c), q_send, q_recv)
                if i == 0 and c is core:
                    pl.when(k != 10)(go)
                else:
                    go()
        return 0

    lax.fori_loop(0, 16, tell, 0)
    q_ref = qs.at[pl.ds(0, 127)]
    gb[...] = u
    fnew[...] = f_new
    f_send, f_recv = next(sends), next(recvs)
    remote(fnew, frecv, partner, f_send, f_recv)
    colv[ROWS_ONE] = col_scale
    gather(EARLY_PLAN_END)
    wait(q_ref, recv.at[q_recv])
    totals = jnp.sum(qs[...], axis=0)
    mean_in = totals[:, 3:4] / D
    mean_out = totals[:, 2:3] / N_OUT
    rms_in = jnp.sqrt(totals[:, :1] * mean_in / (D * N_IN))
    rms_out = jnp.sqrt(totals[:, 1:2] * mean_out / (D * N_OUT))
    scale = jnp.where(is_in, jnp.sqrt(mean_in) / jnp.maximum(1.0, rms_in), jnp.sqrt(mean_out) / jnp.maximum(1.0, rms_out))

    for a in range(2):
        mnew[a] = (0.9 * mx[a] + 0.1 * (gb[W * a:W * a + W] * scale)).astype(BF16).astype(F32)
        t2buf[z, y, a, :, late] = mnew[a, :, late]

    lr_wd = lr * wd
    base = core * HALF

    def put_rows(j, tiles):
        dest = pl.ds(pl.multiple_of(base + j * T, T), T)
        rows = pl.ds(pl.multiple_of(j * T, T), T)
        for h in range(2):
            cols = pl.ds(h * D // 2, D // 2)
            w = wown[rows, cols]
            o_w[dest, cols] = w - lr * jnp.concatenate(tiles(h, rows), axis=0).T - lr_wd * w
        remote(o_w.at[dest], o_w.at[dest], partner, out_send, out_recv)

    def moments(h, rows):
        return [t2buf[2 * h + zz, yy, a, :, rows] for zz, yy, a in blocks]

    def moments_early(h, rows):
        out = []
        for zz, yy, a in blocks:
            where = (2 * h + zz, yy, a, ALL, rows)
            upd = t2buf[where] * rf[(2 * h + zz) * RING + yy, W * a:W * a + W] * colv[ROWS_ONE, rows] * colv[pl.ds(1, 1), rows]
            out.append((0.9 * m2buf[where] + 0.1 * upd).astype(BF16).astype(F32))
        return out

    mo_send, mo_recv = next(sends), next(recvs)
    out_send, out_recv = next(sends), next(recvs)

    def state_out():
        wait(frecv, recv.at[f_recv])
        wait(mrecv, recv.at[mo_recv])
        for mine, theirs, out_in, out_out in ((mnew[core], mrecv[...], o_m_in, o_m_out), (fnew[...], frecv[...], o_c_in, o_r_out)):
            lo = jnp.where(on_first, mine, theirs)
            hi = jnp.where(on_first, theirs, mine)
            out_in[:, :HALF] = lo.astype(out_in.dtype)
            out_out[...] = hi[:, :F_OUT].astype(out_out.dtype)
            out_in[:, HALF:] = pltpu.roll(hi[:, HALF - 2 * T:], TAIL, 1)[:, :TAIL].astype(out_in.dtype)
        for new, out in ((r_new, o_r_in), (c_new, o_c_out)):
            rowpad[...] = jnp.broadcast_to(new, rowpad.shape)
            out[...] = jnp.where(on_first, rowpad[...], pltpu.roll(rowpad[...], T - W, 1))[:1, :W]

    def finish(s):
        if s == 0:
            wait(wown, load_sem.at[w_load])
            colv[pl.ds(1, 1)] = scale
            shifted = lax.broadcasted_iota(jnp.int32, (2 * W, T), 0) + 16 == lax.broadcasted_iota(jnp.int32, (2 * W, T), 1)

            def row_factor(chip, _):
                col = sum_of(jnp.where(shifted, qs[x * 32 + chip * 2 + core], 0.0), 1)
                rf[chip] = jnp.broadcast_to(1.0 / jnp.sqrt(col), (2 * W, T))
                return 0

            lax.fori_loop(0, 16, row_factor, 0)
            a2_end(1)
        if s == 2:
            state_out()
        a2_end(s)
        t0, n, _ = GATHER_SEGS[s]

        def tile(j, _):
            put_rows(j, moments if s else moments_early)
            return 0

        lax.fori_loop(t0, t0 + n, tile, 0)

    remote(mnew.at[1 - core], mrecv, partner, mo_send, mo_recv)
    gather(GATHER_PLAN, F=finish)

    wait(xown, recv.at[out_recv])
    for ref, sem in ((xown, swap_send), (ms, m_send), (tbuf.at[:3], send_1), (tbuf.at[0, :3], send_2), (fv_ref, fv_send), (rv_ref, rv_send), (q_ref, q_send),
                     (fnew, f_send), (o_w.at[pl.ds(0, (HALF + EARLY * T) * 15 // 16)], send_3), (ms, mo_send), (xown, out_send)):
        wait(ref, send.at[sem])


def store_kernel(w, m_in, m_out, r_in, c_in, r_out, c_out, o_w_in, o_w_out, o_m_in, o_m_out, o_r_in, o_c_in, o_r_out, o_c_out, sem):
    pairs = [(w.at[pl.ds(src + k * rows, rows)], out.at[pl.ds(dst + k * rows, rows)]) for src, out, dst, rows, count in (
        (0, o_w_in, 0, TAIL, 6), (HALF, o_w_out, 0, TAIL, 5), (HALF + F_OUT, o_w_in, HALF, TAIL, 1)) for k in range(count)]
    pairs += [(m_in, o_m_in), (m_out, o_m_out), (r_in, o_r_in), (c_in, o_c_in), (r_out, o_r_out), (c_out, o_c_out)]
    work = [pltpu.make_async_copy(src, dst, sem.at[n]) for n, (src, dst) in enumerate(pairs)]
    for c in work:
        c.start()
    for c in work:
        c.wait()


def call(*args):
    vmem = pl.BlockSpec(memory_space=pltpu.VMEM)
    hbm = pl.BlockSpec(memory_space=pltpu.HBM)
    smem = pl.BlockSpec(memory_space=pltpu.SMEM)
    small = (((W, F_IN), BF16), ((W, F_OUT), BF16), ((1, W), F32), ((1, F_IN), F32), ((1, F_OUT), F32), ((1, W), F32))
    in_vmem = [pltpu.VMEM(*a) for a in small]
    args = args[:3] + tuple(pltpu.with_memory_space_constraint(a, pltpu.HBM) for a in args[3:])

    def buf(*shape):
        return pltpu.VMEM(shape, F32)

    half, whole, part, line = (HALF, D), (RING, RING, 2, W, HALF), (W, HALF), (1, HALF)
    held = pl.pallas_call(
        kernel,
        name="adafactor_step",
        out_shape=(buf(2 * HALF, D), *in_vmem),
        in_specs=[smem] * 3 + [hbm] * (len(args) - 3),
        out_specs=(vmem,) * (1 + len(small)),
        scratch_shapes=[
            *in_vmem, buf(*half), buf(*half), buf(*half), buf(*whole), buf(*whole), buf(RING, RING, 2, W, EARLY * T), buf(2, *part), buf(16, 2 * W, T), buf(8, HALF),
            buf(2, RING, *part), buf(2, 2, RING, *part), buf(2, RING, *part), buf(2, *part), buf(3, 2, *part),
            buf(2, *part), buf(*part), buf(*part), buf(*line), buf(*line), buf(*line),
            buf(16, *line), buf(8, 8, T), buf(128, 1, T),
            buf(2 * W, HALF), buf(W, T), buf(W, 2 * T), buf(1, T), buf(1, 2 * T), buf(8, T),
            pltpu.SemaphoreType.DMA((N_LOAD,)), pltpu.SemaphoreType.DMA((N_SEND,)), pltpu.SemaphoreType.DMA((N_RECV,)),
        ],
        compiler_params=pltpu.CompilerParams(collective_id=0, has_side_effects=True, vmem_limit_bytes=40 << 20),
    )(*args)
    return pl.pallas_call(
        store_kernel,
        name="store_outputs",
        out_shape=tuple(jax.ShapeDtypeStruct(*a) for a in (((F_IN, D), F32), ((F_OUT, D), F32), *small)),
        in_specs=[vmem] * (1 + len(small)),
        out_specs=(hbm,) * (2 + len(small)),
        scratch_shapes=[pltpu.SemaphoreType.DMA((18,))],
        compiler_params=pltpu.CompilerParams(vmem_limit_bytes=16 << 20),
    )(*held)


def solution(mesh):
    def body(w_in, w_out, g_in, g_out, m_in, m_out, r_in, c_in, r_out, c_out, learn_rate, weight_decay, beta_two):
        outs = call(learn_rate[None], weight_decay[None], beta_two[None], g_in[0, 0].T, g_out[0, 0], w_in[0].T, w_out[0], m_in[0], m_out[0].T, r_in, c_in, r_out, c_out)
        return (outs[0].T[None], outs[1][None], outs[2][None], outs[3].T[None], *outs[4:])

    rows, cols, f_last, f_mid = P(None, 'dp'), P(None, 'tp'), P(None, None, 'tp'), P(None, 'tp', None)
    m_specs = (P(None, 'dp', 'tp'), P(None, 'tp', 'dp'))
    stats = (rows, cols, cols, rows)
    in_specs = (f_last, f_mid, P('dp', None, None, 'tp'), P('dp', None, 'tp', None), *m_specs, *stats, P(), P(), P())
    return jax.shard_map(body, mesh=mesh, in_specs=in_specs, out_specs=(f_last, f_mid, *m_specs, *stats), check_vma=False)
```

```python
import jax
import jax.numpy as jnp
from jax import lax
from jax.experimental import pallas as pl
from jax.experimental.pallas import tpu as pltpu
from jax.sharding import PartitionSpec as P

MESH = pl.DeviceIdType.MESH
F32 = jnp.float32
BF16 = jnp.bfloat16
ALL = slice(None)

D = 768
F_IN = 1344
F_OUT = 960
HALF = 1152
TAIL = 192
N_IN = 5376
N_OUT = 3840
T = 128
W = 24
RING = 4
REDUCE_SEGS = ((0, 2, 1), (2, 2, 1), (4, 5, 2))
EARLY = 3
GATHER_SEGS = ((0, 3, 2), (0, 3, 1), (3, 4, 2), (7, 2, 1))
BLOCKS = (0, 1, 3, 2)
SPLIT = ((0,), (1, 3), (2,))
GATHER_UNITS = (SPLIT, SPLIT, SPLIT, SPLIT)
REDUCE_UNITS = ((None,), (None,), (2, 1, 3, 0))
RELAY_LAST = (True, False, False)
REDUCE_PLAN = ("K0,a1,b10,S0,B00,S1,B10,M00,S2,B20,B21,B22,B23,M10,E00,M20,M21", "M22,M23,E10,C0,E20,E21,E22,E23,m1,n1,b11,p10,F1,F0,F2")
EARLY_PLAN = ("A0,B00,W1,B12,P11,M0",)
EARLY_PLAN_END = ("N0,B01,P00,W0,B02,P12,P01",)
GATHER_PLAN = ("A2,B20,A3,P02,M2,N2,B21,P20,M3,N3,W2,B22,F0,B30,B31,P21", "W3,B32,P22,P30,P31,P32,F2,F3")
FAR_FIRST = (2, 1, 3, 0)
ROWS_ONE = pl.ds(0, 1)
N_SEND = 11
N_RECV = 54
N_LOAD = 10


def spans(half, lo, hi):
    if half == 0:
        return [(0, lo, lo, hi - lo)]
    out = []
    if lo < F_OUT:
        out.append((1, lo, lo, min(hi, F_OUT) - lo))
    if hi > F_OUT:
        start = max(lo, F_OUT)
        out.append((0, start + TAIL, start, hi - start))
    return out


def join_tail(out_val, tail_val, pad_a, pad_b):
    pad_a[...] = jnp.zeros_like(pad_a)
    pad_b[...] = jnp.zeros_like(pad_b)
    cut = F_OUT - F_OUT % T
    pad_a[:, :F_OUT - cut] = out_val[:, cut:]
    pad_b[:, :TAIL] = tail_val
    moved = pltpu.roll(pad_b[...], F_OUT - cut, 1)
    lane = lax.broadcasted_iota(jnp.int32, pad_a.shape, 1)
    mid = jnp.where(lane < F_OUT - cut, pad_a[...], moved[:, :T])
    return jnp.concatenate([out_val[:, :cut], mid, moved[:, T:]], axis=1)


def kernel(lr_ref, wd_ref, beta_ref, g_in, g_out, w_in, w_out, h_m_in, h_m_out, h_r_in, h_c_in, h_r_out, h_c_out,
           o_w, o_m_in, o_m_out, o_r_in, o_c_in, o_r_out, o_c_out,
           m_in, m_out, r_in, c_in, r_out, c_out,
           xown, xrecv, wown, tbuf, t2buf, m2buf, mnew, rf, colv, far, dc, pbuf, far2, dc2,
           mx, ms, mrecv, fo, fnew, frecv, fv, rv, qs, gb, pad_a, pad_b, pad_c, pad_d, rowpad,
           load_sem, send, recv):
    x = lax.axis_index("tp")
    d = lax.axis_index("dp")
    core = lax.rem(d, 2)
    p = lax.div(d, 2)
    y = lax.rem(p, RING)
    z = lax.div(p, RING)
    on_first = core == 0
    line_me = x * 2 + core

    def at(xx, pp, cc):
        return (xx, pp * 2 + cc)

    turn = 1 + 2 * core

    def step(i, k):
        return lax.rem(i + k * turn, RING)

    partner = at(x, p, 1 - core)
    sends = iter(range(N_SEND))
    recvs = iter(range(N_RECV))
    loads = iter(range(N_LOAD))

    def remote(src, dst, dev, s, r):
        if 0 not in src.shape:
            pltpu.make_async_remote_copy(src_ref=src, dst_ref=dst, send_sem=send.at[s], recv_sem=recv.at[r], device_id=dev, device_id_type=MESH).start()

    def wait(ref, sem):
        pltpu.make_async_copy(ref, ref, sem).wait()

    small = [pltpu.make_async_copy(src, dst, load_sem.at[next(loads)]) for src, dst in (
        (h_m_in, m_in), (h_m_out, m_out), (h_r_in, r_in), (h_c_in, c_in), (h_r_out, r_out), (h_c_out, c_out))]
    for c in small:
        c.start()
    x_load = [next(loads) for _ in REDUCE_SEGS]
    for me in range(2):
        @pl.when(core == me)
        def _():
            for (t0, n, _), sem in zip(REDUCE_SEGS, x_load):
                for which, lo, to, rows in spans(me, t0 * T, (t0 + n) * T):
                    pltpu.make_async_copy((g_in, g_out)[which].at[pl.ds(lo, rows)], xown.at[pl.ds(to, rows)], load_sem.at[sem]).start()

    barrier = pltpu.get_barrier_semaphore()
    ring = ((y, *(at(x, z * RING + step(y, k), core) for k in (1, 3, 2))),
            (z, *(at(x, step(z, k) * RING + y, core) for k in (1, 3, 2))))
    line = []
    for k in range(1, 8):
        other = lax.rem(line_me + k, 8)
        line.append(at(lax.div(other, 2), p, lax.rem(other, 2)))
    plane = [at(x, step(z, i) * RING + step(y, k), core) for i in FAR_FIRST for k in FAR_FIRST if i or k]
    greet = [dev for _, right, left, _ in ring for dev in (right, left)] + [at(step(x, k), p, core) for k in (2, 1, 3)] + [partner]
    for dev in greet:
        pl.semaphore_signal(barrier, inc=1, device_id=dev, device_id_type=MESH)

    for c in small:
        c.wait()
    first = m_in[:, :HALF].astype(F32)
    second = join_tail(m_out[...].astype(F32), m_in[:, HALF:].astype(F32), pad_a, pad_b)
    mx[core] = jnp.where(on_first, first, second)
    ms[...] = jnp.where(on_first, second, first)
    fo[...] = jnp.where(on_first, c_in[:, :HALF], join_tail(r_out[...], c_in[:, HALF:], pad_c, pad_d))
    pl.semaphore_wait(barrier, len(greet))
    m_send, m_recv = next(sends), next(recvs)
    remote(ms, mx.at[core], partner, m_send, m_recv)

    swap_send = next(sends)
    swap_recv = [next(recvs) for _ in REDUCE_SEGS]
    for me in range(2):
        @pl.when(core == me)
        def _():
            for (t0, n, _), sem in zip(REDUCE_SEGS, swap_recv):
                for which, lo, to, rows in spans(1 - me, t0 * T, (t0 + n) * T):
                    remote((g_in, g_out)[which].at[pl.ds(lo, rows)], xrecv.at[pl.ds(to, rows)], partner, swap_send, sem)

    w_load = next(loads)
    for me in range(2):
        @pl.when(core == me)
        def _():
            for which, lo, to, rows in spans(me, 0, HALF):
                pltpu.make_async_copy((w_in, w_out)[which].at[pl.ds(lo, rows)], wown.at[pl.ds(to, rows)], load_sem.at[w_load]).start()

    def lanes_of(seg):
        t0, n, n_a = seg
        return pl.ds(t0 * T, n_a * T), pl.ds((t0 + n_a) * T, (n - n_a) * T), pl.ds(t0 * T, n * T)

    blocks = [(i // 8, i // 2 % RING, i % 2) for i in range(16)]

    def transpose_in(j, _):
        rows = pl.ds(pl.multiple_of(j * T, T), T)
        for h in range(2):
            cols = pl.ds(h * D // 2, D // 2)
            t = (xown[rows, cols] + xrecv[rows, cols]).T
            for i, (zz, yy, a) in enumerate(blocks):
                tbuf[2 * h + zz, yy, a, :, rows] = t[W * i:W * i + W]
        return 0

    cross = (z, y)

    def spot(a, k, q):
        return (q, k, 0) if a == 0 else (k, q, 1)

    def piece(buf, a, k, q, lanes):
        return buf.at[(*spot(a, k, q), ALL, lanes)]

    def ring_of(a):
        i, right, left, _ = ring[a]
        return i, right, left, step(i, 1), step(i, 3), step(i, 2)

    def block(a, off):
        return ALL if off is None else step(cross[a], off)

    send_1, send_2 = next(sends), next(sends)
    far_sem, dc_sem = ([[next(recvs) for _ in u] for u in REDUCE_UNITS] for _ in range(2))
    dc2_sem = [next(recvs) for _ in REDUCE_SEGS]
    far2_sem = [next(recvs) if relay else None for relay in RELAY_LAST]

    def rs_begin(s, u):
        la, lb, _ = lanes_of(REDUCE_SEGS[s])
        off = REDUCE_UNITS[s][u]
        for a in range(2):
            i, right, left, r, l, f = ring_of(a)
            q = block(a, off)
            remote(piece(tbuf, a, f, q, la), far.at[a, q, :, la], right, send_1, far_sem[s][u])
            remote(piece(tbuf, a, f, q, lb), far.at[a, q, :, lb], left, send_1, far_sem[s][u])
        for a in range(2):
            i, right, left, r, l, f = ring_of(a)
            q = block(a, off)
            remote(piece(tbuf, a, r, q, lb), dc.at[0, a, q, :, lb], right, send_1, dc_sem[s][u])
            remote(piece(tbuf, a, l, q, la), dc.at[0, a, q, :, la], left, send_1, dc_sem[s][u])

    def unit_blocks(off):
        return pl.ds(0, RING if off is None else 1)

    def rs_middle(s, u):
        la, lb, full = lanes_of(REDUCE_SEGS[s])
        off = REDUCE_UNITS[s][u]
        wait(far.at[:, unit_blocks(off), :, full], recv.at[far_sem[s][u]])
        for a in range(2):
            i, right, left, r, l, f = ring_of(a)
            q = block(a, off)
            for k, lanes, dev in ((r, la, right), (l, lb, left)):
                if lanes.size:
                    tbuf[(*spot(a, k, q), ALL, lanes)] += far[a, q, :, lanes]
                remote(piece(tbuf, a, k, q, lanes), dc.at[1, a, q, :, lanes], dev, send_1, dc_sem[s][u])

    def rs_end(s, u):
        la, lb, full = lanes_of(REDUCE_SEGS[s])
        off = REDUCE_UNITS[s][u]
        wait(dc.at[:, :, unit_blocks(off), :, full], recv.at[dc_sem[s][u]])
        for a in range(2):
            q = block(a, off)
            pbuf[a, q, :, full] = tbuf[(*spot(a, ring_of(a)[0], q), ALL, full)] + dc[0, a, q, :, full] + dc[1, a, q, :, full]
        for a in range(2):
            i, right, left, r, l, f = ring_of(1 - a)
            if RELAY_LAST[s]:
                remote(pbuf.at[a, f, :, la], far2.at[a, :, la], right, send_2, far2_sem[s])
                remote(pbuf.at[a, f, :, lb], far2.at[a, :, lb], left, send_2, far2_sem[s])
                remote(pbuf.at[a, r, :, lb], dc2.at[0, a, :, lb], right, send_2, dc2_sem[s])
                remote(pbuf.at[a, l, :, la], dc2.at[0, a, :, la], left, send_2, dc2_sem[s])
            else:
                for slot, (k, o, dev) in enumerate(((f, 2, ring[1 - a][-1]), (r, 1, right), (l, 3, left))):
                    if off is None or off == o:
                        remote(pbuf.at[a, k, :, full], dc2.at[slot, a, :, full], dev, send_2, dc2_sem[s])

    def rs_cross(s):
        la, lb, full = lanes_of(REDUCE_SEGS[s])
        wait(far2.at[:, :, full], recv.at[far2_sem[s]])
        for a in range(2):
            i, right, left, r, l, f = ring_of(1 - a)
            for k, lanes, dev in ((r, la, right), (l, lb, left)):
                if lanes.size:
                    pbuf[a, k, :, lanes] += far2[a, :, lanes]
                remote(pbuf.at[a, k, :, lanes], dc2.at[1, a, :, lanes], dev, send_2, dc2_sem[s])

    def rs_finish(s):
        full = lanes_of(REDUCE_SEGS[s])[-1]
        slots = 2 if RELAY_LAST[s] else 3
        wait(dc2.at[:slots, :, :, full], recv.at[dc2_sem[s]])
        for a in range(2):
            acc = pbuf[a, cross[a], :, full]
            for slot in range(slots):
                acc = acc + dc2[slot, a, :, full]
            gb[W * a:W * a + W, full] = acc

    def rs_load(s):
        t0, n, _ = REDUCE_SEGS[s]
        rows = pl.ds(t0 * T, n * T)
        wait(xown.at[rows], load_sem.at[x_load[s]])
        wait(xown.at[rows], recv.at[swap_recv[s]])
        lax.fori_loop(t0, t0 + n, transpose_in, 0)

    send_3 = next(sends)
    a1_first, a1_rest, a1_fwd, a2_rest = ([next(recvs) for _ in GATHER_SEGS] for _ in range(4))
    a2_first = [[next(recvs) for _ in u] for u in GATHER_UNITS]

    def swap_around(ref, ring_a, s, first, rest):
        la, lb, _ = lanes_of(GATHER_SEGS[s])
        for lanes_r, lanes_l, sem in ((la, lb, first), (lb, la, rest)):
            for a in range(2):
                i, right, left, r, l, f = ring_of(ring_a(a))
                for src in ref(a, i, lanes_r):
                    remote(src, src, right, send_3, sem)
                for src in ref(a, i, lanes_l):
                    remote(src, src, left, send_3, sem)

    def pass_on(ref, ring_a, s, sem):
        la, lb, _ = lanes_of(GATHER_SEGS[s])
        for a in range(2):
            i, right, left, r, l, f = ring_of(ring_a(a))
            for src in ref(a, l, la):
                remote(src, src, right, send_3, sem)
            for src in ref(a, r, lb):
                remote(src, src, left, send_3, sem)

    def store_of(s):
        return m2buf if s == 1 else t2buf

    def one_ref(s):
        return lambda a, q, lanes: [piece(store_of(s), a, ring_of(a)[0], q, lanes)]

    def two_ref(s, u):
        offs = GATHER_UNITS[s][u]
        return lambda a, k, lanes: [piece(store_of(s), a, k, block(a, o), lanes) for o in (offs or (None,))]

    def same(a):
        return a

    def other(a):
        return 1 - a

    def a1_begin(s):
        swap_around(one_ref(s), other, s, a1_first[s], a1_rest[s])

    def a2_begin(s, u):
        swap_around(two_ref(s, u), same, s, a2_first[s][u], a2_rest[s])

    def a1_middle(s):
        wait(far2.at[:, :, lanes_of(GATHER_SEGS[s])[-1]], recv.at[a1_first[s]])
        pass_on(one_ref(s), other, s, a1_fwd[s])

    def a1_near(s):
        wait(far2.at[:, :, lanes_of(GATHER_SEGS[s])[-1]], recv.at[a1_rest[s]])

    def a1_far(s):
        wait(far2.at[:, :, lanes_of(GATHER_SEGS[s])[-1]], recv.at[a1_fwd[s]])

    def a2_middle(s, u):
        wait(far.at[:, :len(GATHER_UNITS[s][u] or BLOCKS), :, lanes_of(GATHER_SEGS[s])[-1]], recv.at[a2_first[s][u]])
        pass_on(two_ref(s, u), same, s, a2_rest[s])

    def a2_end(s):
        wait(dc.at[:, :, :, :, lanes_of(GATHER_SEGS[s])[-1]], recv.at[a2_rest[s]])

    def gather(plan, **more):
        follow(plan, dict(A=a1_begin, B=a2_begin, M=a1_middle, N=a1_near, W=a1_far, P=a2_middle, **more))

    early = pl.ds(0, EARLY * T)
    late = pl.ds(EARLY * T, HALF - EARLY * T)

    def keep(_):
        wait(mx.at[0], recv.at[m_recv])
        for a in range(2):
            m2buf[z, y, a] = mx[a, :, early]

    def follow(plan, table):
        for item in ",".join(plan).split(","):
            table[item[0]](*(int(c) for c in item[1:]))

    follow(REDUCE_PLAN, dict(S=rs_load, B=rs_begin, M=rs_middle, E=rs_end, C=rs_cross, F=rs_finish, K=keep, a=a1_begin, b=a2_begin, m=a1_middle, n=a1_near, w=a1_far, p=a2_middle))

    lane = lax.broadcasted_iota(jnp.int32, (1, HALF), 1)
    is_in = lane >= jnp.where(on_first, 0, F_OUT)
    eye = lax.broadcasted_iota(jnp.int32, (2 * W, T), 0) == lax.broadcasted_iota(jnp.int32, (2 * W, T), 1)

    def sum_of(v, axis):
        return jnp.sum(v, axis=axis, keepdims=True)

    def only_in(v):
        return jnp.where(is_in, v, 0.0)

    def only_out(v):
        return jnp.where(is_in, 0.0, v)

    def to_row(col):
        return sum_of(jnp.where(eye, col, 0.0), 0)

    def to_col(row):
        return sum_of(jnp.where(eye, row, 0.0), 1)

    def spread(slots, me, devs):
        ss, rs = next(sends), next(recvs)
        for dev in devs:
            remote(slots.at[me], slots.at[me], dev, ss, rs)
        return slots.at[pl.ds(0, len(devs))], ss, rs

    g = gb[...]
    sq = g * g + 1e-30
    fv[p] = sum_of(sq, 0)
    fv_ref, fv_send, fv_recv = spread(fv, p, plane)
    for row, col in enumerate((only_in(sq), only_out(sq))):
        rv[line_me, row:row + 1, :] = to_row(sum_of(col, 1))
    for row, ref in ((2, r_in), (3, c_out)):
        rowpad[...] = jnp.zeros_like(rowpad)
        rowpad[ROWS_ONE, :W] = ref[...]
        rv[line_me, row:row + 1, :] = jnp.where(on_first, rowpad[...], pltpu.roll(rowpad[...], W, 1))[:1]
    rv[line_me, RING:, :] = jnp.zeros((RING, T), F32)
    rv_ref, rv_send, rv_recv = spread(rv, line_me, line)

    lr, wd, beta = lr_ref[0], wd_ref[0], beta_ref[0]
    for a in range(2):
        t2buf[z, y, a, :, early] = gb[W * a:W * a + W, early]
    gather(EARLY_PLAN)
    wait(rv_ref, recv.at[rv_recv])
    row_sum = jnp.sum(rv[...], axis=0)
    row_old = rv[0] + rv[1]
    r_new = beta * row_old[2:3] + (1.0 - beta) * (row_sum[:1] / N_IN)
    c_new = beta * row_old[3:4] + (1.0 - beta) * (row_sum[1:2] / N_OUT)
    v = g * jnp.where(is_in, 1.0 / jnp.sqrt(to_col(r_new)), 1.0 / jnp.sqrt(to_col(c_new)))
    sum_rows = sum_of(r_new, 1)
    wait(fv_ref, recv.at[fv_recv])
    f_new = beta * fo[...] + (1.0 - beta) * (jnp.sum(fv[...], axis=0) / D)
    col_scale = 1.0 / jnp.sqrt(f_new)
    u = v * col_scale
    uu = u * u
    f_out = sum_of(only_out(f_new), 1)

    def total(v):
        return jnp.broadcast_to(sum_of(sum_of(v, 0), 1), (1, T))

    pick = lax.broadcasted_iota(jnp.int32, (1, T), 1)
    me_all = x * 32 + d
    share = jnp.where(pick == 0, total(only_in(uu)), jnp.where(pick == 1, total(only_out(uu)), jnp.where(pick == 2, f_out / 16, sum_rows / 8)))
    share = jnp.where(pick < 16, share, pltpu.roll(jnp.where(on_first, r_new, c_new), 16, 1))
    qs[me_all] = share
    q_send, q_recv = next(sends), next(recvs)

    def tell(k, _):
        chip = lax.rem(z + 6 - lax.div(k, RING), RING) * RING + lax.rem(y + 6 - lax.rem(k, RING), RING)
        for i in FAR_FIRST:
            for c in (1 - core, core):
                def go():
                    remote(qs.at[me_all], qs.at[me_all], at(lax.rem(x + i, RING), chip, c), q_send, q_recv)
                if i == 0 and c is core:
                    pl.when(k != 10)(go)
                else:
                    go()
        return 0

    lax.fori_loop(0, 16, tell, 0)
    q_ref = qs.at[pl.ds(0, 127)]
    gb[...] = u
    fnew[...] = f_new
    f_send, f_recv = next(sends), next(recvs)
    remote(fnew, frecv, partner, f_send, f_recv)
    colv[ROWS_ONE] = col_scale
    gather(EARLY_PLAN_END)
    wait(q_ref, recv.at[q_recv])
    totals = jnp.sum(qs[...], axis=0)
    mean_in = totals[:, 3:4] / D
    mean_out = totals[:, 2:3] / N_OUT
    rms_in = jnp.sqrt(totals[:, :1] * mean_in / (D * N_IN))
    rms_out = jnp.sqrt(totals[:, 1:2] * mean_out / (D * N_OUT))
    scale = jnp.where(is_in, jnp.sqrt(mean_in) / jnp.maximum(1.0, rms_in), jnp.sqrt(mean_out) / jnp.maximum(1.0, rms_out))

    for a in range(2):
        mnew[a] = (0.9 * mx[a] + 0.1 * (gb[W * a:W * a + W] * scale)).astype(BF16).astype(F32)
        t2buf[z, y, a, :, late] = mnew[a, :, late]

    lr_wd = lr * wd
    base = core * HALF

    def put_rows(j, tiles):
        dest = pl.ds(pl.multiple_of(base + j * T, T), T)
        rows = pl.ds(pl.multiple_of(j * T, T), T)
        for h in range(2):
            cols = pl.ds(h * D // 2, D // 2)
            w = wown[rows, cols]
            o_w[dest, cols] = w - lr * jnp.concatenate(tiles(h, rows), axis=0).T - lr_wd * w
        remote(o_w.at[dest], o_w.at[dest], partner, out_send, out_recv)

    def moments(h, rows):
        return [t2buf[2 * h + zz, yy, a, :, rows] for zz, yy, a in blocks]

    def moments_early(h, rows):
        out = []
        for zz, yy, a in blocks:
            where = (2 * h + zz, yy, a, ALL, rows)
            upd = t2buf[where] * rf[(2 * h + zz) * RING + yy, W * a:W * a + W] * colv[ROWS_ONE, rows] * colv[pl.ds(1, 1), rows]
            out.append((0.9 * m2buf[where] + 0.1 * upd).astype(BF16).astype(F32))
        return out

    mo_send, mo_recv = next(sends), next(recvs)
    out_send, out_recv = next(sends), next(recvs)

    def state_out():
        wait(frecv, recv.at[f_recv])
        wait(mrecv, recv.at[mo_recv])
        for mine, theirs, out_in, out_out in ((mnew[core], mrecv[...], o_m_in, o_m_out), (fnew[...], frecv[...], o_c_in, o_r_out)):
            lo = jnp.where(on_first, mine, theirs)
            hi = jnp.where(on_first, theirs, mine)
            out_in[:, :HALF] = lo.astype(out_in.dtype)
            out_out[...] = hi[:, :F_OUT].astype(out_out.dtype)
            out_in[:, HALF:] = pltpu.roll(hi[:, HALF - 2 * T:], TAIL, 1)[:, :TAIL].astype(out_in.dtype)
        for new, out in ((r_new, o_r_in), (c_new, o_c_out)):
            rowpad[...] = jnp.broadcast_to(new, rowpad.shape)
            out[...] = jnp.where(on_first, rowpad[...], pltpu.roll(rowpad[...], T - W, 1))[:1, :W]

    def finish(s):
        if s == 0:
            wait(wown, load_sem.at[w_load])
            colv[pl.ds(1, 1)] = scale
            shifted = lax.broadcasted_iota(jnp.int32, (2 * W, T), 0) + 16 == lax.broadcasted_iota(jnp.int32, (2 * W, T), 1)

            def row_factor(chip, _):
                col = sum_of(jnp.where(shifted, qs[x * 32 + chip * 2 + core], 0.0), 1)
                rf[chip] = jnp.broadcast_to(1.0 / jnp.sqrt(col), (2 * W, T))
                return 0

            lax.fori_loop(0, 16, row_factor, 0)
            a2_end(1)
        if s == 2:
            state_out()
        a2_end(s)
        t0, n, _ = GATHER_SEGS[s]

        def tile(j, _):
            put_rows(j, moments if s else moments_early)
            return 0

        lax.fori_loop(t0, t0 + n, tile, 0)

    remote(mnew.at[1 - core], mrecv, partner, mo_send, mo_recv)
    gather(GATHER_PLAN, F=finish)

    wait(xown, recv.at[out_recv])
    for ref, sem in ((xown, swap_send), (ms, m_send), (tbuf.at[:3], send_1), (tbuf.at[0, :3], send_2), (fv_ref, fv_send), (rv_ref, rv_send), (q_ref, q_send),
                     (fnew, f_send), (o_w.at[pl.ds(0, (HALF + EARLY * T) * 15 // 16)], send_3), (ms, mo_send), (xown, out_send)):
        wait(ref, send.at[sem])


def store_kernel(w, m_in, m_out, r_in, c_in, r_out, c_out, o_w_in, o_w_out, o_m_in, o_m_out, o_r_in, o_c_in, o_r_out, o_c_out, sem):
    pairs = [(w.at[pl.ds(src + k * rows, rows)], out.at[pl.ds(dst + k * rows, rows)]) for src, out, dst, rows, count in (
        (0, o_w_in, 0, TAIL, 6), (HALF, o_w_out, 0, TAIL, 5), (HALF + F_OUT, o_w_in, HALF, TAIL, 1)) for k in range(count)]
    pairs += [(m_in, o_m_in), (m_out, o_m_out), (r_in, o_r_in), (c_in, o_c_in), (r_out, o_r_out), (c_out, o_c_out)]
    work = [pltpu.make_async_copy(src, dst, sem.at[n]) for n, (src, dst) in enumerate(pairs)]
    for c in work:
        c.start()
    for c in work:
        c.wait()


def call(*args):
    vmem = pl.BlockSpec(memory_space=pltpu.VMEM)
    hbm = pl.BlockSpec(memory_space=pltpu.HBM)
    smem = pl.BlockSpec(memory_space=pltpu.SMEM)
    small = (((W, F_IN), BF16), ((W, F_OUT), BF16), ((1, W), F32), ((1, F_IN), F32), ((1, F_OUT), F32), ((1, W), F32))
    in_vmem = [pltpu.VMEM(*a) for a in small]
    args = args[:3] + tuple(pltpu.with_memory_space_constraint(a, pltpu.HBM) for a in args[3:])

    def buf(*shape):
        return pltpu.VMEM(shape, F32)

    half, whole, part, line = (HALF, D), (RING, RING, 2, W, HALF), (W, HALF), (1, HALF)
    held = pl.pallas_call(
        kernel,
        name="adafactor_step",
        out_shape=(buf(2 * HALF, D), *in_vmem),
        in_specs=[smem] * 3 + [hbm] * (len(args) - 3),
        out_specs=(vmem,) * (1 + len(small)),
        scratch_shapes=[
            *in_vmem, buf(*half), buf(*half), buf(*half), buf(*whole), buf(*whole), buf(RING, RING, 2, W, EARLY * T), buf(2, *part), buf(16, 2 * W, T), buf(8, HALF),
            buf(2, RING, *part), buf(2, 2, RING, *part), buf(2, RING, *part), buf(2, *part), buf(3, 2, *part),
            buf(2, *part), buf(*part), buf(*part), buf(*line), buf(*line), buf(*line),
            buf(16, *line), buf(8, 8, T), buf(128, 1, T),
            buf(2 * W, HALF), buf(W, T), buf(W, 2 * T), buf(1, T), buf(1, 2 * T), buf(8, T),
            pltpu.SemaphoreType.DMA((N_LOAD,)), pltpu.SemaphoreType.DMA((N_SEND,)), pltpu.SemaphoreType.DMA((N_RECV,)),
        ],
        compiler_params=pltpu.CompilerParams(collective_id=0, has_side_effects=True, vmem_limit_bytes=40 << 20),
    )(*args)
    return pl.pallas_call(
        store_kernel,
        name="store_outputs",
        out_shape=tuple(jax.ShapeDtypeStruct(*a) for a in (((F_IN, D), F32), ((F_OUT, D), F32), *small)),
        in_specs=[vmem] * (1 + len(small)),
        out_specs=(hbm,) * (2 + len(small)),
        scratch_shapes=[pltpu.SemaphoreType.DMA((18,))],
        compiler_params=pltpu.CompilerParams(vmem_limit_bytes=16 << 20),
    )(*held)


def solution(mesh):
    def body(w_in, w_out, g_in, g_out, m_in, m_out, r_in, c_in, r_out, c_out, learn_rate, weight_decay, beta_two):
        outs = call(learn_rate[None], weight_decay[None], beta_two[None], g_in[0, 0].T, g_out[0, 0], w_in[0].T, w_out[0], m_in[0], m_out[0].T, r_in, c_in, r_out, c_out)
        return (outs[0].T[None], outs[1][None], outs[2][None], outs[3].T[None], *outs[4:])

    rows, cols, f_last, f_mid = P(None, 'dp'), P(None, 'tp'), P(None, None, 'tp'), P(None, 'tp', None)
    m_specs = (P(None, 'dp', 'tp'), P(None, 'tp', 'dp'))
    stats = (rows, cols, cols, rows)
    in_specs = (f_last, f_mid, P('dp', None, None, 'tp'), P('dp', None, 'tp', None), *m_specs, *stats, P(), P(), P())
    return jax.shard_map(body, mesh=mesh, in_specs=in_specs, out_specs=(f_last, f_mid, *m_specs, *stats), check_vma=False)
```

```python
import jax
import jax.numpy as jnp
from jax import lax
from jax.experimental import pallas as pl
from jax.experimental.pallas import tpu as pltpu
from jax.sharding import PartitionSpec as P

MESH = pl.DeviceIdType.MESH
F32 = jnp.float32
BF16 = jnp.bfloat16
ALL = slice(None)

D = 768
F_IN = 1344
F_OUT = 960
HALF = 1152
TAIL = 192
N_IN = 5376
N_OUT = 3840
T = 128
W = 24
RING = 4
REDUCE_SEGS = ((0, 2, 1), (2, 2, 1), (4, 5, 2))
EARLY = 3
GATHER_SEGS = ((0, 3, 2), (0, 3, 1), (3, 2, 1), (5, 2, 1), (7, 2, 1))
BLOCKS = (0, 1, 3, 2)
SPLIT = ((0,), (1, 3), (2,))
GATHER_UNITS = (SPLIT, SPLIT, SPLIT, SPLIT, SPLIT)
REDUCE_UNITS = ((None,), (None,), (2, 1, 3, 0))
RELAY_LAST = (True, False, False)
REDUCE_PLAN = ("K0,a1,b10,S0,B00,S1,B10,M00,S2,B20,B21,B22,B23,M10,E00,M20,M21", "M22,M23,E10,C0,E20,E21,E22,E23,m1,n1,b11,p10,F1,F0,F2")
EARLY_PLAN = ("A0,B00,W1,B12,P11,M0",)
EARLY_PLAN_END = ("N0,B01,P00,W0,B02,P12,P01",)
GATHER_PLAN = ("A2,A3,B30,A4,B20,B40,P02,R0,M2,M3,N3,B31,M4,N2,B21", "W2,B22,N4,G0,W3,B32,G1,B41,W4,G2,B42,P21,P20,P22,P31", "P30,P32,P40,P41,P42,F2,F3,F4")
FAR_FIRST = (2, 1, 3, 0)
ROWS_ONE = pl.ds(0, 1)
N_SEND = 11
N_RECV = 61
N_LOAD = 10


def spans(half, lo, hi):
    if half == 0:
        return [(0, lo, lo, hi - lo)]
    out = []
    if lo < F_OUT:
        out.append((1, lo, lo, min(hi, F_OUT) - lo))
    if hi > F_OUT:
        start = max(lo, F_OUT)
        out.append((0, start + TAIL, start, hi - start))
    return out


def join_tail(out_val, tail_val, pad_a, pad_b):
    pad_a[...] = jnp.zeros_like(pad_a)
    pad_b[...] = jnp.zeros_like(pad_b)
    cut = F_OUT - F_OUT % T
    pad_a[:, :F_OUT - cut] = out_val[:, cut:]
    pad_b[:, :TAIL] = tail_val
    moved = pltpu.roll(pad_b[...], F_OUT - cut, 1)
    lane = lax.broadcasted_iota(jnp.int32, pad_a.shape, 1)
    mid = jnp.where(lane < F_OUT - cut, pad_a[...], moved[:, :T])
    return jnp.concatenate([out_val[:, :cut], mid, moved[:, T:]], axis=1)


def kernel(lr_ref, wd_ref, beta_ref, g_in, g_out, w_in, w_out, h_m_in, h_m_out, h_r_in, h_c_in, h_r_out, h_c_out,
           o_w, o_m_in, o_m_out, o_r_in, o_c_in, o_r_out, o_c_out,
           m_in, m_out, r_in, c_in, r_out, c_out,
           xown, xrecv, wown, tbuf, t2buf, m2buf, mnew, rf, colv, far, dc, pbuf, far2, dc2,
           mx, ms, mrecv, fo, fnew, frecv, fv, rv, qs, gb, pad_a, pad_b, pad_c, pad_d, rowpad,
           load_sem, send, recv):
    x = lax.axis_index("tp")
    d = lax.axis_index("dp")
    core = lax.rem(d, 2)
    p = lax.div(d, 2)
    y = lax.rem(p, RING)
    z = lax.div(p, RING)
    on_first = core == 0
    line_me = x * 2 + core

    def at(xx, pp, cc):
        return (xx, pp * 2 + cc)

    turn = 1 + 2 * core

    def step(i, k):
        return lax.rem(i + k * turn, RING)

    partner = at(x, p, 1 - core)
    sends = iter(range(N_SEND))
    recvs = iter(range(N_RECV))
    loads = iter(range(N_LOAD))

    def remote(src, dst, dev, s, r):
        if 0 not in src.shape:
            pltpu.make_async_remote_copy(src_ref=src, dst_ref=dst, send_sem=send.at[s], recv_sem=recv.at[r], device_id=dev, device_id_type=MESH).start()

    def wait(ref, sem):
        pltpu.make_async_copy(ref, ref, sem).wait()

    small = [pltpu.make_async_copy(src, dst, load_sem.at[next(loads)]) for src, dst in (
        (h_m_in, m_in), (h_m_out, m_out), (h_r_in, r_in), (h_c_in, c_in), (h_r_out, r_out), (h_c_out, c_out))]
    for c in small:
        c.start()
    x_load = [next(loads) for _ in REDUCE_SEGS]
    for me in range(2):
        @pl.when(core == me)
        def _():
            for (t0, n, _), sem in zip(REDUCE_SEGS, x_load):
                for which, lo, to, rows in spans(me, t0 * T, (t0 + n) * T):
                    pltpu.make_async_copy((g_in, g_out)[which].at[pl.ds(lo, rows)], xown.at[pl.ds(to, rows)], load_sem.at[sem]).start()

    barrier = pltpu.get_barrier_semaphore()
    ring = ((y, *(at(x, z * RING + step(y, k), core) for k in (1, 3, 2))),
            (z, *(at(x, step(z, k) * RING + y, core) for k in (1, 3, 2))))
    line = []
    for k in range(1, 8):
        other = lax.rem(line_me + k, 8)
        line.append(at(lax.div(other, 2), p, lax.rem(other, 2)))
    plane = [at(x, step(z, i) * RING + step(y, k), core) for i in FAR_FIRST for k in FAR_FIRST if i or k]
    greet = [dev for _, right, left, _ in ring for dev in (right, left)] + [at(step(x, k), p, core) for k in (2, 1, 3)] + [partner]
    for dev in greet:
        pl.semaphore_signal(barrier, inc=1, device_id=dev, device_id_type=MESH)

    for c in small:
        c.wait()
    first = m_in[:, :HALF].astype(F32)
    second = join_tail(m_out[...].astype(F32), m_in[:, HALF:].astype(F32), pad_a, pad_b)
    mx[core] = jnp.where(on_first, first, second)
    ms[...] = jnp.where(on_first, second, first)
    fo[...] = jnp.where(on_first, c_in[:, :HALF], join_tail(r_out[...], c_in[:, HALF:], pad_c, pad_d))
    pl.semaphore_wait(barrier, len(greet))
    m_send, m_recv = next(sends), next(recvs)
    remote(ms, mx.at[core], partner, m_send, m_recv)

    swap_send = next(sends)
    swap_recv = [next(recvs) for _ in REDUCE_SEGS]
    for me in range(2):
        @pl.when(core == me)
        def _():
            for (t0, n, _), sem in zip(REDUCE_SEGS, swap_recv):
                for which, lo, to, rows in spans(1 - me, t0 * T, (t0 + n) * T):
                    remote((g_in, g_out)[which].at[pl.ds(lo, rows)], xrecv.at[pl.ds(to, rows)], partner, swap_send, sem)

    w_load = next(loads)
    for me in range(2):
        @pl.when(core == me)
        def _():
            for which, lo, to, rows in spans(me, 0, HALF):
                pltpu.make_async_copy((w_in, w_out)[which].at[pl.ds(lo, rows)], wown.at[pl.ds(to, rows)], load_sem.at[w_load]).start()

    def lanes_of(seg):
        t0, n, n_a = seg
        return pl.ds(t0 * T, n_a * T), pl.ds((t0 + n_a) * T, (n - n_a) * T), pl.ds(t0 * T, n * T)

    blocks = [(i // 8, i // 2 % RING, i % 2) for i in range(16)]

    def transpose_in(j, _):
        rows = pl.ds(pl.multiple_of(j * T, T), T)
        for h in range(2):
            cols = pl.ds(h * D // 2, D // 2)
            t = (xown[rows, cols] + xrecv[rows, cols]).T
            for i, (zz, yy, a) in enumerate(blocks):
                tbuf[2 * h + zz, yy, a, :, rows] = t[W * i:W * i + W]
        return 0

    cross = (z, y)

    def spot(a, k, q):
        return (q, k, 0) if a == 0 else (k, q, 1)

    def piece(buf, a, k, q, lanes):
        return buf.at[(*spot(a, k, q), ALL, lanes)]

    def ring_of(a):
        i, right, left, _ = ring[a]
        return i, right, left, step(i, 1), step(i, 3), step(i, 2)

    def block(a, off):
        return ALL if off is None else step(cross[a], off)

    send_1, send_2 = next(sends), next(sends)
    far_sem, dc_sem = ([[next(recvs) for _ in u] for u in REDUCE_UNITS] for _ in range(2))
    dc2_sem = [next(recvs) for _ in REDUCE_SEGS]
    far2_sem = [next(recvs) if relay else None for relay in RELAY_LAST]

    def rs_begin(s, u):
        la, lb, _ = lanes_of(REDUCE_SEGS[s])
        off = REDUCE_UNITS[s][u]
        for a in range(2):
            i, right, left, r, l, f = ring_of(a)
            q = block(a, off)
            remote(piece(tbuf, a, f, q, la), far.at[a, q, :, la], right, send_1, far_sem[s][u])
            remote(piece(tbuf, a, f, q, lb), far.at[a, q, :, lb], left, send_1, far_sem[s][u])
        for a in range(2):
            i, right, left, r, l, f = ring_of(a)
            q = block(a, off)
            remote(piece(tbuf, a, r, q, lb), dc.at[0, a, q, :, lb], right, send_1, dc_sem[s][u])
            remote(piece(tbuf, a, l, q, la), dc.at[0, a, q, :, la], left, send_1, dc_sem[s][u])

    def unit_blocks(off):
        return pl.ds(0, RING if off is None else 1)

    def rs_middle(s, u):
        la, lb, full = lanes_of(REDUCE_SEGS[s])
        off = REDUCE_UNITS[s][u]
        wait(far.at[:, unit_blocks(off), :, full], recv.at[far_sem[s][u]])
        for a in range(2):
            i, right, left, r, l, f = ring_of(a)
            q = block(a, off)
            for k, lanes, dev in ((r, la, right), (l, lb, left)):
                if lanes.size:
                    tbuf[(*spot(a, k, q), ALL, lanes)] += far[a, q, :, lanes]
                remote(piece(tbuf, a, k, q, lanes), dc.at[1, a, q, :, lanes], dev, send_1, dc_sem[s][u])

    def rs_end(s, u):
        la, lb, full = lanes_of(REDUCE_SEGS[s])
        off = REDUCE_UNITS[s][u]
        wait(dc.at[:, :, unit_blocks(off), :, full], recv.at[dc_sem[s][u]])
        for a in range(2):
            q = block(a, off)
            pbuf[a, q, :, full] = tbuf[(*spot(a, ring_of(a)[0], q), ALL, full)] + dc[0, a, q, :, full] + dc[1, a, q, :, full]
        for a in range(2):
            i, right, left, r, l, f = ring_of(1 - a)
            if RELAY_LAST[s]:
                remote(pbuf.at[a, f, :, la], far2.at[a, :, la], right, send_2, far2_sem[s])
                remote(pbuf.at[a, f, :, lb], far2.at[a, :, lb], left, send_2, far2_sem[s])
                remote(pbuf.at[a, r, :, lb], dc2.at[0, a, :, lb], right, send_2, dc2_sem[s])
                remote(pbuf.at[a, l, :, la], dc2.at[0, a, :, la], left, send_2, dc2_sem[s])
            else:
                for slot, (k, o, dev) in enumerate(((f, 2, ring[1 - a][-1]), (r, 1, right), (l, 3, left))):
                    if off is None or off == o:
                        remote(pbuf.at[a, k, :, full], dc2.at[slot, a, :, full], dev, send_2, dc2_sem[s])

    def rs_cross(s):
        la, lb, full = lanes_of(REDUCE_SEGS[s])
        wait(far2.at[:, :, full], recv.at[far2_sem[s]])
        for a in range(2):
            i, right, left, r, l, f = ring_of(1 - a)
            for k, lanes, dev in ((r, la, right), (l, lb, left)):
                if lanes.size:
                    pbuf[a, k, :, lanes] += far2[a, :, lanes]
                remote(pbuf.at[a, k, :, lanes], dc2.at[1, a, :, lanes], dev, send_2, dc2_sem[s])

    def rs_finish(s):
        full = lanes_of(REDUCE_SEGS[s])[-1]
        slots = 2 if RELAY_LAST[s] else 3
        wait(dc2.at[:slots, :, :, full], recv.at[dc2_sem[s]])
        for a in range(2):
            acc = pbuf[a, cross[a], :, full]
            for slot in range(slots):
                acc = acc + dc2[slot, a, :, full]
            gb[W * a:W * a + W, full] = acc

    def rs_load(s):
        t0, n, _ = REDUCE_SEGS[s]
        rows = pl.ds(t0 * T, n * T)
        wait(xown.at[rows], load_sem.at[x_load[s]])
        wait(xown.at[rows], recv.at[swap_recv[s]])
        lax.fori_loop(t0, t0 + n, transpose_in, 0)

    send_3 = next(sends)
    a1_first, a1_rest, a1_fwd, a2_rest = ([next(recvs) for _ in GATHER_SEGS] for _ in range(4))
    a2_first = [[next(recvs) for _ in u] for u in GATHER_UNITS]

    def swap_around(ref, ring_a, s, first, rest):
        la, lb, _ = lanes_of(GATHER_SEGS[s])
        for lanes_r, lanes_l, sem in ((la, lb, first), (lb, la, rest)):
            for a in range(2):
                i, right, left, r, l, f = ring_of(ring_a(a))
                for src in ref(a, i, lanes_r):
                    remote(src, src, right, send_3, sem)
                for src in ref(a, i, lanes_l):
                    remote(src, src, left, send_3, sem)

    def pass_on(ref, ring_a, s, sem):
        la, lb, _ = lanes_of(GATHER_SEGS[s])
        for a in range(2):
            i, right, left, r, l, f = ring_of(ring_a(a))
            for src in ref(a, l, la):
                remote(src, src, right, send_3, sem)
            for src in ref(a, r, lb):
                remote(src, src, left, send_3, sem)

    def store_of(s):
        return m2buf if s == 1 else t2buf

    def one_ref(s):
        return lambda a, q, lanes: [piece(store_of(s), a, ring_of(a)[0], q, lanes)]

    def two_ref(s, u):
        offs = GATHER_UNITS[s][u]
        return lambda a, k, lanes: [piece(store_of(s), a, k, block(a, o), lanes) for o in (offs or (None,))]

    def same(a):
        return a

    def other(a):
        return 1 - a

    def a1_begin(s):
        swap_around(one_ref(s), other, s, a1_first[s], a1_rest[s])

    def a2_begin(s, u):
        swap_around(two_ref(s, u), same, s, a2_first[s][u], a2_rest[s])

    def a1_middle(s):
        wait(far2.at[:, :, lanes_of(GATHER_SEGS[s])[-1]], recv.at[a1_first[s]])
        pass_on(one_ref(s), other, s, a1_fwd[s])

    def a1_near(s):
        wait(far2.at[:, :, lanes_of(GATHER_SEGS[s])[-1]], recv.at[a1_rest[s]])

    def a1_far(s):
        wait(far2.at[:, :, lanes_of(GATHER_SEGS[s])[-1]], recv.at[a1_fwd[s]])

    def a2_middle(s, u):
        wait(far.at[:, :len(GATHER_UNITS[s][u] or BLOCKS), :, lanes_of(GATHER_SEGS[s])[-1]], recv.at[a2_first[s][u]])
        pass_on(two_ref(s, u), same, s, a2_rest[s])

    def a2_end(s):
        wait(dc.at[:, :, :, :, lanes_of(GATHER_SEGS[s])[-1]], recv.at[a2_rest[s]])

    def gather(plan, **more):
        follow(plan, dict(A=a1_begin, B=a2_begin, M=a1_middle, N=a1_near, W=a1_far, P=a2_middle, **more))

    early = pl.ds(0, EARLY * T)
    late = pl.ds(EARLY * T, HALF - EARLY * T)

    def keep(_):
        wait(mx.at[0], recv.at[m_recv])
        for a in range(2):
            m2buf[z, y, a] = mx[a, :, early]

    def follow(plan, table):
        for item in ",".join(plan).split(","):
            table[item[0]](*(int(c) for c in item[1:]))

    follow(REDUCE_PLAN, dict(S=rs_load, B=rs_begin, M=rs_middle, E=rs_end, C=rs_cross, F=rs_finish, K=keep, a=a1_begin, b=a2_begin, m=a1_middle, n=a1_near, w=a1_far, p=a2_middle))

    lane = lax.broadcasted_iota(jnp.int32, (1, HALF), 1)
    is_in = lane >= jnp.where(on_first, 0, F_OUT)
    eye = lax.broadcasted_iota(jnp.int32, (2 * W, T), 0) == lax.broadcasted_iota(jnp.int32, (2 * W, T), 1)

    def sum_of(v, axis):
        return jnp.sum(v, axis=axis, keepdims=True)

    def only_in(v):
        return jnp.where(is_in, v, 0.0)

    def only_out(v):
        return jnp.where(is_in, 0.0, v)

    def to_row(col):
        return sum_of(jnp.where(eye, col, 0.0), 0)

    def to_col(row):
        return sum_of(jnp.where(eye, row, 0.0), 1)

    def spread(slots, me, devs):
        ss, rs = next(sends), next(recvs)
        for dev in devs:
            remote(slots.at[me], slots.at[me], dev, ss, rs)
        return slots.at[pl.ds(0, len(devs))], ss, rs

    g = gb[...]
    sq = g * g + 1e-30
    fv[p] = sum_of(sq, 0)
    fv_ref, fv_send, fv_recv = spread(fv, p, plane)
    for row, col in enumerate((only_in(sq), only_out(sq))):
        rv[line_me, row:row + 1, :] = to_row(sum_of(col, 1))
    for row, ref in ((2, r_in), (3, c_out)):
        rowpad[...] = jnp.zeros_like(rowpad)
        rowpad[ROWS_ONE, :W] = ref[...]
        rv[line_me, row:row + 1, :] = jnp.where(on_first, rowpad[...], pltpu.roll(rowpad[...], W, 1))[:1]
    rv[line_me, RING:, :] = jnp.zeros((RING, T), F32)
    rv_ref, rv_send, rv_recv = spread(rv, line_me, line)

    lr, wd, beta = lr_ref[0], wd_ref[0], beta_ref[0]
    for a in range(2):
        t2buf[z, y, a, :, early] = gb[W * a:W * a + W, early]
    gather(EARLY_PLAN)
    wait(rv_ref, recv.at[rv_recv])
    row_sum = jnp.sum(rv[...], axis=0)
    row_old = rv[0] + rv[1]
    r_new = beta * row_old[2:3] + (1.0 - beta) * (row_sum[:1] / N_IN)
    c_new = beta * row_old[3:4] + (1.0 - beta) * (row_sum[1:2] / N_OUT)
    v = g * jnp.where(is_in, 1.0 / jnp.sqrt(to_col(r_new)), 1.0 / jnp.sqrt(to_col(c_new)))
    sum_rows = sum_of(r_new, 1)
    wait(fv_ref, recv.at[fv_recv])
    f_new = beta * fo[...] + (1.0 - beta) * (jnp.sum(fv[...], axis=0) / D)
    col_scale = 1.0 / jnp.sqrt(f_new)
    u = v * col_scale
    uu = u * u
    f_out = sum_of(only_out(f_new), 1)

    def total(v):
        return jnp.broadcast_to(sum_of(sum_of(v, 0), 1), (1, T))

    pick = lax.broadcasted_iota(jnp.int32, (1, T), 1)
    me_all = x * 32 + d
    share = jnp.where(pick == 0, total(only_in(uu)), jnp.where(pick == 1, total(only_out(uu)), jnp.where(pick == 2, f_out / 16, sum_rows / 8)))
    share = jnp.where(pick < 16, share, pltpu.roll(jnp.where(on_first, r_new, c_new), 16, 1))
    qs[me_all] = share
    q_send, q_recv = next(sends), next(recvs)

    def tell(k, _):
        chip = lax.rem(z + 6 - lax.div(k, RING), RING) * RING + lax.rem(y + 6 - lax.rem(k, RING), RING)
        for i in FAR_FIRST:
            for c in (1 - core, core):
                def go():
                    remote(qs.at[me_all], qs.at[me_all], at(lax.rem(x + i, RING), chip, c), q_send, q_recv)
                if i == 0 and c is core:
                    pl.when(k != 10)(go)
                else:
                    go()
        return 0

    lax.fori_loop(0, 16, tell, 0)
    q_ref = qs.at[pl.ds(0, 127)]
    gb[...] = u
    fnew[...] = f_new
    f_send, f_recv = next(sends), next(recvs)
    remote(fnew, frecv, partner, f_send, f_recv)
    colv[ROWS_ONE] = col_scale
    gather(EARLY_PLAN_END)
    wait(q_ref, recv.at[q_recv])
    totals = jnp.sum(qs[...], axis=0)
    mean_in = totals[:, 3:4] / D
    mean_out = totals[:, 2:3] / N_OUT
    rms_in = jnp.sqrt(totals[:, :1] * mean_in / (D * N_IN))
    rms_out = jnp.sqrt(totals[:, 1:2] * mean_out / (D * N_OUT))
    scale = jnp.where(is_in, jnp.sqrt(mean_in) / jnp.maximum(1.0, rms_in), jnp.sqrt(mean_out) / jnp.maximum(1.0, rms_out))

    for a in range(2):
        mnew[a] = (0.9 * mx[a] + 0.1 * (gb[W * a:W * a + W] * scale)).astype(BF16).astype(F32)
        t2buf[z, y, a, :, late] = mnew[a, :, late]

    lr_wd = lr * wd
    base = core * HALF

    def put_rows(j, tiles):
        dest = pl.ds(pl.multiple_of(base + j * T, T), T)
        rows = pl.ds(pl.multiple_of(j * T, T), T)
        for h in range(2):
            cols = pl.ds(h * D // 2, D // 2)
            w = wown[rows, cols]
            o_w[dest, cols] = w - lr * jnp.concatenate(tiles(h, rows), axis=0).T - lr_wd * w
        remote(o_w.at[dest], o_w.at[dest], partner, out_send, out_recv)

    def moments(h, rows):
        return [t2buf[2 * h + zz, yy, a, :, rows] for zz, yy, a in blocks]

    def moments_early(h, rows):
        out = []
        for zz, yy, a in blocks:
            where = (2 * h + zz, yy, a, ALL, rows)
            upd = t2buf[where] * rf[(2 * h + zz) * RING + yy, W * a:W * a + W] * colv[ROWS_ONE, rows] * colv[pl.ds(1, 1), rows]
            out.append((0.9 * m2buf[where] + 0.1 * upd).astype(BF16).astype(F32))
        return out

    mo_send, mo_recv = next(sends), next(recvs)
    out_send, out_recv = next(sends), next(recvs)

    def state_out():
        wait(frecv, recv.at[f_recv])
        wait(mrecv, recv.at[mo_recv])
        for mine, theirs, out_in, out_out in ((mnew[core], mrecv[...], o_m_in, o_m_out), (fnew[...], frecv[...], o_c_in, o_r_out)):
            lo = jnp.where(on_first, mine, theirs)
            hi = jnp.where(on_first, theirs, mine)
            out_in[:, :HALF] = lo.astype(out_in.dtype)
            out_out[...] = hi[:, :F_OUT].astype(out_out.dtype)
            out_in[:, HALF:] = pltpu.roll(hi[:, HALF - 2 * T:], TAIL, 1)[:, :TAIL].astype(out_in.dtype)
        for new, out in ((r_new, o_r_in), (c_new, o_c_out)):
            rowpad[...] = jnp.broadcast_to(new, rowpad.shape)
            out[...] = jnp.where(on_first, rowpad[...], pltpu.roll(rowpad[...], T - W, 1))[:1, :W]

    def factors(_):
        wait(wown, load_sem.at[w_load])
        colv[pl.ds(1, 1)] = scale
        shifted = lax.broadcasted_iota(jnp.int32, (2 * W, T), 0) + 16 == lax.broadcasted_iota(jnp.int32, (2 * W, T), 1)

        def row_factor(chip, _):
            col = sum_of(jnp.where(shifted, qs[x * 32 + chip * 2 + core], 0.0), 1)
            rf[chip] = jnp.broadcast_to(1.0 / jnp.sqrt(col), (2 * W, T))
            return 0

        lax.fori_loop(0, 16, row_factor, 0)

    def finish_early(j):
        if j == 0:
            a2_end(0)
            a2_end(1)
        put_rows(jnp.int32(j), moments_early)

    def finish(s):
        if s == 2:
            state_out()
        a2_end(s)
        t0, n, _ = GATHER_SEGS[s]

        def tile(j, _):
            put_rows(j, moments)
            return 0

        lax.fori_loop(t0, t0 + n, tile, 0)

    remote(mnew.at[1 - core], mrecv, partner, mo_send, mo_recv)
    gather(GATHER_PLAN, F=finish, R=factors, G=finish_early)

    wait(xown, recv.at[out_recv])
    for ref, sem in ((xown, swap_send), (ms, m_send), (tbuf.at[:3], send_1), (tbuf.at[0, :3], send_2), (fv_ref, fv_send), (rv_ref, rv_send), (q_ref, q_send),
                     (fnew, f_send), (o_w.at[pl.ds(0, (HALF + EARLY * T) * 15 // 16)], send_3), (ms, mo_send), (xown, out_send)):
        wait(ref, send.at[sem])


def store_kernel(w, m_in, m_out, r_in, c_in, r_out, c_out, o_w_in, o_w_out, o_m_in, o_m_out, o_r_in, o_c_in, o_r_out, o_c_out, sem):
    pairs = [(w.at[pl.ds(src + k * rows, rows)], out.at[pl.ds(dst + k * rows, rows)]) for src, out, dst, rows, count in (
        (0, o_w_in, 0, TAIL, 6), (HALF, o_w_out, 0, TAIL, 5), (HALF + F_OUT, o_w_in, HALF, TAIL, 1)) for k in range(count)]
    pairs += [(m_in, o_m_in), (m_out, o_m_out), (r_in, o_r_in), (c_in, o_c_in), (r_out, o_r_out), (c_out, o_c_out)]
    work = [pltpu.make_async_copy(src, dst, sem.at[n]) for n, (src, dst) in enumerate(pairs)]
    for c in work:
        c.start()
    for c in work:
        c.wait()


def call(*args):
    vmem = pl.BlockSpec(memory_space=pltpu.VMEM)
    hbm = pl.BlockSpec(memory_space=pltpu.HBM)
    smem = pl.BlockSpec(memory_space=pltpu.SMEM)
    small = (((W, F_IN), BF16), ((W, F_OUT), BF16), ((1, W), F32), ((1, F_IN), F32), ((1, F_OUT), F32), ((1, W), F32))
    in_vmem = [pltpu.VMEM(*a) for a in small]
    args = args[:3] + tuple(pltpu.with_memory_space_constraint(a, pltpu.HBM) for a in args[3:])

    def buf(*shape):
        return pltpu.VMEM(shape, F32)

    half, whole, part, line = (HALF, D), (RING, RING, 2, W, HALF), (W, HALF), (1, HALF)
    held = pl.pallas_call(
        kernel,
        name="adafactor_step",
        out_shape=(buf(2 * HALF, D), *in_vmem),
        in_specs=[smem] * 3 + [hbm] * (len(args) - 3),
        out_specs=(vmem,) * (1 + len(small)),
        scratch_shapes=[
            *in_vmem, buf(*half), buf(*half), buf(*half), buf(*whole), buf(*whole), buf(RING, RING, 2, W, EARLY * T), buf(2, *part), buf(16, 2 * W, T), buf(8, HALF),
            buf(2, RING, *part), buf(2, 2, RING, *part), buf(2, RING, *part), buf(2, *part), buf(3, 2, *part),
            buf(2, *part), buf(*part), buf(*part), buf(*line), buf(*line), buf(*line),
            buf(16, *line), buf(8, 8, T), buf(128, 1, T),
            buf(2 * W, HALF), buf(W, T), buf(W, 2 * T), buf(1, T), buf(1, 2 * T), buf(8, T),
            pltpu.SemaphoreType.DMA((N_LOAD,)), pltpu.SemaphoreType.DMA((N_SEND,)), pltpu.SemaphoreType.DMA((N_RECV,)),
        ],
        compiler_params=pltpu.CompilerParams(collective_id=0, has_side_effects=True, vmem_limit_bytes=40 << 20),
    )(*args)
    return pl.pallas_call(
        store_kernel,
        name="store_outputs",
        out_shape=tuple(jax.ShapeDtypeStruct(*a) for a in (((F_IN, D), F32), ((F_OUT, D), F32), *small)),
        in_specs=[vmem] * (1 + len(small)),
        out_specs=(hbm,) * (2 + len(small)),
        scratch_shapes=[pltpu.SemaphoreType.DMA((18,))],
        compiler_params=pltpu.CompilerParams(vmem_limit_bytes=16 << 20),
    )(*held)


def solution(mesh):
    def body(w_in, w_out, g_in, g_out, m_in, m_out, r_in, c_in, r_out, c_out, learn_rate, weight_decay, beta_two):
        outs = call(learn_rate[None], weight_decay[None], beta_two[None], g_in[0, 0].T, g_out[0, 0], w_in[0].T, w_out[0], m_in[0], m_out[0].T, r_in, c_in, r_out, c_out)
        return (outs[0].T[None], outs[1][None], outs[2][None], outs[3].T[None], *outs[4:])

    rows, cols, f_last, f_mid = P(None, 'dp'), P(None, 'tp'), P(None, None, 'tp'), P(None, 'tp', None)
    m_specs = (P(None, 'dp', 'tp'), P(None, 'tp', 'dp'))
    stats = (rows, cols, cols, rows)
    in_specs = (f_last, f_mid, P('dp', None, None, 'tp'), P('dp', None, 'tp', None), *m_specs, *stats, P(), P(), P())
    return jax.shard_map(body, mesh=mesh, in_specs=in_specs, out_specs=(f_last, f_mid, *m_specs, *stats), check_vma=False)
```

```python
import jax
import jax.numpy as jnp
from jax import lax
from jax.experimental import pallas as pl
from jax.experimental.pallas import tpu as pltpu
from jax.sharding import PartitionSpec as P

MESH = pl.DeviceIdType.MESH
F32 = jnp.float32
BF16 = jnp.bfloat16
ALL = slice(None)

D = 768
F_IN = 1344
F_OUT = 960
HALF = 1152
TAIL = 192
N_IN = 5376
N_OUT = 3840
T = 128
W = 24
RING = 4
REDUCE_SEGS = ((0, 2, 1), (2, 2, 1), (4, 5, 2))
EARLY = 3
GATHER_SEGS = ((0, 3, 2), (0, 3, 1), (3, 2, 1), (5, 2, 1), (7, 2, 1))
BLOCKS = (0, 1, 3, 2)
SPLIT = ((0,), (1, 3), (2,))
GATHER_UNITS = (SPLIT, SPLIT, SPLIT, SPLIT, SPLIT)
REDUCE_UNITS = ((None,), (None,), (2, 1, 3, 0))
RELAY_LAST = (True, False, False)
REDUCE_PLAN = ("K0,a1,b10,S0,B00,S1,B10,M00,S2,B20,B21,B22,B23,M10,E00,M20,M21", "M22,M23,E10,C0,E20,E21,E22,E23,m1,n1,b11,p10,F1,F0,F2")
EARLY_PLAN = ("A0,B00,W1,B12,P11,M0",)
EARLY_PLAN_END = ("N0,B01,P00,W0,B02,P12,P01",)
GATHER_PLAN = ("A2,A3,B30,A4,B20,B40,P02,R0,M2,M3,N3,B31,M4,N2,B21", "W2,B22,N4,G0,W3,B32,G1,B41,W4,G2,B42,P21,P20,P22,P31", "P30,P32,P40,P41,P42,F2,F3,F4")
FAR_FIRST = (2, 1, 3, 0)
ROWS_ONE = pl.ds(0, 1)
N_SEND = 11
N_RECV = 61
N_LOAD = 10


def spans(half, lo, hi):
    if half == 0:
        return [(0, lo, lo, hi - lo)]
    out = []
    if lo < F_OUT:
        out.append((1, lo, lo, min(hi, F_OUT) - lo))
    if hi > F_OUT:
        start = max(lo, F_OUT)
        out.append((0, start + TAIL, start, hi - start))
    return out


def join_tail(out_val, tail_val, pad_a, pad_b):
    pad_a[...] = jnp.zeros_like(pad_a)
    pad_b[...] = jnp.zeros_like(pad_b)
    cut = F_OUT - F_OUT % T
    pad_a[:, :F_OUT - cut] = out_val[:, cut:]
    pad_b[:, :TAIL] = tail_val
    moved = pltpu.roll(pad_b[...], F_OUT - cut, 1)
    lane = lax.broadcasted_iota(jnp.int32, pad_a.shape, 1)
    mid = jnp.where(lane < F_OUT - cut, pad_a[...], moved[:, :T])
    return jnp.concatenate([out_val[:, :cut], mid, moved[:, T:]], axis=1)


def kernel(lr_ref, wd_ref, beta_ref, g_in, g_out, w_in, w_out, h_m_in, h_m_out, h_r_in, h_c_in, h_r_out, h_c_out,
           o_w, o_m_in, o_m_out, o_r_in, o_c_in, o_r_out, o_c_out,
           m_in, m_out, r_in, c_in, r_out, c_out,
           xown, xrecv, wown, tbuf, t2buf, m2buf, mnew, rf, colv, far, dc, pbuf, far2, dc2,
           mx, ms, mrecv, fo, fnew, frecv, fv, rv, qs, gb, pad_a, pad_b, pad_c, pad_d, rowpad,
           load_sem, send, recv):
    x = lax.axis_index("tp")
    d = lax.axis_index("dp")
    core = lax.rem(d, 2)
    p = lax.div(d, 2)
    y = lax.rem(p, RING)
    z = lax.div(p, RING)
    on_first = core == 0
    line_me = x * 2 + core

    def at(xx, pp, cc):
        return (xx, pp * 2 + cc)

    turn = 1 + 2 * core

    def step(i, k):
        return lax.rem(i + k * turn, RING)

    partner = at(x, p, 1 - core)
    sends = iter(range(N_SEND))
    recvs = iter(range(N_RECV))
    loads = iter(range(N_LOAD))

    def remote(src, dst, dev, s, r):
        if 0 not in src.shape:
            pltpu.make_async_remote_copy(src_ref=src, dst_ref=dst, send_sem=send.at[s], recv_sem=recv.at[r], device_id=dev, device_id_type=MESH).start()

    def wait(ref, sem):
        pltpu.make_async_copy(ref, ref, sem).wait()

    small = [pltpu.make_async_copy(src, dst, load_sem.at[next(loads)]) for src, dst in (
        (h_m_in, m_in), (h_m_out, m_out), (h_r_in, r_in), (h_c_in, c_in), (h_r_out, r_out), (h_c_out, c_out))]
    for c in small:
        c.start()
    x_load = [next(loads) for _ in REDUCE_SEGS]
    for me in range(2):
        @pl.when(core == me)
        def _():
            for (t0, n, _), sem in zip(REDUCE_SEGS, x_load):
                for which, lo, to, rows in spans(me, t0 * T, (t0 + n) * T):
                    pltpu.make_async_copy((g_in, g_out)[which].at[pl.ds(lo, rows)], xown.at[pl.ds(to, rows)], load_sem.at[sem]).start()

    barrier = pltpu.get_barrier_semaphore()
    ring = ((y, *(at(x, z * RING + step(y, k), core) for k in (1, 3, 2))),
            (z, *(at(x, step(z, k) * RING + y, core) for k in (1, 3, 2))))
    line = []
    for k in range(1, 8):
        other = lax.rem(line_me + k, 8)
        line.append(at(lax.div(other, 2), p, lax.rem(other, 2)))
    plane = [at(x, step(z, i) * RING + step(y, k), core) for i in FAR_FIRST for k in FAR_FIRST if i or k]
    greet = [dev for _, right, left, _ in ring for dev in (right, left)] + [at(step(x, k), p, core) for k in (2, 1, 3)] + [partner]
    for dev in greet:
        pl.semaphore_signal(barrier, inc=1, device_id=dev, device_id_type=MESH)

    for c in small:
        c.wait()
    first = m_in[:, :HALF].astype(F32)
    second = join_tail(m_out[...].astype(F32), m_in[:, HALF:].astype(F32), pad_a, pad_b)
    mx[core] = jnp.where(on_first, first, second)
    ms[...] = jnp.where(on_first, second, first)
    fo[...] = jnp.where(on_first, c_in[:, :HALF], join_tail(r_out[...], c_in[:, HALF:], pad_c, pad_d))
    pl.semaphore_wait(barrier, len(greet))
    m_send, m_recv = next(sends), next(recvs)
    remote(ms, mx.at[core], partner, m_send, m_recv)

    swap_send = next(sends)
    swap_recv = [next(recvs) for _ in REDUCE_SEGS]
    for me in range(2):
        @pl.when(core == me)
        def _():
            for (t0, n, _), sem in zip(REDUCE_SEGS, swap_recv):
                for which, lo, to, rows in spans(1 - me, t0 * T, (t0 + n) * T):
                    remote((g_in, g_out)[which].at[pl.ds(lo, rows)], xrecv.at[pl.ds(to, rows)], partner, swap_send, sem)

    w_load = next(loads)
    for me in range(2):
        @pl.when(core == me)
        def _():
            for which, lo, to, rows in spans(me, 0, HALF):
                pltpu.make_async_copy((w_in, w_out)[which].at[pl.ds(lo, rows)], wown.at[pl.ds(to, rows)], load_sem.at[w_load]).start()

    def lanes_of(seg):
        t0, n, n_a = seg
        return pl.ds(t0 * T, n_a * T), pl.ds((t0 + n_a) * T, (n - n_a) * T), pl.ds(t0 * T, n * T)

    blocks = [(i // 8, i // 2 % RING, i % 2) for i in range(16)]

    def transpose_in(j, _):
        rows = pl.ds(pl.multiple_of(j * T, T), T)
        for h in range(2):
            cols = pl.ds(h * D // 2, D // 2)
            t = (xown[rows, cols] + xrecv[rows, cols]).T
            for i, (zz, yy, a) in enumerate(blocks):
                tbuf[2 * h + zz, yy, a, :, rows] = t[W * i:W * i + W]
        return 0

    cross = (z, y)

    def spot(a, k, q):
        return (q, k, 0) if a == 0 else (k, q, 1)

    def piece(buf, a, k, q, lanes):
        return buf.at[(*spot(a, k, q), ALL, lanes)]

    def ring_of(a):
        i, right, left, _ = ring[a]
        return i, right, left, step(i, 1), step(i, 3), step(i, 2)

    def block(a, off):
        return ALL if off is None else step(cross[a], off)

    send_1, send_2 = next(sends), next(sends)
    far_sem, dc_sem = ([[next(recvs) for _ in u] for u in REDUCE_UNITS] for _ in range(2))
    dc2_sem = [next(recvs) for _ in REDUCE_SEGS]
    far2_sem = [next(recvs) if relay else None for relay in RELAY_LAST]

    def rs_begin(s, u):
        la, lb, _ = lanes_of(REDUCE_SEGS[s])
        off = REDUCE_UNITS[s][u]
        for a in range(2):
            i, right, left, r, l, f = ring_of(a)
            q = block(a, off)
            remote(piece(tbuf, a, f, q, la), far.at[a, q, :, la], right, send_1, far_sem[s][u])
            remote(piece(tbuf, a, f, q, lb), far.at[a, q, :, lb], left, send_1, far_sem[s][u])
        for a in range(2):
            i, right, left, r, l, f = ring_of(a)
            q = block(a, off)
            remote(piece(tbuf, a, r, q, lb), dc.at[0, a, q, :, lb], right, send_1, dc_sem[s][u])
            remote(piece(tbuf, a, l, q, la), dc.at[0, a, q, :, la], left, send_1, dc_sem[s][u])

    def unit_blocks(off):
        return pl.ds(0, RING if off is None else 1)

    def rs_middle(s, u):
        la, lb, full = lanes_of(REDUCE_SEGS[s])
        off = REDUCE_UNITS[s][u]
        wait(far.at[:, unit_blocks(off), :, full], recv.at[far_sem[s][u]])
        for a in range(2):
            i, right, left, r, l, f = ring_of(a)
            q = block(a, off)
            for k, lanes, dev in ((r, la, right), (l, lb, left)):
                if lanes.size:
                    tbuf[(*spot(a, k, q), ALL, lanes)] += far[a, q, :, lanes]
                remote(piece(tbuf, a, k, q, lanes), dc.at[1, a, q, :, lanes], dev, send_1, dc_sem[s][u])

    def rs_end(s, u):
        la, lb, full = lanes_of(REDUCE_SEGS[s])
        off = REDUCE_UNITS[s][u]
        wait(dc.at[:, :, unit_blocks(off), :, full], recv.at[dc_sem[s][u]])
        for a in range(2):
            q = block(a, off)
            pbuf[a, q, :, full] = tbuf[(*spot(a, ring_of(a)[0], q), ALL, full)] + dc[0, a, q, :, full] + dc[1, a, q, :, full]
        for a in range(2):
            i, right, left, r, l, f = ring_of(1 - a)
            if RELAY_LAST[s]:
                remote(pbuf.at[a, f, :, la], far2.at[a, :, la], right, send_2, far2_sem[s])
                remote(pbuf.at[a, f, :, lb], far2.at[a, :, lb], left, send_2, far2_sem[s])
                remote(pbuf.at[a, r, :, lb], dc2.at[0, a, :, lb], right, send_2, dc2_sem[s])
                remote(pbuf.at[a, l, :, la], dc2.at[0, a, :, la], left, send_2, dc2_sem[s])
            else:
                for slot, (k, o, dev) in enumerate(((f, 2, ring[1 - a][-1]), (r, 1, right), (l, 3, left))):
                    if off is None or off == o:
                        remote(pbuf.at[a, k, :, full], dc2.at[slot, a, :, full], dev, send_2, dc2_sem[s])

    def rs_cross(s):
        la, lb, full = lanes_of(REDUCE_SEGS[s])
        wait(far2.at[:, :, full], recv.at[far2_sem[s]])
        for a in range(2):
            i, right, left, r, l, f = ring_of(1 - a)
            for k, lanes, dev in ((r, la, right), (l, lb, left)):
                if lanes.size:
                    pbuf[a, k, :, lanes] += far2[a, :, lanes]
                remote(pbuf.at[a, k, :, lanes], dc2.at[1, a, :, lanes], dev, send_2, dc2_sem[s])

    def rs_finish(s):
        full = lanes_of(REDUCE_SEGS[s])[-1]
        slots = 2 if RELAY_LAST[s] else 3
        wait(dc2.at[:slots, :, :, full], recv.at[dc2_sem[s]])
        for a in range(2):
            acc = pbuf[a, cross[a], :, full]
            for slot in range(slots):
                acc = acc + dc2[slot, a, :, full]
            gb[W * a:W * a + W, full] = acc

    def rs_load(s):
        t0, n, _ = REDUCE_SEGS[s]
        rows = pl.ds(t0 * T, n * T)
        wait(xown.at[rows], load_sem.at[x_load[s]])
        wait(xown.at[rows], recv.at[swap_recv[s]])
        lax.fori_loop(t0, t0 + n, transpose_in, 0)

    send_3 = next(sends)
    a1_first, a1_rest, a1_fwd, a2_rest = ([next(recvs) for _ in GATHER_SEGS] for _ in range(4))
    a1_rest[3] = a1_first[3]
    a2_first = [[next(recvs) for _ in u] for u in GATHER_UNITS]

    def swap_around(ref, ring_a, s, first, rest):
        la, lb, _ = lanes_of(GATHER_SEGS[s])
        for lanes_r, lanes_l, sem in ((la, lb, first), (lb, la, rest)):
            for a in range(2):
                i, right, left, r, l, f = ring_of(ring_a(a))
                for src in ref(a, i, lanes_r):
                    remote(src, src, right, send_3, sem)
                for src in ref(a, i, lanes_l):
                    remote(src, src, left, send_3, sem)

    def pass_on(ref, ring_a, s, sem):
        la, lb, _ = lanes_of(GATHER_SEGS[s])
        for a in range(2):
            i, right, left, r, l, f = ring_of(ring_a(a))
            for src in ref(a, l, la):
                remote(src, src, right, send_3, sem)
            for src in ref(a, r, lb):
                remote(src, src, left, send_3, sem)

    def store_of(s):
        return m2buf if s == 1 else t2buf

    def one_ref(s):
        return lambda a, q, lanes: [piece(store_of(s), a, ring_of(a)[0], q, lanes)]

    def two_ref(s, u):
        offs = GATHER_UNITS[s][u]
        return lambda a, k, lanes: [piece(store_of(s), a, k, block(a, o), lanes) for o in (offs or (None,))]

    def same(a):
        return a

    def other(a):
        return 1 - a

    def a1_begin(s):
        swap_around(one_ref(s), other, s, a1_first[s], a1_rest[s])

    def a2_begin(s, u):
        swap_around(two_ref(s, u), same, s, a2_first[s][u], a2_rest[s])

    def a1_middle(s):
        full = lanes_of(GATHER_SEGS[s])[-1]
        both = a1_rest[s] == a1_first[s]
        wait(dc2.at[:2, :, :, full] if both else far2.at[:, :, full], recv.at[a1_first[s]])
        pass_on(one_ref(s), other, s, a1_fwd[s])

    def a1_near(s):
        if a1_rest[s] != a1_first[s]:
            wait(far2.at[:, :, lanes_of(GATHER_SEGS[s])[-1]], recv.at[a1_rest[s]])

    def a1_far(s):
        wait(far2.at[:, :, lanes_of(GATHER_SEGS[s])[-1]], recv.at[a1_fwd[s]])

    def a2_middle(s, u):
        wait(far.at[:, :len(GATHER_UNITS[s][u] or BLOCKS), :, lanes_of(GATHER_SEGS[s])[-1]], recv.at[a2_first[s][u]])
        pass_on(two_ref(s, u), same, s, a2_rest[s])

    def a2_end(s):
        wait(dc.at[:, :, :, :, lanes_of(GATHER_SEGS[s])[-1]], recv.at[a2_rest[s]])

    def gather(plan, **more):
        follow(plan, dict(A=a1_begin, B=a2_begin, M=a1_middle, N=a1_near, W=a1_far, P=a2_middle, **more))

    early = pl.ds(0, EARLY * T)
    late = pl.ds(EARLY * T, HALF - EARLY * T)

    def keep(_):
        wait(mx.at[0], recv.at[m_recv])
        for a in range(2):
            m2buf[z, y, a] = mx[a, :, early]

    def follow(plan, table):
        for item in ",".join(plan).split(","):
            table[item[0]](*(int(c) for c in item[1:]))

    follow(REDUCE_PLAN, dict(S=rs_load, B=rs_begin, M=rs_middle, E=rs_end, C=rs_cross, F=rs_finish, K=keep, a=a1_begin, b=a2_begin, m=a1_middle, n=a1_near, w=a1_far, p=a2_middle))

    lane = lax.broadcasted_iota(jnp.int32, (1, HALF), 1)
    is_in = lane >= jnp.where(on_first, 0, F_OUT)
    eye = lax.broadcasted_iota(jnp.int32, (2 * W, T), 0) == lax.broadcasted_iota(jnp.int32, (2 * W, T), 1)

    def sum_of(v, axis):
        return jnp.sum(v, axis=axis, keepdims=True)

    def only_in(v):
        return jnp.where(is_in, v, 0.0)

    def only_out(v):
        return jnp.where(is_in, 0.0, v)

    def to_row(col):
        return sum_of(jnp.where(eye, col, 0.0), 0)

    def to_col(row):
        return sum_of(jnp.where(eye, row, 0.0), 1)

    def spread(slots, me, devs):
        ss, rs = next(sends), next(recvs)
        for dev in devs:
            remote(slots.at[me], slots.at[me], dev, ss, rs)
        return slots.at[pl.ds(0, len(devs))], ss, rs

    g = gb[...]
    sq = g * g + 1e-30
    fv[p] = sum_of(sq, 0)
    fv_ref, fv_send, fv_recv = spread(fv, p, plane)
    for row, col in enumerate((only_in(sq), only_out(sq))):
        rv[line_me, row:row + 1, :] = to_row(sum_of(col, 1))
    for row, ref in ((2, r_in), (3, c_out)):
        rowpad[...] = jnp.zeros_like(rowpad)
        rowpad[ROWS_ONE, :W] = ref[...]
        rv[line_me, row:row + 1, :] = jnp.where(on_first, rowpad[...], pltpu.roll(rowpad[...], W, 1))[:1]
    rv[line_me, RING:, :] = jnp.zeros((RING, T), F32)
    rv_ref, rv_send, rv_recv = spread(rv, line_me, line)

    lr, wd, beta = lr_ref[0], wd_ref[0], beta_ref[0]
    for a in range(2):
        t2buf[z, y, a, :, early] = gb[W * a:W * a + W, early]
    gather(EARLY_PLAN)
    wait(rv_ref, recv.at[rv_recv])
    row_sum = jnp.sum(rv[...], axis=0)
    row_old = rv[0] + rv[1]
    r_new = beta * row_old[2:3] + (1.0 - beta) * (row_sum[:1] / N_IN)
    c_new = beta * row_old[3:4] + (1.0 - beta) * (row_sum[1:2] / N_OUT)
    v = g * jnp.where(is_in, 1.0 / jnp.sqrt(to_col(r_new)), 1.0 / jnp.sqrt(to_col(c_new)))
    sum_rows = sum_of(r_new, 1)
    wait(fv_ref, recv.at[fv_recv])
    f_new = beta * fo[...] + (1.0 - beta) * (jnp.sum(fv[...], axis=0) / D)
    col_scale = 1.0 / jnp.sqrt(f_new)
    u = v * col_scale
    uu = u * u
    f_out = sum_of(only_out(f_new), 1)

    def total(v):
        return jnp.broadcast_to(sum_of(sum_of(v, 0), 1), (1, T))

    pick = lax.broadcasted_iota(jnp.int32, (1, T), 1)
    me_all = x * 32 + d
    share = jnp.where(pick == 0, total(only_in(uu)), jnp.where(pick == 1, total(only_out(uu)), jnp.where(pick == 2, f_out / 16, sum_rows / 8)))
    share = jnp.where(pick < 16, share, pltpu.roll(jnp.where(on_first, r_new, c_new), 16, 1))
    qs[me_all] = share
    q_send, q_recv = next(sends), next(recvs)

    def tell(k, _):
        chip = lax.rem(z + 6 - lax.div(k, RING), RING) * RING + lax.rem(y + 6 - lax.rem(k, RING), RING)
        for i in FAR_FIRST:
            for c in (1 - core, core):
                def go():
                    remote(qs.at[me_all], qs.at[me_all], at(lax.rem(x + i, RING), chip, c), q_send, q_recv)
                if i == 0 and c is core:
                    pl.when(k != 10)(go)
                else:
                    go()
        return 0

    lax.fori_loop(0, 16, tell, 0)
    q_ref = qs.at[pl.ds(0, 127)]
    gb[...] = u
    fnew[...] = f_new
    f_send, f_recv = next(sends), next(recvs)
    remote(fnew, frecv, partner, f_send, f_recv)
    colv[ROWS_ONE] = col_scale
    gather(EARLY_PLAN_END)
    wait(q_ref, recv.at[q_recv])
    totals = jnp.sum(qs[...], axis=0)
    mean_in = totals[:, 3:4] / D
    mean_out = totals[:, 2:3] / N_OUT
    rms_in = jnp.sqrt(totals[:, :1] * mean_in / (D * N_IN))
    rms_out = jnp.sqrt(totals[:, 1:2] * mean_out / (D * N_OUT))
    scale = jnp.where(is_in, jnp.sqrt(mean_in) / jnp.maximum(1.0, rms_in), jnp.sqrt(mean_out) / jnp.maximum(1.0, rms_out))

    for a in range(2):
        mnew[a] = (0.9 * mx[a] + 0.1 * (gb[W * a:W * a + W] * scale)).astype(BF16).astype(F32)
        t2buf[z, y, a, :, late] = mnew[a, :, late]

    lr_wd = lr * wd
    base = core * HALF

    def put_rows(j, tiles):
        dest = pl.ds(pl.multiple_of(base + j * T, T), T)
        rows = pl.ds(pl.multiple_of(j * T, T), T)
        for h in range(2):
            cols = pl.ds(h * D // 2, D // 2)
            w = wown[rows, cols]
            o_w[dest, cols] = w - lr * jnp.concatenate(tiles(h, rows), axis=0).T - lr_wd * w
        remote(o_w.at[dest], o_w.at[dest], partner, out_send, out_recv)

    def moments(h, rows):
        return [t2buf[2 * h + zz, yy, a, :, rows] for zz, yy, a in blocks]

    def moments_early(h, rows):
        out = []
        for zz, yy, a in blocks:
            where = (2 * h + zz, yy, a, ALL, rows)
            upd = t2buf[where] * rf[(2 * h + zz) * RING + yy, W * a:W * a + W] * colv[ROWS_ONE, rows] * colv[pl.ds(1, 1), rows]
            out.append((0.9 * m2buf[where] + 0.1 * upd).astype(BF16).astype(F32))
        return out

    mo_send, mo_recv = next(sends), next(recvs)
    out_send, out_recv = next(sends), next(recvs)

    def state_out():
        wait(frecv, recv.at[f_recv])
        wait(mrecv, recv.at[mo_recv])
        for mine, theirs, out_in, out_out in ((mnew[core], mrecv[...], o_m_in, o_m_out), (fnew[...], frecv[...], o_c_in, o_r_out)):
            lo = jnp.where(on_first, mine, theirs)
            hi = jnp.where(on_first, theirs, mine)
            out_in[:, :HALF] = lo.astype(out_in.dtype)
            out_out[...] = hi[:, :F_OUT].astype(out_out.dtype)
            out_in[:, HALF:] = pltpu.roll(hi[:, HALF - 2 * T:], TAIL, 1)[:, :TAIL].astype(out_in.dtype)
        for new, out in ((r_new, o_r_in), (c_new, o_c_out)):
            rowpad[...] = jnp.broadcast_to(new, rowpad.shape)
            out[...] = jnp.where(on_first, rowpad[...], pltpu.roll(rowpad[...], T - W, 1))[:1, :W]

    def factors(_):
        wait(wown, load_sem.at[w_load])
        colv[pl.ds(1, 1)] = scale
        shifted = lax.broadcasted_iota(jnp.int32, (2 * W, T), 0) + 16 == lax.broadcasted_iota(jnp.int32, (2 * W, T), 1)

        def row_factor(chip, _):
            col = sum_of(jnp.where(shifted, qs[x * 32 + chip * 2 + core], 0.0), 1)
            rf[chip] = jnp.broadcast_to(1.0 / jnp.sqrt(col), (2 * W, T))
            return 0

        lax.fori_loop(0, 16, row_factor, 0)

    def finish_early(j):
        if j == 0:
            a2_end(0)
            a2_end(1)
        put_rows(jnp.int32(j), moments_early)

    def finish(s):
        if s == 2:
            state_out()
        a2_end(s)
        t0, n, _ = GATHER_SEGS[s]

        def tile(j, _):
            put_rows(j, moments)
            return 0

        lax.fori_loop(t0, t0 + n, tile, 0)

    remote(mnew.at[1 - core], mrecv, partner, mo_send, mo_recv)
    gather(GATHER_PLAN, F=finish, R=factors, G=finish_early)

    wait(xown, recv.at[out_recv])
    for ref, sem in ((xown, swap_send), (ms, m_send), (tbuf.at[:3], send_1), (tbuf.at[0, :3], send_2), (fv_ref, fv_send), (rv_ref, rv_send), (q_ref, q_send),
                     (fnew, f_send), (o_w.at[pl.ds(0, (HALF + EARLY * T) * 15 // 16)], send_3), (ms, mo_send), (xown, out_send)):
        wait(ref, send.at[sem])


def store_kernel(w, m_in, m_out, r_in, c_in, r_out, c_out, o_w_in, o_w_out, o_m_in, o_m_out, o_r_in, o_c_in, o_r_out, o_c_out, sem):
    work = [pltpu.make_async_copy(w.at[pl.ds(src, rows)], out.at[pl.ds(dst, rows)], sem.at[0]) for src, out, dst, rows in (
        (0, o_w_in, 0, HALF), (HALF, o_w_out, 0, F_OUT), (HALF + F_OUT, o_w_in, HALF, TAIL))]
    few = [pltpu.make_async_copy(src, dst, sem.at[n + 1]) for n, (src, dst) in enumerate((
        (m_in, o_m_in), (m_out, o_m_out), (r_in, o_r_in), (c_in, o_c_in), (r_out, o_r_out), (c_out, o_c_out)))]
    for c in work + few:
        c.start()
    for c in few:
        c.wait()
    pltpu.make_async_copy(w, w, sem.at[0]).wait()


def call(*args):
    vmem = pl.BlockSpec(memory_space=pltpu.VMEM)
    hbm = pl.BlockSpec(memory_space=pltpu.HBM)
    smem = pl.BlockSpec(memory_space=pltpu.SMEM)
    small = (((W, F_IN), BF16), ((W, F_OUT), BF16), ((1, W), F32), ((1, F_IN), F32), ((1, F_OUT), F32), ((1, W), F32))
    in_vmem = [pltpu.VMEM(*a) for a in small]
    args = args[:3] + tuple(pltpu.with_memory_space_constraint(a, pltpu.HBM) for a in args[3:])

    def buf(*shape):
        return pltpu.VMEM(shape, F32)

    half, whole, part, line = (HALF, D), (RING, RING, 2, W, HALF), (W, HALF), (1, HALF)
    held = pl.pallas_call(
        kernel,
        name="adafactor_step",
        out_shape=(buf(2 * HALF, D), *in_vmem),
        in_specs=[smem] * 3 + [hbm] * (len(args) - 3),
        out_specs=(vmem,) * (1 + len(small)),
        scratch_shapes=[
            *in_vmem, buf(*half), buf(*half), buf(*half), buf(*whole), buf(*whole), buf(RING, RING, 2, W, EARLY * T), buf(2, *part), buf(16, 2 * W, T), buf(8, HALF),
            buf(2, RING, *part), buf(2, 2, RING, *part), buf(2, RING, *part), buf(2, *part), buf(3, 2, *part),
            buf(2, *part), buf(*part), buf(*part), buf(*line), buf(*line), buf(*line),
            buf(16, *line), buf(8, 8, T), buf(128, 1, T),
            buf(2 * W, HALF), buf(W, T), buf(W, 2 * T), buf(1, T), buf(1, 2 * T), buf(8, T),
            pltpu.SemaphoreType.DMA((N_LOAD,)), pltpu.SemaphoreType.DMA((N_SEND,)), pltpu.SemaphoreType.DMA((N_RECV,)),
        ],
        compiler_params=pltpu.CompilerParams(collective_id=0, has_side_effects=True, vmem_limit_bytes=40 << 20),
    )(*args)
    return pl.pallas_call(
        store_kernel,
        name="store_outputs",
        out_shape=tuple(jax.ShapeDtypeStruct(*a) for a in (((F_IN, D), F32), ((F_OUT, D), F32), *small)),
        in_specs=[vmem] * (1 + len(small)),
        out_specs=(hbm,) * (2 + len(small)),
        scratch_shapes=[pltpu.SemaphoreType.DMA((7,))],
        compiler_params=pltpu.CompilerParams(vmem_limit_bytes=16 << 20),
    )(*held)


def solution(mesh):
    def body(w_in, w_out, g_in, g_out, m_in, m_out, r_in, c_in, r_out, c_out, learn_rate, weight_decay, beta_two):
        outs = call(learn_rate[None], weight_decay[None], beta_two[None], g_in[0, 0].T, g_out[0, 0], w_in[0].T, w_out[0], m_in[0], m_out[0].T, r_in, c_in, r_out, c_out)
        return (outs[0].T[None], outs[1][None], outs[2][None], outs[3].T[None], *outs[4:])

    rows, cols, f_last, f_mid = P(None, 'dp'), P(None, 'tp'), P(None, None, 'tp'), P(None, 'tp', None)
    m_specs = (P(None, 'dp', 'tp'), P(None, 'tp', 'dp'))
    stats = (rows, cols, cols, rows)
    in_specs = (f_last, f_mid, P('dp', None, None, 'tp'), P('dp', None, 'tp', None), *m_specs, *stats, P(), P(), P())
    return jax.shard_map(body, mesh=mesh, in_specs=in_specs, out_specs=(f_last, f_mid, *m_specs, *stats), check_vma=False)
```
